128 devices in a mesh: gx: 8 (over z, core), gy: 4 (over y), gz: 4 (over x).
Axes of the slice: x: 4, y: 4, z: 4, core: 2. Of those that a mesh axis runs over, the one named last changes fastest.
Arguments:
- pressure_rhs: float32 [128, 128, 2048], P('gx', 'gy', 'gz'), may hold values from -6 to 6
- shift_diag: float32 [128, 128, 2048], P('gx', 'gy', 'gz'), may hold values from 0.02 to 0.3
- positions: float32 [3, 1048576], P(None, ('gx', 'gy', 'gz')), may hold values from -6 to 6
- normals: float32 [3, 1048576], P(None, ('gx', 'gy', 'gz')), may hold values from -6 to 6
- tension: float32 [1048576], P(('gx', 'gy', 'gz')), may hold values from 0.3 to 3
- edge_weight: float32 [6, 1048576], P(None, ('gx', 'gy', 'gz')), may hold values from 0.5 to 2
- owner_map: int32 [1048576, 1], P(('gx', 'gy', 'gz')), may hold values from 0 to 127; in each aligned block of 8192 rows (0 to 8191, 8192 to 16383, ...) at most 256 rows name the same one
- cell_map: int32 [1048576], P(('gx', 'gy', 'gz')), may hold values from 0 to 262143
- connectivity: int32 [6, 1048576], P(None, ('gx', 'gy', 'gz')), may hold values from 0 to 1048575, as said below
Outputs:
- pressure: float32 [128, 128, 2048], P('gx', 'gy', 'gz')
- surface_force: float32 [3, 1048576], P(None, ('gx', 'gy', 'gz'))
The draws below stay inside these ranges and needn't reach their ends.
Inputs may be any that keep to these rules, and one draw needn't show every extreme that they name: `connectivity`: each neighbour index differs from the point's own index by 1 to 64, counted cyclically over 1048576; the distance 64 occurs. `owner_map`: among the points of one device no owner is named more than 256 times, a bound that some block reaches.
All inputs are finite; a program needn't handle non-finite values.
Results may differ from the reference program's by a relative error of at most 0.0003.
Values sent between devices are 32-bit elements; how exact they have to be, the bound alone decides.
A program may use at most 192 MiB of HBM per device.

```python
import math
import jax
import jax.numpy as jnp
import numpy as np

CX = 16
CY = 32
CZ = 512
PTS_DEV = 8192
NEIGH = 6
HALO = 64
SMOOTH = 3
COARSE_SMOOTH = 4
POINTS = 1048576
CAP = 256
NX = 128
NY = 128
NZ = 2048
N_GY = 4
N_GZ = 4
DEVICES = 128


def draw_connectivity(key, part):
    first = jax.random.fold_in(key, 11)
    second = jax.random.fold_in(key, 12)
    reach = jax.random.randint(first, (NEIGH, POINTS), 1, HALO + 1)
    reach = reach.at[0, 0].set(HALO)
    sign = jax.random.randint(second, (NEIGH, POINTS), 0, 2) * 2 - 1
    base = jnp.arange(POINTS, dtype=jnp.int32)[None, :]
    return ((base + sign * reach) % POINTS).astype(jnp.int32)


def plant(entries, stream_key, smallest, high):
    dims = entries.shape
    place = [jax.random.randint(jax.random.fold_in(stream_key, axis), (), 0, dims[axis]) for axis in range(len(dims))]
    entries = entries.at[tuple(place)].set(smallest)
    longest = dims.index(max(dims))
    place[longest] = (place[longest] + 1) % dims[longest]
    return entries.at[tuple(place)].set(high)


def block_levels(own_key, extent, pieces, least, top_value):
    factor_of, own = 1.0, jax.random.fold_in(own_key, 6)
    for axis_at, shards_of in pieces:
        heights = jnp.exp(jax.random.uniform(jax.random.fold_in(own, axis_at), (shards_of,), jnp.float32, least / len(pieces), top_value / len(pieces)))
        factor_of = factor_of * jnp.repeat(heights, extent[axis_at] // shards_of).reshape([-1 if axis == axis_at else 1 for axis in range(len(extent))])
    return factor_of


def deal_out(key, own, number, rows, amount, top, most, slope):
    sequence = jax.random.permutation(key, amount)
    heavy_load, common = shares(amount, rows * top, most, slope, True), shares(amount, rows * top, most, slope, False)
    places = jnp.arange(amount)

    def named(tallies, rotation):
        used = int((tallies > 0).sum())
        fixed = max(1, used // 4)
        shifted = fixed + (places - fixed + rotation * (used - fixed)) % max(1, amount - fixed)
        return jnp.zeros((amount,), jnp.int32).at[sequence[jnp.where(places < fixed, places, shifted)]].set(jnp.asarray(tallies, jnp.int32))

    tallies = jnp.where(number % 4 == 0, named(heavy_load, number // 4), named(common, number - number // 4 - 1))
    mixed = jax.random.permutation(jax.random.fold_in(own, 3), amount)
    giver, taker = mixed[0:amount // 2 * 2:2], mixed[1:amount // 2 * 2:2]
    room = jnp.minimum(tallies[giver] - 1, most - tallies[taker]) // 2
    room = jnp.where((giver == sequence[0]) | (taker == sequence[0]) | (tallies[taker] == 0), 0, jnp.maximum(room, 0))
    shifted = jax.random.randint(jax.random.fold_in(own, 4), (amount // 2,), 0, 1 << 20) % (room + 1)
    tallies = tallies.at[giver].add(-shifted).at[taker].add(shifted)
    members = jnp.searchsorted(jnp.cumsum(tallies), jnp.arange(rows * top), side="right").astype(jnp.int32)
    listing = members.reshape(top, rows).T
    listing = listing[jax.random.permutation(jax.random.fold_in(own, 1), rows)]
    rotation = jax.random.randint(jax.random.fold_in(own, 2), (rows, 1), 0, top)
    return jnp.take_along_axis(listing, (jnp.arange(top)[None, :] + rotation) % top, axis=1)


def shares(count, total, bound, slope, full):
    weights = [(1 << 20) // math.isqrt(grade ** slope) + 1 for grade in range(1, count + 1)]
    largest = bound if full else min(bound, max(-(-total // count), total * weights[0] // sum(weights)))
    least = 1 if total - largest >= count - 1 else 0
    given, surplus = [largest] + [least] * (count - 1), total - largest - least * (count - 1)
    while surplus > 0:
        free = [i for i in range(1, count) if given[i] < largest] or [i for i in range(1, count) if given[i] < bound]
        whole, budget = sum([weights[i] for i in free]), surplus
        for i in free:
            more = min(bound - given[i], max(1, budget * weights[i] // whole), surplus)
            given[i] = given[i] + more
            surplus = surplus - more
    return np.array(given)


def scatter_about(stream_key, extent, scale, most, split=(), kind=jnp.bfloat16):
    gain = block_levels(stream_key, extent, split, -0.22, 0.18) if split else 1.0
    array = jax.random.normal(stream_key, extent, jnp.float32) * scale * gain
    return jnp.minimum(jnp.maximum(array, -most), most).astype(kind)


def setup_inputs(seed: int = 0) -> dict:
    keys = jax.random.split(jax.random.key(seed), 10)
    pressure_rhs = scatter_about(keys[0], (NX, NY, NZ), 1.0, 6.0, ((0, 8), (1, 4), (2, 4)), jnp.float32)
    shift_diag = jnp.clip(jnp.exp(math.log(0.3) - 2.7080503 * jax.random.uniform(keys[1], (NX, NY, NZ), jnp.float32) ** block_levels(keys[1], (NX, NY, NZ), ((0, 8), (1, 4), (2, 4)), -0.2, 0.2)), 0.02, 0.3)
    positions = scatter_about(keys[2], (3, POINTS), 1.0, 6.0, ((1, 128),), jnp.float32)
    normals = scatter_about(keys[3], (3, POINTS), 1.0, 6.0, ((1, 128),), jnp.float32)
    tension = jnp.clip(jnp.exp(math.log(3.0) - 2.3025851 * jax.random.uniform(keys[4], (POINTS,), jnp.float32) ** block_levels(keys[4], (POINTS,), ((0, 128),), -0.2, 0.2)), 0.3, 3.0)
    edge_weight = jnp.clip(jnp.exp(math.log(2.0) - 1.3862944 * jax.random.uniform(keys[5], (NEIGH, POINTS), jnp.float32) ** block_levels(keys[5], (NEIGH, POINTS), ((1, 128),), -0.2, 0.2)), 0.5, 2.0)
    owner_map_keys = jax.random.split(jax.random.fold_in(keys[6], 1), POINTS // PTS_DEV)
    owner_map_turns = jax.random.permutation(jax.random.fold_in(keys[6], 3), POINTS // PTS_DEV)
    owner_map = jax.vmap(lambda own, number: deal_out(jax.random.fold_in(keys[6], 2), own, number, PTS_DEV, DEVICES, 1, CAP, 2))(owner_map_keys, owner_map_turns).reshape((POINTS, 1))
    cell_map = plant(jax.random.randint(keys[7], (POINTS,), 0, CX * CY * CZ), jax.random.fold_in(keys[7], 1), 0, (CX * CY * CZ) - 1).astype(jnp.int32)
    connectivity = draw_connectivity(jax.random.fold_in(keys[9], 71), 0)
    return dict(pressure_rhs=pressure_rhs, shift_diag=shift_diag, positions=positions, normals=normals, tension=tension, edge_weight=edge_weight, owner_map=owner_map, cell_map=cell_map, connectivity=connectivity)


centre = 1.125
spread = 0.875


def operate(field, shift):
    padded = jnp.pad(field, 1)
    beside = padded[2:, 1:-1, 1:-1] + padded[:-2, 1:-1, 1:-1]
    beside = beside + padded[1:-1, 2:, 1:-1] + padded[1:-1, :-2, 1:-1]
    beside = beside + padded[1:-1, 1:-1, 2:] + padded[1:-1, 1:-1, :-2]
    return (6.0 + shift) * field - beside


def chebyshev(target, shift, start, sweeps):
    inverse = 1.0 / (6.0 + shift)
    ratio = centre / spread
    factor = 1.0 / ratio
    if start is None:
        update = inverse * target / centre
        answer = update
    else:
        update = inverse * (target - operate(start, shift)) / centre
        answer = start + update
    for sweep in range(1, sweeps):
        remain = inverse * (target - operate(answer, shift))
        factor_new = 1.0 / (2.0 * ratio - factor)
        update = factor_new * factor * update + (2.0 * factor_new / spread) * remain
        answer = answer + update
        factor = factor_new
    return answer


def blocks(field):
    nxh, nyh, nzh = field.shape[0] // 2, field.shape[1] // 2, field.shape[2] // 2
    return field.reshape(nxh, 2, nyh, 2, nzh, 2)


def reference(pressure_rhs, shift_diag, positions, normals, tension, edge_weight, owner_map, cell_map, connectivity):
    neighbours = positions[:, connectivity]
    surface_force = tension[None, :] * jnp.sum(edge_weight[None, :, :] * (neighbours - positions[:, None, :]), axis=1)
    jump = jnp.sum(surface_force * normals, axis=0)
    owner = owner_map[:, 0]
    ox = owner // (N_GY * N_GZ)
    oy = (owner // N_GZ) % N_GY
    oz = owner % N_GZ
    cx = cell_map // (CY * CZ)
    cy = (cell_map // CZ) % CY
    cz = cell_map % CZ
    forcing = pressure_rhs.at[ox * CX + cx, oy * CY + cy, oz * CZ + cz].add(jump)
    smooth = chebyshev(forcing, shift_diag, None, SMOOTH)
    remain = forcing - operate(smooth, shift_diag)
    coarse_rhs = 0.5 * jnp.sum(blocks(remain), axis=(1, 3, 5))
    coarse_shift = 4.0 * jnp.mean(blocks(shift_diag), axis=(1, 3, 5))
    coarse_fix = chebyshev(coarse_rhs, coarse_shift, None, COARSE_SMOOTH)
    spreadout = jnp.repeat(jnp.repeat(jnp.repeat(coarse_fix, 2, axis=0), 2, axis=1), 2, axis=2)
    pressure = chebyshev(forcing, shift_diag, smooth + spreadout, SMOOTH)
    return pressure, surface_force
```

```python
import jax
import jax.numpy as jnp
from jax import lax
from jax.experimental import pallas as pl
from jax.experimental.pallas import tpu as pltpu
from jax.sharding import PartitionSpec as P


HALO = 64
SMOOTH = 3
COARSE_SMOOTH = 4


centre = 1.125
spread = 0.875


def extended(value, sides, width):
    edges = {}
    for axis, dim in sides:
        devices, length = (lax.axis_size(axis), value.shape[dim])
        up = [(i, (i + 1) % devices) for i in range(devices - 1)]
        last = lax.slice_in_dim(value, length - width, length, axis=dim)
        initial = lax.slice_in_dim(value, 0, width, axis=dim)
        edges[dim] = (
            lax.ppermute(last, axis, up),
            lax.ppermute(initial, axis, [(b, a) for a, b in up]),
        )
    done = []
    for _, dim in sides:
        low, high = edges[dim]
        around = [(width, width) if d in done else (0, 0) for d in range(value.ndim)]
        value = jnp.concatenate([jnp.pad(low, around), value, jnp.pad(high, around)], axis=dim)
        done.append(dim)
    return value


def padded_2(cells, sides, width, closed):
    for axis, dim in sides:
        count = lax.axis_size(axis)
        ends = count if closed else count - 1
        head = lax.slice_in_dim(cells, 0, width, axis=dim)
        tail = lax.slice_in_dim(cells, cells.shape[dim] - width, cells.shape[dim], axis=dim)
        cells = jnp.concatenate(
            [
                lax.ppermute(tail, axis, [(i, (i + 1) % count) for i in range(ends)]),
                cells,
                lax.ppermute(head, axis, [((i + 1) % count, i) for i in range(ends)]),
            ],
            axis=dim,
        )
    return cells


def side_by_side(arrays, axis, split_dim, concat_dim, along):
    both = jnp.concatenate(arrays, axis=along)
    filled, at, outs = (
        lax.all_to_all(both, axis, split_axis=split_dim, concat_axis=concat_dim, tiled=True),
        0,
        [],
    )
    for a in arrays:
        outs.append(lax.slice_in_dim(filled, at, at + a.shape[along], axis=along))
        at += a.shape[along]
    return tuple(outs)


def stencil(padded, field, shift):
    beside = padded[2:, 1:-1, 1:-1] + padded[:-2, 1:-1, 1:-1]
    beside = beside + padded[1:-1, 2:, 1:-1] + padded[1:-1, :-2, 1:-1]
    beside = beside + padded[1:-1, 1:-1, 2:] + padded[1:-1, 1:-1, :-2]
    return (6.0 + shift) * field - beside


def coarse_apply(field, shift):
    padded = extended(field, (("gx", 0), ("gy", 1), ("gz", 2)), 1)
    return stencil(padded, field, shift)


def local_apply(field, shift):
    return stencil(jnp.pad(field, 1), field, shift)


def chebyshev(target, shift, start, sweeps, apply_fn, inside):
    inverse = 1.0 / (6.0 + shift)
    ratio = centre / spread
    factor = 1.0 / ratio
    if start is None:
        update = inverse * target / centre
        answer = update
    else:
        update = inverse * (target - apply_fn(start, shift)) / centre
        update = update * inside
        answer = start + update
    for sweep in range(1, sweeps):
        remain = inverse * (target - apply_fn(answer, shift))
        if inside is not None:
            remain = remain * inside
        factor_new = 1.0 / (2.0 * ratio - factor)
        update = factor_new * factor * update + 2.0 * factor_new / spread * remain
        answer = answer + update
        factor = factor_new
    return answer


def domain_mask(shape, width):
    places = (lax.axis_index("gx"), lax.axis_index("gy"), lax.axis_index("gz"))
    counts = (lax.axis_size("gx"), lax.axis_size("gy"), lax.axis_size("gz"))
    factors = []
    for which in range(3):
        length = shape[which]
        where = places[which] * length - width + jnp.arange(length + 2 * width, dtype=jnp.int32)
        factors.append(((where >= 0) & (where < length * counts[which])).astype(jnp.float32))
    return factors[0][:, None, None] * factors[1][None, :, None] * factors[2][None, None, :]


def interior(field, width):
    return field[width:-width, width:-width, width:-width]


def blocks(field):
    return field.reshape(field.shape[0] // 2, 2, field.shape[1] // 2, 2, field.shape[2] // 2, 2)


LANES = 128
BIG = 524288.0
GROUP_ROWS = 80
CELL_BITS = 18


def permute(value, lane_xor, sub_xor):
    if sub_xor:
        where = lax.broadcasted_iota(jnp.int32, value.shape, 0) ^ sub_xor
        value = pick(value, where, 0)
    if lane_xor:
        where = lax.broadcasted_iota(jnp.int32, value.shape, 1) ^ lane_xor
        value = pick(value, where, 1)
    return value


def pick(value, where, axis):
    numbers = lax.GatherDimensionNumbers(
        offset_dims=(),
        collapsed_slice_dims=(axis,),
        start_index_map=(axis,),
        operand_batching_dims=(1 - axis,),
        start_indices_batching_dims=(1 - axis,),
    )
    return lax.gather(
        value,
        where[:, :, None],
        numbers,
        (1, 1),
        mode=lax.GatherScatterMode.PROMISE_IN_BOUNDS,
    )


def exchange(keys, loads, places, bits, top):
    lane_xor = sub_xor = row_xor = 0
    for bit in bits:
        kind, amount = places[bit]
        lane_xor |= amount if kind == "l" else 0
        sub_xor |= amount if kind == "s" else 0
        row_xor |= amount if kind == "v" else 0
    top_kind, top_amount = places[top]
    count = len(keys)
    new_keys, new_loads = [None] * count, [None] * count
    if top_kind == "v":
        for a in range(count):
            if a & top_amount:
                continue
            b = a ^ row_xor
            low, high, low_load, high_load = keys[a], keys[b], loads[a], loads[b]
            stored = b
            if lane_xor or sub_xor:
                high = permute(high, lane_xor, sub_xor)
                high_load = permute(high_load, lane_xor, sub_xor)
                stored = a | top_amount
            swap = low > high
            new_keys[a] = jnp.minimum(low, high)
            new_keys[stored] = jnp.maximum(low, high)
            new_loads[a] = jnp.where(swap, high_load, low_load)
            new_loads[stored] = jnp.where(swap, low_load, high_load)
        return new_keys, new_loads
    axis = 1 if top_kind == "l" else 0
    upper = (lax.broadcasted_iota(jnp.int32, keys[0].shape, axis) & top_amount) != 0
    for a in range(count):
        b = a ^ row_xor
        other = permute(keys[b], lane_xor, sub_xor)
        other_load = permute(loads[b], lane_xor, sub_xor)
        best = jnp.where(upper, jnp.maximum(keys[a], other), jnp.minimum(keys[a], other))
        new_keys[a] = best
        new_loads[a] = jnp.where(best == keys[a], loads[a], other_load)
    return new_keys, new_loads


def merge_levels(keys, loads, places, first, last):
    for level in range(first, last + 1):
        keys, loads = exchange(keys, loads, places, range(level + 1), level)
        for bit in reversed(range(level)):
            keys, loads = exchange(keys, loads, places, (bit,), bit)
    return keys, loads


def surface_kernel(
    begin_ref, low_ref, high_ref, positions_ref, normals_ref, tension_ref, weight_ref,
    owner_ref, cell_ref, connect_ref, force_ref, packed_ref,
    wide, jumps, turned, lists, counted, counted_scalar, sem,
):
    npoint = positions_ref.shape[1]
    nrow = npoint // LANES
    nowner = packed_ref.shape[0]
    begin, total = begin_ref[0], begin_ref[1]
    half = lax.broadcasted_iota(jnp.int32, (3, LANES), 1) < HALO
    before = pltpu.roll(low_ref[...], HALO, 1)
    for row in range(nrow + 1):
        source = high_ref[...] if row == nrow else positions_ref[:, row * LANES : (row + 1) * LANES]
        after = pltpu.roll(source, HALO, 1)
        wide[0:3, row * LANES : (row + 1) * LANES] = jnp.where(half, before, after)
        before = after

    def one_row(row, carry):
        at = pl.multiple_of(row * LANES, LANES)
        here, there = pl.ds(at, LANES), pl.ds(at + LANES, LANES)
        blank = jnp.zeros((2, LANES), jnp.int32)
        index = jnp.concatenate([connect_ref[:, here], blank], axis=0)
        index = ((index - begin + HALO) & (total - 1)) - at
        weight = jnp.concatenate([weight_ref[:, here], blank.astype(jnp.float32)], axis=0)
        second = index >= LANES
        index = index & (LANES - 1)
        strength = tension_ref[pl.ds(row, 1), :]
        jump = jnp.zeros((1, LANES), jnp.float32)
        for axis in range(3):
            lower = jnp.broadcast_to(wide[axis : axis + 1, here], (8, LANES))
            upper = jnp.broadcast_to(wide[axis : axis + 1, there], (8, LANES))
            taken = jnp.where(second, pick(upper, index, 1), pick(lower, index, 1))
            pulled = weight * (taken - positions_ref[axis : axis + 1, here])
            force = strength * jnp.sum(pulled, axis=0, keepdims=True)
            force_ref[axis : axis + 1, here] = force
            jump = jump + force * normals_ref[axis : axis + 1, here]
        jumps[pl.ds(row, 1), :] = jump
        return carry

    lax.fori_loop(0, nrow, one_row, 0, unroll=8)

    ranks = lax.broadcasted_iota(jnp.int32, (nowner, LANES), 0)

    def count_row(row, below):
        names = owner_ref[pl.ds(row, 1), :]
        return below + jnp.where(names < ranks, 1, 0)

    below = lax.fori_loop(0, nrow, count_row, jnp.zeros((nowner, LANES), jnp.int32), unroll=4)
    starts = jnp.sum(below.astype(jnp.float32), axis=1, keepdims=True)
    turned[...] = jnp.broadcast_to(starts, (nowner, LANES))
    counted[...] = jnp.transpose(turned[...])[0:8, :].astype(jnp.int32)
    fetch = pltpu.make_async_copy(counted, counted_scalar, sem)

    keys, loads = [], []
    for tile in range(nrow // 8):
        rows = slice(8 * tile, 8 * tile + 8)
        cell = cell_ref[rows, :]
        cell = ((cell & 384) << 9) | ((cell >> 9) << 7) | (cell & 127)
        keys.append((owner_ref[rows, :] << CELL_BITS) | cell)
        loads.append(jumps[rows, :])
    fetch.start()
    places = [("v", 1), ("v", 2), ("v", 4), ("s", 1), ("s", 2), ("s", 4)]
    places += [("l", 1 << bit) for bit in range(7)]
    keys, loads = merge_levels(keys, loads, places, 0, 12)
    for which, arrays in ((0, keys), (1, loads)):
        for tile in range(8):
            value = arrays[tile]
            if which == 0:
                value = (value & ((1 << CELL_BITS) - 1)).astype(jnp.float32)
            turned[pl.ds(tile, 8, stride=8), :] = value
        flipped = jnp.transpose(turned[...])
        turned[...] = flipped
        even = turned[pl.ds(0, 64, stride=2), :]
        odd = pltpu.roll(turned[pl.ds(1, 64, stride=2), :], 64, 1)
        lane = lax.broadcasted_iota(jnp.int32, (64, LANES), 1)
        lists[pl.ds(which, 64, stride=2), :] = jnp.where(lane < 64, even, odd)
    lists[128:144, :] = jnp.zeros((16, LANES), jnp.float32)
    fetch.wait()

    lane = lax.broadcasted_iota(jnp.int32, (8, LANES), 1)
    line = lax.broadcasted_iota(jnp.int32, (8, LANES), 0)
    slot = lane + LANES * (line >> 1)
    filler = jnp.where((line & 1) == 0, BIG, 0.0).astype(jnp.float32)

    def one_owner(owner, carry):
        start = counted_scalar[0, owner]
        following = jnp.where(owner == nowner - 1, npoint, counted_scalar[0, jnp.minimum(owner + 1, nowner - 1)])
        shift = start & (LANES - 1)
        block = lists[pl.ds((start >> 7) * 2, 8), :]
        block = pltpu.roll(block, (LANES - shift) & (LANES - 1), 1)
        block = jnp.where(lane < LANES - shift, block, pltpu.roll(block, 6, 0))
        block = jnp.where(slot < following - start, block, filler)
        packed_ref[owner] = block[0:4, :]
        return carry

    lax.fori_loop(0, nowner, one_owner, 0, unroll=8)


def spread_kernel(
    got_ref, rhs_ref, forcing_ref,
    keys_scratch, loads_scratch, grid, turned, bounds, bounds_scalar, work, sem,
):
    nsender = got_ref.shape[0] // 4
    ngroup = nsender // 32
    places = [("l", 1 << bit) for bit in range(7)] + [("v", 1), ("v", 2), ("v", 4)]
    places += [("s", 1), ("s", 2), ("s", 4)]

    def zero(step, carry):
        grid[pl.ds(pl.multiple_of(step * 64, 64), 64), :] = jnp.zeros((64, LANES), jnp.float32)
        return carry

    lax.fori_loop(0, grid.shape[0] // 64, zero, 0)

    def one_group(group):
        keys, loads = [], []
        for quarter in range(4):
            for side in range(2):
                first = (group * 32 + quarter * 8) * 4 + 2 * side
                keys.append(got_ref[pl.ds(first, 8, stride=4), :])
                loads.append(got_ref[pl.ds(first + 1, 8, stride=4), :])
        keys, loads = merge_levels(keys, loads, places, 8, 12)
        for quarter in range(4):
            rows = pl.ds(group * 32 + quarter, 8, stride=4)
            last = jnp.full((8, 1), -1, jnp.int32)
            base = None
            for side in range(2):
                key = keys[2 * quarter + side]
                columns = slice(side * LANES, (side + 1) * LANES)
                cell = key.astype(jnp.int32)
                keys_scratch[side, rows, :] = cell
                loads_scratch[side, rows, :] = loads[2 * quarter + side]
                inside = key < BIG
                line = (cell >> 7).astype(jnp.float32)
                top = jnp.max(jnp.where(inside, line, -1.0), axis=1, keepdims=True)
                last = jnp.maximum(last, top.astype(jnp.int32))
                if side == 0:
                    base = jnp.min(line, axis=1, keepdims=True).astype(jnp.int32) & -8
            repeats = jnp.where(last < 0, 0, (((last - base) * 52429) >> 22) + 1)
            pair = jnp.where(last < 0, 0, base) * 32 + repeats
            turned[rows, :] = jnp.broadcast_to(pair.astype(jnp.float32), (8, LANES))

    for group in range(ngroup):
        one_group(group)
    bounds[...] = jnp.transpose(turned[...])[0:8, :].astype(jnp.int32)
    fetch = pltpu.make_async_copy(bounds, bounds_scalar, sem)
    fetch.start()
    fetch.wait()

    def list_chunk(chunk, filled):
        pair = bounds_scalar[0, chunk]
        base = pair >> 5

        def list_piece(piece, filled):
            work[filled] = (chunk << 12) | (base + piece * GROUP_ROWS)
            return filled + 1

        return lax.fori_loop(0, pair & 31, list_piece, filled)

    filled = lax.fori_loop(0, 32 * ngroup, list_chunk, 0)
    for extra in range(BATCH):
        work[filled + extra] = 2048
    lines = lax.broadcasted_iota(jnp.int32, (GROUP_ROWS, 2 * LANES), 0)
    columns = lax.broadcasted_iota(jnp.int32, (LANES, 2 * LANES), 0)

    def one_batch(batch, carry):
        sums, bases = [], []
        for piece in range(BATCH):
            item = work[batch * BATCH + piece]
            chunk = item >> 12
            base = pl.multiple_of(item & 4095, 8)
            cell = jnp.concatenate([keys_scratch[side, pl.ds(chunk, 1), :] for side in range(2)], axis=1)
            load = jnp.concatenate([loads_scratch[side, pl.ds(chunk, 1), :] for side in range(2)], axis=1)
            coarse = load.astype(jnp.bfloat16).astype(jnp.float32)
            here = ((cell >> 7) - base) == lines
            left = jnp.concatenate(
                [
                    jnp.where(here, coarse, 0.0).astype(jnp.bfloat16),
                    jnp.where(here, load - coarse, 0.0).astype(jnp.bfloat16),
                ],
                axis=0,
            )
            right = jnp.where((cell & (LANES - 1)) == columns, 1.0, 0.0).astype(jnp.bfloat16)
            both = lax.dot_general(
                left, right, (((1,), (1,)), ((), ())), preferred_element_type=jnp.float32
            )
            sums.append(both[:GROUP_ROWS] + both[GROUP_ROWS:])
            bases.append(base)
        for total, base in zip(sums, bases):
            grid[pl.ds(base, GROUP_ROWS), :] += total
        return carry

    lax.fori_loop(0, (filled + BATCH - 1) // BATCH, one_batch, 0)

    shape = forcing_ref.shape
    for plane in range(shape[0]):
        for part in range(shape[2] // LANES):
            columns = slice(part * LANES, (part + 1) * LANES)
            first = (part * shape[0] + plane) * shape[1]
            forcing_ref[plane, :, columns] = rhs_ref[plane, :, columns] + grid[first : first + shape[1], :]


BATCH = 8


def surface_and_pack(begin, low, high, positions, normals, tension, edge_weight, owners, cells, connectivity, nowner):
    vmem = pl.BlockSpec(memory_space=pltpu.VMEM)
    return pl.pallas_call(
        surface_kernel,
        name="surface",
        out_shape=(
            jax.ShapeDtypeStruct(positions.shape, jnp.float32),
            jax.ShapeDtypeStruct((nowner, 4, LANES), jnp.float32),
        ),
        in_specs=[pl.BlockSpec(memory_space=pltpu.SMEM)] + [vmem] * 9,
        out_specs=(vmem, vmem),
        scratch_shapes=[
            pltpu.VMEM((8, positions.shape[1] + LANES), jnp.float32),
            pltpu.VMEM((positions.shape[1] // LANES, LANES), jnp.float32),
            pltpu.VMEM((128, LANES), jnp.float32),
            pltpu.VMEM((144, LANES), jnp.float32),
            pltpu.VMEM((8, LANES), jnp.int32),
            pltpu.SMEM((8, LANES), jnp.int32),
            pltpu.SemaphoreType.DMA,
        ],
        compiler_params=pltpu.CompilerParams(vmem_limit_bytes=32 * 1024 * 1024),
    )(begin, low, high, positions, normals, tension, edge_weight, owners, cells, connectivity)


def spread_cells(got, pressure_rhs):
    vmem = pl.BlockSpec(memory_space=pltpu.VMEM)
    return pl.pallas_call(
        spread_kernel,
        name="spread",
        out_shape=jax.ShapeDtypeStruct(pressure_rhs.shape, jnp.float32),
        in_specs=[vmem, vmem],
        out_specs=vmem,
        scratch_shapes=[
            pltpu.VMEM((2, 128, LANES), jnp.int32),
            pltpu.VMEM((2, 128, LANES), jnp.float32),
            pltpu.VMEM((2048 + 128, LANES), jnp.float32),
            pltpu.VMEM((128, LANES), jnp.float32),
            pltpu.VMEM((8, LANES), jnp.int32),
            pltpu.SMEM((8, LANES), jnp.int32),
            pltpu.SMEM((512,), jnp.int32),
            pltpu.SemaphoreType.DMA,
        ],
        compiler_params=pltpu.CompilerParams(vmem_limit_bytes=32 * 1024 * 1024),
    )(got, pressure_rhs)


def body(
    pressure_rhs,
    shift_diag,
    positions,
    normals,
    tension,
    edge_weight,
    owner_map,
    cell_map,
    connectivity,
):
    every = ("gx", "gy", "gz")
    npoint = positions.shape[1]
    ndevice = lax.axis_size(every)
    begin = lax.axis_index(every) * npoint
    up = [(i, (i + 1) % ndevice) for i in range(ndevice)]
    low = lax.ppermute(positions[:, npoint - LANES :], every, up)
    high = lax.ppermute(positions[:, :LANES], every, [(b, a) for a, b in up])
    surface_force, packed = surface_and_pack(
        jnp.stack([begin, npoint * ndevice]).astype(jnp.int32),
        low,
        high,
        positions,
        normals,
        tension.reshape(npoint // LANES, LANES),
        edge_weight,
        owner_map.reshape(npoint // LANES, LANES),
        cell_map.reshape(npoint // LANES, LANES),
        connectivity,
        ndevice,
    )
    got = lax.all_to_all(packed, every, split_axis=0, concat_axis=0, tiled=True)
    forcing = spread_cells(got.reshape(4 * ndevice, LANES), pressure_rhs)
    shape = pressure_rhs.shape
    coarse_shift = 4.0 * jnp.mean(blocks(shift_diag), axis=(1, 3, 5))
    width = SMOOTH
    inside = domain_mask(shape, width)
    forcing_wide, shift_wide = (
        padded_2(forcing, (("gx", 0), ("gy", 1), ("gz", 2)), width, False),
        padded_2(shift_diag, (("gx", 0), ("gy", 1), ("gz", 2)), width, False),
    )
    smooth_wide = chebyshev(forcing_wide, shift_wide, None, SMOOTH, local_apply, inside)
    remain = interior(forcing_wide - local_apply(smooth_wide, shift_wide), width)
    smooth = interior(smooth_wide, width)
    coarse_rhs = 0.5 * jnp.sum(blocks(remain), axis=(1, 3, 5))
    coarse_fix = chebyshev(coarse_rhs, coarse_shift, None, COARSE_SMOOTH, coarse_apply, None)
    spreadout = jnp.broadcast_to(
        coarse_fix[:, None, :, None, :, None], blocks(shift_diag).shape
    ).reshape(shape)
    start_wide = padded_2(smooth + spreadout, (("gx", 0), ("gy", 1), ("gz", 2)), width, False)
    pressure = interior(
        chebyshev(forcing_wide, shift_wide, start_wide, SMOOTH, local_apply, inside), width
    )
    return (pressure, surface_force)


def solution(mesh):
    return jax.shard_map(
        body,
        mesh=mesh,
        in_specs=(
            P("gx", "gy", "gz"),
            P("gx", "gy", "gz"),
            P(None, ("gx", "gy", "gz")),
            P(None, ("gx", "gy", "gz")),
            P(("gx", "gy", "gz")),
            P(None, ("gx", "gy", "gz")),
            P(("gx", "gy", "gz"), None),
            P(("gx", "gy", "gz")),
            P(None, ("gx", "gy", "gz")),
        ),
        out_specs=(P("gx", "gy", "gz"), P(None, ("gx", "gy", "gz"))),
        check_vma=False,
    )
```

```python
import functools
import jax
import jax.numpy as jnp
from jax import lax
from jax.experimental import pallas as pl
from jax.experimental.pallas import tpu as pltpu
from jax.sharding import PartitionSpec as P

HALO = 64
SMOOTH = 3
COARSE_SMOOTH = 4


centre = 1.125
spread = 0.875


LANES = 128
BIG = 524288.0
GROUP_ROWS = 80
CELL_BITS = 18


def permute(value, lane_xor, sub_xor):
    if sub_xor:
        where = lax.broadcasted_iota(jnp.int32, value.shape, 0) ^ sub_xor
        value = pick(value, where, 0)
    if lane_xor:
        where = lax.broadcasted_iota(jnp.int32, value.shape, 1) ^ lane_xor
        value = pick(value, where, 1)
    return value


def pick(value, where, axis):
    numbers = lax.GatherDimensionNumbers(
        offset_dims=(),
        collapsed_slice_dims=(axis,),
        start_index_map=(axis,),
        operand_batching_dims=(1 - axis,),
        start_indices_batching_dims=(1 - axis,),
    )
    return lax.gather(
        value,
        where[:, :, None],
        numbers,
        (1, 1),
        mode=lax.GatherScatterMode.PROMISE_IN_BOUNDS,
    )


def exchange(keys, loads, places, bits, top):
    lane_xor = sub_xor = row_xor = 0
    for bit in bits:
        kind, amount = places[bit]
        lane_xor |= amount if kind == "l" else 0
        sub_xor |= amount if kind == "s" else 0
        row_xor |= amount if kind == "v" else 0
    top_kind, top_amount = places[top]
    count = len(keys)
    new_keys, new_loads = [None] * count, [None] * count
    if top_kind == "v":
        for a in range(count):
            if a & top_amount:
                continue
            b = a ^ row_xor
            low, high, low_load, high_load = keys[a], keys[b], loads[a], loads[b]
            stored = b
            if lane_xor or sub_xor:
                high = permute(high, lane_xor, sub_xor)
                high_load = permute(high_load, lane_xor, sub_xor)
                stored = a | top_amount
            swap = low > high
            new_keys[a] = jnp.minimum(low, high)
            new_keys[stored] = jnp.maximum(low, high)
            new_loads[a] = jnp.where(swap, high_load, low_load)
            new_loads[stored] = jnp.where(swap, low_load, high_load)
        return new_keys, new_loads
    axis = 1 if top_kind == "l" else 0
    upper = (lax.broadcasted_iota(jnp.int32, keys[0].shape, axis) & top_amount) != 0
    for a in range(count):
        b = a ^ row_xor
        other = permute(keys[b], lane_xor, sub_xor)
        other_load = permute(loads[b], lane_xor, sub_xor)
        best = jnp.where(upper, jnp.maximum(keys[a], other), jnp.minimum(keys[a], other))
        new_keys[a] = best
        new_loads[a] = jnp.where(best == keys[a], loads[a], other_load)
    return new_keys, new_loads


def merge_levels(keys, loads, places, first, last):
    for level in range(first, last + 1):
        keys, loads = exchange(keys, loads, places, range(level + 1), level)
        for bit in reversed(range(level)):
            keys, loads = exchange(keys, loads, places, (bit,), bit)
    return keys, loads


def surface_kernel(
    begin_ref, low_ref, high_ref, positions_ref, normals_ref, tension_ref, weight_ref,
    owner_ref, cell_ref, connect_ref, force_ref, packed_ref,
    wide, jumps, turned, lists, counted, counted_scalar, sem,
):
    npoint = positions_ref.shape[1]
    nrow = npoint // LANES
    nowner = packed_ref.shape[0]
    begin, total = begin_ref[0], begin_ref[1]
    half = lax.broadcasted_iota(jnp.int32, (3, LANES), 1) < HALO
    before = pltpu.roll(low_ref[...], HALO, 1)
    for row in range(nrow + 1):
        source = high_ref[...] if row == nrow else positions_ref[:, row * LANES : (row + 1) * LANES]
        after = pltpu.roll(source, HALO, 1)
        wide[0:3, row * LANES : (row + 1) * LANES] = jnp.where(half, before, after)
        before = after

    def one_row(row, carry):
        at = pl.multiple_of(row * LANES, LANES)
        here, there = pl.ds(at, LANES), pl.ds(at + LANES, LANES)
        blank = jnp.zeros((2, LANES), jnp.int32)
        index = jnp.concatenate([connect_ref[:, here], blank], axis=0)
        index = ((index - begin + HALO) & (total - 1)) - at
        weight = jnp.concatenate([weight_ref[:, here], blank.astype(jnp.float32)], axis=0)
        second = index >= LANES
        index = index & (LANES - 1)
        strength = tension_ref[pl.ds(row, 1), :]
        jump = jnp.zeros((1, LANES), jnp.float32)
        for axis in range(3):
            lower = jnp.broadcast_to(wide[axis : axis + 1, here], (8, LANES))
            upper = jnp.broadcast_to(wide[axis : axis + 1, there], (8, LANES))
            taken = jnp.where(second, pick(upper, index, 1), pick(lower, index, 1))
            pulled = weight * (taken - positions_ref[axis : axis + 1, here])
            force = strength * jnp.sum(pulled, axis=0, keepdims=True)
            force_ref[axis : axis + 1, here] = force
            jump = jump + force * normals_ref[axis : axis + 1, here]
        jumps[pl.ds(row, 1), :] = jump
        return carry

    lax.fori_loop(0, nrow, one_row, 0, unroll=8)

    ranks = lax.broadcasted_iota(jnp.int32, (nowner, LANES), 0)

    def count_row(row, below):
        names = owner_ref[pl.ds(row, 1), :]
        return below + jnp.where(names < ranks, 1, 0)

    below = lax.fori_loop(0, nrow, count_row, jnp.zeros((nowner, LANES), jnp.int32), unroll=4)
    starts = jnp.sum(below.astype(jnp.float32), axis=1, keepdims=True)
    turned[...] = jnp.broadcast_to(starts, (nowner, LANES))
    counted[...] = jnp.transpose(turned[...])[0:8, :].astype(jnp.int32)
    fetch = pltpu.make_async_copy(counted, counted_scalar, sem)

    keys, loads = [], []
    for tile in range(nrow // 8):
        rows = slice(8 * tile, 8 * tile + 8)
        cell = cell_ref[rows, :]
        cell = ((cell & 384) << 9) | ((cell >> 9) << 7) | (cell & 127)
        keys.append((owner_ref[rows, :] << CELL_BITS) | cell)
        loads.append(jumps[rows, :])
    fetch.start()
    places = [("v", 1), ("v", 2), ("v", 4), ("s", 1), ("s", 2), ("s", 4)]
    places += [("l", 1 << bit) for bit in range(7)]
    keys, loads = merge_levels(keys, loads, places, 0, 12)
    for which, arrays in ((0, keys), (1, loads)):
        for tile in range(8):
            value = arrays[tile]
            if which == 0:
                value = (value & ((1 << CELL_BITS) - 1)).astype(jnp.float32)
            turned[pl.ds(tile, 8, stride=8), :] = value
        flipped = jnp.transpose(turned[...])
        turned[...] = flipped
        even = turned[pl.ds(0, 64, stride=2), :]
        odd = pltpu.roll(turned[pl.ds(1, 64, stride=2), :], 64, 1)
        lane = lax.broadcasted_iota(jnp.int32, (64, LANES), 1)
        lists[pl.ds(which, 64, stride=2), :] = jnp.where(lane < 64, even, odd)
    lists[128:144, :] = jnp.zeros((16, LANES), jnp.float32)
    fetch.wait()

    lane = lax.broadcasted_iota(jnp.int32, (8, LANES), 1)
    line = lax.broadcasted_iota(jnp.int32, (8, LANES), 0)
    slot = lane + LANES * (line >> 1)
    filler = jnp.where((line & 1) == 0, BIG, 0.0).astype(jnp.float32)

    def one_owner(owner, carry):
        start = counted_scalar[0, owner]
        following = jnp.where(owner == nowner - 1, npoint, counted_scalar[0, jnp.minimum(owner + 1, nowner - 1)])
        shift = start & (LANES - 1)
        block = lists[pl.ds((start >> 7) * 2, 8), :]
        block = pltpu.roll(block, (LANES - shift) & (LANES - 1), 1)
        block = jnp.where(lane < LANES - shift, block, pltpu.roll(block, 6, 0))
        block = jnp.where(slot < following - start, block, filler)
        packed_ref[owner] = block[0:4, :]
        return carry

    lax.fori_loop(0, nowner, one_owner, 0, unroll=8)


def spread_kernel(
    got_ref, rhs_ref, forcing_ref,
    keys_scratch, loads_scratch, grid, turned, bounds, bounds_scalar, work, sem,
):
    nsender = got_ref.shape[0] // 4
    ngroup = nsender // 32
    places = [("l", 1 << bit) for bit in range(7)] + [("v", 1), ("v", 2), ("v", 4)]
    places += [("s", 1), ("s", 2), ("s", 4)]

    def zero(step, carry):
        grid[pl.ds(pl.multiple_of(step * 64, 64), 64), :] = jnp.zeros((64, LANES), jnp.float32)
        return carry

    lax.fori_loop(0, grid.shape[0] // 64, zero, 0)

    def one_group(group):
        keys, loads = [], []
        for quarter in range(4):
            for side in range(2):
                first = (group * 32 + quarter * 8) * 4 + 2 * side
                keys.append(got_ref[pl.ds(first, 8, stride=4), :])
                loads.append(got_ref[pl.ds(first + 1, 8, stride=4), :])
        keys, loads = merge_levels(keys, loads, places, 8, 12)
        for quarter in range(4):
            rows = pl.ds(group * 32 + quarter, 8, stride=4)
            last = jnp.full((8, 1), -1, jnp.int32)
            base = None
            for side in range(2):
                key = keys[2 * quarter + side]
                columns = slice(side * LANES, (side + 1) * LANES)
                cell = key.astype(jnp.int32)
                keys_scratch[side, rows, :] = cell
                loads_scratch[side, rows, :] = loads[2 * quarter + side]
                inside = key < BIG
                line = (cell >> 7).astype(jnp.float32)
                top = jnp.max(jnp.where(inside, line, -1.0), axis=1, keepdims=True)
                last = jnp.maximum(last, top.astype(jnp.int32))
                if side == 0:
                    base = jnp.min(line, axis=1, keepdims=True).astype(jnp.int32) & -8
            repeats = jnp.where(last < 0, 0, (((last - base) * 52429) >> 22) + 1)
            pair = jnp.where(last < 0, 0, base) * 32 + repeats
            turned[rows, :] = jnp.broadcast_to(pair.astype(jnp.float32), (8, LANES))

    for group in range(ngroup):
        one_group(group)
    bounds[...] = jnp.transpose(turned[...])[0:8, :].astype(jnp.int32)
    fetch = pltpu.make_async_copy(bounds, bounds_scalar, sem)
    fetch.start()
    fetch.wait()

    def list_chunk(chunk, filled):
        pair = bounds_scalar[0, chunk]
        base = pair >> 5

        def list_piece(piece, filled):
            work[filled] = (chunk << 12) | (base + piece * GROUP_ROWS)
            return filled + 1

        return lax.fori_loop(0, pair & 31, list_piece, filled)

    filled = lax.fori_loop(0, 32 * ngroup, list_chunk, 0)
    for extra in range(BATCH):
        work[filled + extra] = 2048
    lines = lax.broadcasted_iota(jnp.int32, (GROUP_ROWS, 2 * LANES), 0)
    columns = lax.broadcasted_iota(jnp.int32, (LANES, 2 * LANES), 0)

    def one_batch(batch, carry):
        sums, bases = [], []
        for piece in range(BATCH):
            item = work[batch * BATCH + piece]
            chunk = item >> 12
            base = pl.multiple_of(item & 4095, 8)
            cell = jnp.concatenate([keys_scratch[side, pl.ds(chunk, 1), :] for side in range(2)], axis=1)
            load = jnp.concatenate([loads_scratch[side, pl.ds(chunk, 1), :] for side in range(2)], axis=1)
            coarse = load.astype(jnp.bfloat16).astype(jnp.float32)
            here = ((cell >> 7) - base) == lines
            left = jnp.concatenate(
                [
                    jnp.where(here, coarse, 0.0).astype(jnp.bfloat16),
                    jnp.where(here, load - coarse, 0.0).astype(jnp.bfloat16),
                ],
                axis=0,
            )
            right = jnp.where((cell & (LANES - 1)) == columns, 1.0, 0.0).astype(jnp.bfloat16)
            both = lax.dot_general(
                left, right, (((1,), (1,)), ((), ())), preferred_element_type=jnp.float32
            )
            sums.append(both[:GROUP_ROWS] + both[GROUP_ROWS:])
            bases.append(base)
        for total, base in zip(sums, bases):
            grid[pl.ds(base, GROUP_ROWS), :] += total
        return carry

    lax.fori_loop(0, (filled + BATCH - 1) // BATCH, one_batch, 0)

    shape = forcing_ref.shape
    for plane in range(shape[0]):
        for part in range(shape[2] // LANES):
            columns = slice(part * LANES, (part + 1) * LANES)
            first = (part * shape[0] + plane) * shape[1]
            forcing_ref[plane, :, columns] = rhs_ref[plane, :, columns] + grid[first : first + shape[1], :]


BATCH = 8


def surface_and_pack(begin, low, high, positions, normals, tension, edge_weight, owners, cells, connectivity, nowner):
    vmem = pl.BlockSpec(memory_space=pltpu.VMEM)
    return pl.pallas_call(
        surface_kernel,
        name="surface",
        out_shape=(
            jax.ShapeDtypeStruct(positions.shape, jnp.float32),
            jax.ShapeDtypeStruct((nowner, 4, LANES), jnp.float32),
        ),
        in_specs=[pl.BlockSpec(memory_space=pltpu.SMEM)] + [vmem] * 9,
        out_specs=(vmem, vmem),
        scratch_shapes=[
            pltpu.VMEM((8, positions.shape[1] + LANES), jnp.float32),
            pltpu.VMEM((positions.shape[1] // LANES, LANES), jnp.float32),
            pltpu.VMEM((128, LANES), jnp.float32),
            pltpu.VMEM((144, LANES), jnp.float32),
            pltpu.VMEM((8, LANES), jnp.int32),
            pltpu.SMEM((8, LANES), jnp.int32),
            pltpu.SemaphoreType.DMA,
        ],
        compiler_params=pltpu.CompilerParams(vmem_limit_bytes=32 * 1024 * 1024),
    )(begin, low, high, positions, normals, tension, edge_weight, owners, cells, connectivity)


def spread_cells(got, pressure_rhs):
    vmem = pl.BlockSpec(memory_space=pltpu.VMEM)
    return pl.pallas_call(
        spread_kernel,
        name="spread",
        out_shape=jax.ShapeDtypeStruct(pressure_rhs.shape, jnp.float32),
        in_specs=[vmem, vmem],
        out_specs=vmem,
        scratch_shapes=[
            pltpu.VMEM((2, 128, LANES), jnp.int32),
            pltpu.VMEM((2, 128, LANES), jnp.float32),
            pltpu.VMEM((2048 + 128, LANES), jnp.float32),
            pltpu.VMEM((128, LANES), jnp.float32),
            pltpu.VMEM((8, LANES), jnp.int32),
            pltpu.SMEM((8, LANES), jnp.int32),
            pltpu.SMEM((512,), jnp.int32),
            pltpu.SemaphoreType.DMA,
        ],
        compiler_params=pltpu.CompilerParams(vmem_limit_bytes=32 * 1024 * 1024),
    )(got, pressure_rhs)


AXES = ("gx", "gy", "gz")


def halo_copies(sides, slot, send_sems, recv_sems):
    copies = []
    for which, (axis, step, source, target) in enumerate(sides):
        here = lax.axis_index(axis)
        there = here + step
        back = here - step
        size = lax.axis_size(axis)
        copy = pltpu.make_async_remote_copy(
            src_ref=source,
            dst_ref=target,
            send_sem=send_sems.at[slot, which],
            recv_sem=recv_sems.at[slot, which],
            device_id={axis: there},
            device_id_type=pl.DeviceIdType.MESH,
        )
        copies.append((copy, (there >= 0) & (there < size), (back >= 0) & (back < size)))
    return copies


def cycle_kernel(
    plane_rows, forcing_ref, shift_ref, pressure_ref,
    wide_a, wide_b, coarse_a, coarse_b, inverse, update, coarse_rhs, coarse_inverse, coarse_update,
    rows_out, rows_in, columns_out, columns_in, send_sems, recv_sems,
):
    width = forcing_ref.shape[1]
    nplane = forcing_ref.shape[0] // plane_rows
    ncoarse = nplane // 2
    tiles = plane_rows // 8
    wide, coarse = (wide_a, wide_b), (coarse_a, coarse_b)
    blank = jnp.zeros((plane_rows, width), jnp.float32)
    for slot in range(2):
        wide[slot][0:plane_rows, :] = blank
        wide[slot][(nplane + 1) * plane_rows : (nplane + 2) * plane_rows, :] = blank
        coarse[slot][0:plane_rows, :] = blank
        coarse[slot][(ncoarse + 1) * plane_rows : (ncoarse + 2) * plane_rows, :] = blank
        for side in range(2):
            rows_in[slot, side] = jnp.zeros(rows_in.shape[2:], jnp.float32)
            columns_in[slot, side] = jnp.zeros(columns_in.shape[2:], jnp.float32)

    barrier = pltpu.get_barrier_semaphore()
    neighbours = 0
    for axis in AXES:
        here, size = lax.axis_index(axis), lax.axis_size(axis)
        for step in (-1, 1):
            there = here + step
            exists = (there >= 0) & (there < size)
            neighbours = neighbours + exists.astype(jnp.int32)

            @pl.when(exists)
            def _():
                pl.semaphore_signal(
                    barrier, inc=1, device_id={axis: there}, device_id_type=pl.DeviceIdType.MESH
                )

    pl.semaphore_wait(barrier, neighbours)

    lane = lax.broadcasted_iota(jnp.int32, (8, LANES), 1)

    def columns_of(field, plane, slot, low, high):
        rows_out[slot, 0, pl.ds(plane, 1), :] = field[0:1, :]
        rows_out[slot, 1, pl.ds(plane, 1), :] = field[plane_rows - 1 : plane_rows, :]
        for tile in range(tiles):
            rows = slice(8 * tile, 8 * tile + 8)
            mine = lane == plane * tiles + tile
            first = pick(field[rows, 0:LANES], jnp.zeros((8, LANES), jnp.int32), 1)
            last = pick(field[rows, width - LANES : width], jnp.full((8, LANES), LANES - 1, jnp.int32), 1)
            low = jnp.where(mine, first, low)
            high = jnp.where(mine, last, high)
        return low, high

    def exchange_faces(field, count, slot, low, high):
        columns_out[slot, 0] = low
        columns_out[slot, 1] = high
        here = pl.ds(0, count)

        def planes(first):
            return field.at[pl.ds(first * plane_rows, plane_rows), :]

        sides = (
            ("gx", -1, planes(1), planes(count + 1)),
            ("gx", 1, planes(count), planes(0)),
            ("gy", -1, rows_out.at[slot, 0, here], rows_in.at[slot, 1, here]),
            ("gy", 1, rows_out.at[slot, 1, here], rows_in.at[slot, 0, here]),
            ("gz", -1, columns_out.at[slot, 0], columns_in.at[slot, 1]),
            ("gz", 1, columns_out.at[slot, 1], columns_in.at[slot, 0]),
        )
        copies = halo_copies(sides, slot, send_sems, recv_sems)
        for copy, sends, receives in copies:
            pl.when(sends)(copy.start)
        for copy, sends, receives in copies:
            pl.when(sends)(copy.wait_send)
            pl.when(receives)(copy.wait_recv)

    row_index = lax.broadcasted_iota(jnp.int32, (plane_rows, width), 0)
    lane_index = lax.broadcasted_iota(jnp.int32, (plane_rows, LANES), 1)

    def beside(field, plane, slot, reach):
        first = pl.multiple_of((plane + 1) * plane_rows, plane_rows)
        centre_plane = field[pl.ds(first, plane_rows), :]
        total = field[pl.ds(first - plane_rows, plane_rows), :] + field[pl.ds(first + plane_rows, plane_rows), :]
        above = rows_in[slot, 0, pl.ds(plane, 1), :]
        below = rows_in[slot, 1, pl.ds(plane, 1), :]
        total = total + jnp.where(row_index < reach, above, pltpu.roll(centre_plane, reach, 0))
        total = total + jnp.where(
            row_index >= plane_rows - reach, below, pltpu.roll(centre_plane, plane_rows - reach, 0)
        )
        spread_low, spread_high = [], []
        for tile in range(tiles):
            where = jnp.full((8, LANES), plane * tiles + tile, jnp.int32)
            spread_low.append(pick(columns_in[slot, 0], where, 1))
            spread_high.append(pick(columns_in[slot, 1], where, 1))
        left = pltpu.roll(centre_plane, reach, 1)
        right = pltpu.roll(centre_plane, width - reach, 1)
        left_edge = jnp.where(lane_index < reach, jnp.concatenate(spread_low, axis=0), left[:, :LANES])
        right_edge = jnp.where(
            lane_index >= LANES - reach, jnp.concatenate(spread_high, axis=0), right[:, width - LANES :]
        )
        total = total + jnp.concatenate([left_edge, left[:, LANES:]], axis=1)
        total = total + jnp.concatenate([right[:, : width - LANES], right_edge], axis=1)
        return centre_plane, total

    def rows_of(plane):
        return pl.ds(pl.multiple_of(plane * plane_rows, plane_rows), plane_rows)

    nothing = jnp.zeros((8, LANES), jnp.float32)

    def each_plane(count, step):
        return lax.fori_loop(0, count, step, (nothing, nothing))

    def sweep(source, target, slot, count, reach, rhs, scale, change, keep, gain, out=None):
        def step(plane, carry):
            here = rows_of(plane)
            field, total = beside(source, plane, slot, reach)
            remain = scale[here, :] * (rhs[here, :] + total) - field
            moved = gain * remain
            if keep:
                moved = moved + keep * change[here, :]
            answer = field + moved
            if out is not None:
                out[here, :] = answer
                return carry
            change[here, :] = moved
            target[rows_of(plane + 1), :] = answer
            return columns_of(answer, plane, 1 - slot, *carry)

        return each_plane(count, step)

    ratio = centre / spread
    gains, factor = [], 1.0 / ratio
    for _ in range(COARSE_SMOOTH):
        factor_new = 1.0 / (2.0 * ratio - factor)
        gains.append((factor_new * factor, 2.0 * factor_new / spread))
        factor = factor_new

    def first_step(plane, carry):
        here = rows_of(plane)
        scale = 1.0 / (6.0 + shift_ref[here, :])
        inverse[here, :] = scale
        answer = scale * forcing_ref[here, :] * (1.0 / centre)
        update[here, :] = answer
        wide_a[rows_of(plane + 1), :] = answer
        return columns_of(answer, plane, 0, *carry)

    edges = each_plane(nplane, first_step)
    slot = 0
    exchange_faces(wide[slot], nplane, slot, *edges)
    for sweep_index in range(SMOOTH - 1):
        keep, gain = gains[sweep_index]
        edges = sweep(
            wide[slot], wide[1 - slot], slot, nplane, 1, forcing_ref, inverse, update, keep, gain
        )
        slot = 1 - slot
        exchange_faces(wide[slot], nplane, slot, *edges)
    smooth = wide[slot]

    lane_pair = lax.broadcasted_iota(jnp.int32, (8, LANES), 1) ^ 1
    line_pair = lax.broadcasted_iota(jnp.int32, (8, LANES), 0) ^ 1

    def pair_sum(value):
        lines = []
        for tile in range(tiles):
            parts = []
            for part in range(width // LANES):
                block = value[8 * tile : 8 * tile + 8, part * LANES : (part + 1) * LANES]
                block = block + pick(block, lane_pair, 1)
                parts.append(block + pick(block, line_pair, 0))
            lines.append(jnp.concatenate(parts, axis=1))
        return jnp.concatenate(lines, axis=0)

    smooth_slot = slot
    slot = 1 - slot

    def restrict(plane, carry):
        remains, shifts = None, None
        for half in range(2):
            fine = 2 * plane + half
            here = rows_of(fine)
            field, total = beside(smooth, fine, smooth_slot, 1)
            shift = shift_ref[here, :]
            remain = forcing_ref[here, :] - ((6.0 + shift) * field - total)
            remains = remain if remains is None else remains + remain
            shifts = shift if shifts is None else shifts + shift
        rhs = 0.5 * pair_sum(remains)
        scale = 1.0 / (6.0 + 0.5 * pair_sum(shifts))
        answer = scale * rhs * (1.0 / centre)
        here = rows_of(plane)
        coarse_rhs[here, :] = rhs
        coarse_inverse[here, :] = scale
        coarse_update[here, :] = answer
        coarse[slot][rows_of(plane + 1), :] = answer
        return columns_of(answer, plane, slot, *carry)

    edges = each_plane(ncoarse, restrict)
    for sweep_index in range(COARSE_SMOOTH - 1):
        exchange_faces(coarse[slot], ncoarse, slot, *edges)
        keep, gain = gains[sweep_index]
        edges = sweep(
            coarse[slot], coarse[1 - slot], slot, ncoarse, 2,
            coarse_rhs, coarse_inverse, coarse_update, keep, gain,
        )
        slot = 1 - slot
    fix = coarse[slot]

    def begin_again(plane, carry):
        here = rows_of(plane + 1)
        answer = smooth[here, :] + fix[rows_of(lax.div(plane, 2) + 1), :]
        wide[slot][here, :] = answer
        return columns_of(answer, plane, slot, *carry)

    edges = each_plane(nplane, begin_again)
    for sweep_index in range(SMOOTH):
        exchange_faces(wide[slot], nplane, slot, *edges)
        keep, gain = gains[sweep_index - 1] if sweep_index else (0.0, 1.0 / centre)
        edges = sweep(
            wide[slot], wide[1 - slot], slot, nplane, 1, forcing_ref, inverse, update, keep, gain,
            pressure_ref if sweep_index == SMOOTH - 1 else None,
        )
        slot = 1 - slot


def multigrid(forcing, shift_diag):
    planes, rows, width = forcing.shape
    vmem = pl.BlockSpec(memory_space=pltpu.VMEM)
    flat = (planes * rows, width)
    half = (planes // 2 * rows, width)
    f32 = jnp.float32
    return pl.pallas_call(
        functools.partial(cycle_kernel, rows),
        name="multigrid",
        out_shape=jax.ShapeDtypeStruct(flat, f32),
        in_specs=[vmem, vmem],
        out_specs=vmem,
        scratch_shapes=[
            pltpu.VMEM((flat[0] + 2 * rows, width), f32),
            pltpu.VMEM((flat[0] + 2 * rows, width), f32),
            pltpu.VMEM((half[0] + 2 * rows, width), f32),
            pltpu.VMEM((half[0] + 2 * rows, width), f32),
            pltpu.VMEM(flat, f32),
            pltpu.VMEM(flat, f32),
            pltpu.VMEM(half, f32),
            pltpu.VMEM(half, f32),
            pltpu.VMEM(half, f32),
            pltpu.VMEM((2, 2, planes, width), f32),
            pltpu.VMEM((2, 2, planes, width), f32),
            pltpu.VMEM((2, 2, 8, LANES), f32),
            pltpu.VMEM((2, 2, 8, LANES), f32),
            pltpu.SemaphoreType.DMA((2, 6)),
            pltpu.SemaphoreType.DMA((2, 6)),
        ],
        compiler_params=pltpu.CompilerParams(
            vmem_limit_bytes=48 * 1024 * 1024, collective_id=0, has_side_effects=True
        ),
    )(forcing.reshape(flat), shift_diag.reshape(flat)).reshape(forcing.shape)


def body(
    pressure_rhs,
    shift_diag,
    positions,
    normals,
    tension,
    edge_weight,
    owner_map,
    cell_map,
    connectivity,
):
    every = ("gx", "gy", "gz")
    npoint = positions.shape[1]
    ndevice = lax.axis_size(every)
    begin = lax.axis_index(every) * npoint
    up = [(i, (i + 1) % ndevice) for i in range(ndevice)]
    low = lax.ppermute(positions[:, npoint - LANES :], every, up)
    high = lax.ppermute(positions[:, :LANES], every, [(b, a) for a, b in up])
    surface_force, packed = surface_and_pack(
        jnp.stack([begin, npoint * ndevice]).astype(jnp.int32),
        low,
        high,
        positions,
        normals,
        tension.reshape(npoint // LANES, LANES),
        edge_weight,
        owner_map.reshape(npoint // LANES, LANES),
        cell_map.reshape(npoint // LANES, LANES),
        connectivity,
        ndevice,
    )
    got = lax.all_to_all(packed, every, split_axis=0, concat_axis=0, tiled=True)
    forcing = spread_cells(got.reshape(4 * ndevice, LANES), pressure_rhs)
    pressure = multigrid(forcing, shift_diag)
    return (pressure, surface_force)


def solution(mesh):
    return jax.shard_map(
        body,
        mesh=mesh,
        in_specs=(
            P("gx", "gy", "gz"),
            P("gx", "gy", "gz"),
            P(None, ("gx", "gy", "gz")),
            P(None, ("gx", "gy", "gz")),
            P(("gx", "gy", "gz")),
            P(None, ("gx", "gy", "gz")),
            P(("gx", "gy", "gz"), None),
            P(("gx", "gy", "gz")),
            P(None, ("gx", "gy", "gz")),
        ),
        out_specs=(P("gx", "gy", "gz"), P(None, ("gx", "gy", "gz"))),
        check_vma=False,
    )
```

```python
import functools
import jax
import jax.numpy as jnp
from jax import lax
from jax.experimental import pallas as pl
from jax.experimental.pallas import tpu as pltpu
from jax.sharding import PartitionSpec as P

HALO = 64
SMOOTH = 3
COARSE_SMOOTH = 4


centre = 1.125
spread = 0.875


LANES = 128
BIG = 524288.0
GROUP_ROWS = 80
CELL_BITS = 18


def permute(value, lane_xor, sub_xor):
    if sub_xor:
        where = lax.broadcasted_iota(jnp.int32, value.shape, 0) ^ sub_xor
        value = pick(value, where, 0)
    if lane_xor:
        where = lax.broadcasted_iota(jnp.int32, value.shape, 1) ^ lane_xor
        value = pick(value, where, 1)
    return value


def pick(value, where, axis):
    numbers = lax.GatherDimensionNumbers(
        offset_dims=(),
        collapsed_slice_dims=(axis,),
        start_index_map=(axis,),
        operand_batching_dims=(1 - axis,),
        start_indices_batching_dims=(1 - axis,),
    )
    return lax.gather(
        value,
        where[:, :, None],
        numbers,
        (1, 1),
        mode=lax.GatherScatterMode.PROMISE_IN_BOUNDS,
    )


def exchange(keys, loads, places, bits, top):
    lane_xor = sub_xor = row_xor = 0
    for bit in bits:
        kind, amount = places[bit]
        lane_xor |= amount if kind == "l" else 0
        sub_xor |= amount if kind == "s" else 0
        row_xor |= amount if kind == "v" else 0
    top_kind, top_amount = places[top]
    count = len(keys)
    new_keys, new_loads = [None] * count, [None] * count
    if top_kind == "v":
        for a in range(count):
            if a & top_amount:
                continue
            b = a ^ row_xor
            low, high, low_load, high_load = keys[a], keys[b], loads[a], loads[b]
            stored = b
            if lane_xor or sub_xor:
                high = permute(high, lane_xor, sub_xor)
                high_load = permute(high_load, lane_xor, sub_xor)
                stored = a | top_amount
            swap = low > high
            new_keys[a] = jnp.minimum(low, high)
            new_keys[stored] = jnp.maximum(low, high)
            new_loads[a] = jnp.where(swap, high_load, low_load)
            new_loads[stored] = jnp.where(swap, low_load, high_load)
        return new_keys, new_loads
    axis = 1 if top_kind == "l" else 0
    upper = (lax.broadcasted_iota(jnp.int32, keys[0].shape, axis) & top_amount) != 0
    for a in range(count):
        b = a ^ row_xor
        other = permute(keys[b], lane_xor, sub_xor)
        other_load = permute(loads[b], lane_xor, sub_xor)
        best = jnp.where(upper, jnp.maximum(keys[a], other), jnp.minimum(keys[a], other))
        new_keys[a] = best
        new_loads[a] = jnp.where(best == keys[a], loads[a], other_load)
    return new_keys, new_loads


def merge_levels(keys, loads, places, first, last):
    for level in range(first, last + 1):
        keys, loads = exchange(keys, loads, places, range(level + 1), level)
        for bit in reversed(range(level)):
            keys, loads = exchange(keys, loads, places, (bit,), bit)
    return keys, loads


VMEM_BYTES = 67043328


def device_of(index):
    ny, nz = lax.axis_size("gy"), lax.axis_size("gz")
    return {"gx": index // (ny * nz), "gy": (index // nz) % ny, "gz": index % nz}


def surface_kernel(
    positions_hbm, normals_hbm, tension_hbm, weight_hbm, owner_hbm, cell_hbm, connect_hbm,
    force_ref, got_ref,
    positions_ref, normals_ref, tension_ref, weight_ref, owner_ref, cell_ref, connect_ref,
    low_ref, high_ref, packed_ref, wide, jumps, turned, lists, below_ref, counted, counted_scalar,
    load_sems, sem, edge_send, edge_recv, all_send, all_recv,
):
    npoint = positions_ref.shape[1]
    nrow = npoint // LANES
    nowner = packed_ref.shape[0]
    total = npoint * nowner
    me = lax.axis_index(("gx", "gy", "gz"))
    begin = me * npoint
    sources = (positions_hbm, connect_hbm, weight_hbm, normals_hbm, tension_hbm, owner_hbm, cell_hbm)
    targets = (positions_ref, connect_ref, weight_ref, normals_ref, tension_ref, owner_ref, cell_ref)
    reads = [
        pltpu.make_async_copy(source, target, load_sems.at[which])
        for which, (source, target) in enumerate(zip(sources, targets))
    ]
    for read in reads:
        read.start()

    barrier = pltpu.get_barrier_semaphore()

    def greet(offset, carry):
        pl.semaphore_signal(
            barrier, inc=1, device_id=device_of((me + offset) % nowner),
            device_id_type=pl.DeviceIdType.MESH,
        )
        return carry

    lax.fori_loop(1, nowner, greet, 0)
    for read in reads:
        read.wait()

    half = lax.broadcasted_iota(jnp.int32, (3, LANES), 1) < HALO
    first_block = pltpu.roll(positions_ref[:, 0:LANES], HALO, 1)
    before = first_block
    for row in range(1, nrow):
        after = pltpu.roll(positions_ref[:, row * LANES : (row + 1) * LANES], HALO, 1)
        wide[0:3, row * LANES : (row + 1) * LANES] = jnp.where(half, before, after)
        before = after
    last_block = before

    def one_row(row, carry):
        at = row * LANES if isinstance(row, int) else pl.multiple_of(row * LANES, LANES)
        here, there = pl.ds(at, LANES), pl.ds(at + LANES, LANES)
        blank = jnp.zeros((2, LANES), jnp.int32)
        index = jnp.concatenate([connect_ref[:, here], blank], axis=0)
        index = ((index - begin + HALO) & (total - 1)) - at
        weight = jnp.concatenate([weight_ref[:, here], blank.astype(jnp.float32)], axis=0)
        second = index >= LANES
        index = index & (LANES - 1)
        strength = tension_ref[pl.ds(row, 1), :]
        jump = jnp.zeros((1, LANES), jnp.float32)
        for axis in range(3):
            lower = jnp.broadcast_to(wide[axis : axis + 1, here], (8, LANES))
            upper = jnp.broadcast_to(wide[axis : axis + 1, there], (8, LANES))
            taken = jnp.where(second, pick(upper, index, 1), pick(lower, index, 1))
            pulled = weight * (taken - positions_ref[axis : axis + 1, here])
            force = strength * jnp.sum(pulled, axis=0, keepdims=True)
            force_ref[axis : axis + 1, here] = force
            jump = jump + force * normals_ref[axis : axis + 1, here]
        jumps[pl.ds(row, 1), :] = jump
        return carry

    lax.fori_loop(0, (nrow - 2) // 2, lambda i, c: one_row(2 * i + 2, one_row(2 * i + 1, c)), 0, unroll=4)

    pl.semaphore_wait(barrier, nowner - 1)
    edges = (
        (positions_ref.at[:, pl.ds(npoint - LANES, LANES)], low_ref, 1),
        (positions_ref.at[:, pl.ds(0, LANES)], high_ref, nowner - 1),
    )
    sends = []
    for which, (source, target, offset) in enumerate(edges):
        sends.append(
            pltpu.make_async_remote_copy(
                src_ref=source, dst_ref=target,
                send_sem=edge_send.at[which], recv_sem=edge_recv.at[which],
                device_id=device_of((me + offset) % nowner), device_id_type=pl.DeviceIdType.MESH,
            )
        )
    for send in sends:
        send.start()

    ranks = lax.broadcasted_iota(jnp.int32, (nowner, LANES), 0)

    def count_row(row, below):
        names = owner_ref[pl.ds(row, 1), :]
        return below + jnp.where(names < ranks, 1, 0)

    below = lax.fori_loop(0, nrow, count_row, jnp.zeros((nowner, LANES), jnp.int32), unroll=4)
    for bit in range(7):
        below = below + pltpu.roll(below, 1 << bit, 1)
    below_ref[...] = below
    counted[...] = jnp.transpose(below_ref[...])[0:8, :]
    fetch = pltpu.make_async_copy(counted, counted_scalar, sem)

    for send in sends:
        send.wait()
    wide[0:3, 0:LANES] = jnp.where(half, pltpu.roll(low_ref[...], HALO, 1), first_block)
    wide[0:3, npoint : npoint + LANES] = jnp.where(half, last_block, pltpu.roll(high_ref[...], HALO, 1))
    one_row(0, 0)
    one_row(nrow - 1, 0)

    keys, loads = [], []
    for tile in range(nrow // 8):
        rows = slice(8 * tile, 8 * tile + 8)
        cell = cell_ref[rows, :]
        cell = ((cell & 384) << 9) | ((cell >> 9) << 7) | (cell & 127)
        keys.append((owner_ref[rows, :] << CELL_BITS) | cell)
        loads.append(jumps[rows, :])
    fetch.start()
    places = [("v", 1), ("v", 2), ("v", 4), ("s", 1), ("s", 2), ("s", 4)]
    places += [("l", 1 << bit) for bit in range(7)]
    keys, loads = merge_levels(keys, loads, places, 0, 12)
    for which, arrays in ((0, keys), (1, loads)):
        for tile in range(8):
            value = arrays[tile]
            if which == 0:
                value = (value & ((1 << CELL_BITS) - 1)).astype(jnp.float32)
            turned[pl.ds(tile, 8, stride=8), :] = value
        turned[64:128, :] = jnp.zeros((64, LANES), jnp.float32)
        flipped = jnp.transpose(turned[...])
        turned[...] = flipped
        even = turned[pl.ds(0, 64, stride=2), :]
        odd = pltpu.roll(turned[pl.ds(1, 64, stride=2), :], 64, 1)
        lane = lax.broadcasted_iota(jnp.int32, (64, LANES), 1)
        lists[pl.ds(which, 64, stride=2), :] = jnp.where(lane < 64, even, odd)
    lists[128:144, :] = jnp.zeros((16, LANES), jnp.float32)
    fetch.wait()

    lane = lax.broadcasted_iota(jnp.int32, (8, LANES), 1)
    line = lax.broadcasted_iota(jnp.int32, (8, LANES), 0)
    slot = lane + LANES * (line >> 1)
    filler = jnp.where((line & 1) == 0, BIG, 0.0).astype(jnp.float32)

    def one_owner(owner, carry):
        start = counted_scalar[0, owner]
        following = jnp.where(owner == nowner - 1, npoint, counted_scalar[0, jnp.minimum(owner + 1, nowner - 1)])
        shift = start & (LANES - 1)
        block = lists[pl.ds((start >> 7) * 2, 8), :]
        block = pltpu.roll(block, (LANES - shift) & (LANES - 1), 1)
        block = jnp.where(lane < LANES - shift, block, pltpu.roll(block, 6, 0))
        block = jnp.where(slot < following - start, block, filler)
        packed_ref[owner] = block[0:4, :]
        return carry

    lax.fori_loop(0, nowner, one_owner, 0, unroll=8)

    def send_one(offset, carry):
        other = (me + offset) % nowner
        pltpu.make_async_remote_copy(
            src_ref=packed_ref.at[other], dst_ref=got_ref.at[me],
            send_sem=all_send, recv_sem=all_recv,
            device_id=device_of(other), device_id_type=pl.DeviceIdType.MESH,
        ).start()
        return carry

    lax.fori_loop(1, nowner, send_one, 0)
    keep = pltpu.make_async_copy(packed_ref.at[me], got_ref.at[me], sem)
    keep.start()
    everything = pltpu.make_async_remote_copy(
        src_ref=packed_ref.at[pl.ds(0, nowner - 1)], dst_ref=got_ref.at[pl.ds(0, nowner - 1)],
        send_sem=all_send, recv_sem=all_recv,
        device_id=device_of((me + 1) % nowner), device_id_type=pl.DeviceIdType.MESH,
    )
    everything.wait_send()
    everything.wait_recv()
    keep.wait()


def spread_kernel(
    got_ref, rhs_hbm, force_in, forcing_ref, force_ref,
    keys_scratch, loads_scratch, grid, turned, bounds, bounds_scalar, work, rhs_ref, sem, rhs_sem,
):
    read = pltpu.make_async_copy(rhs_hbm, rhs_ref, rhs_sem)
    read.start()
    force_ref[...] = force_in[...]
    nsender = got_ref.shape[0] // 4
    ngroup = nsender // 32
    places = [("l", 1 << bit) for bit in range(7)] + [("v", 1), ("v", 2), ("v", 4)]
    places += [("s", 1), ("s", 2), ("s", 4)]

    def zero(step, carry):
        grid[pl.ds(pl.multiple_of(step * 64, 64), 64), :] = jnp.zeros((64, LANES), jnp.float32)
        return carry

    lax.fori_loop(0, grid.shape[0] // 64, zero, 0)

    def one_group(group):
        keys, loads = [], []
        for quarter in range(4):
            for side in range(2):
                first = (group * 32 + quarter * 8) * 4 + 2 * side
                keys.append(got_ref[pl.ds(first, 8, stride=4), :])
                loads.append(got_ref[pl.ds(first + 1, 8, stride=4), :])
        keys, loads = merge_levels(keys, loads, places, 8, 12)
        for quarter in range(4):
            rows = pl.ds(group * 32 + quarter, 8, stride=4)
            last = jnp.full((8, 1), -1, jnp.int32)
            base = None
            for side in range(2):
                key = keys[2 * quarter + side]
                columns = slice(side * LANES, (side + 1) * LANES)
                cell = key.astype(jnp.int32)
                keys_scratch[side, rows, :] = cell
                loads_scratch[side, rows, :] = loads[2 * quarter + side]
                inside = key < BIG
                line = (cell >> 7).astype(jnp.float32)
                top = jnp.max(jnp.where(inside, line, -1.0), axis=1, keepdims=True)
                last = jnp.maximum(last, top.astype(jnp.int32))
                if side == 0:
                    base = jnp.min(line, axis=1, keepdims=True).astype(jnp.int32) & -8
            repeats = jnp.where(last < 0, 0, (((last - base) * 52429) >> 22) + 1)
            pair = jnp.where(last < 0, 0, base) * 32 + repeats
            turned[rows, :] = jnp.broadcast_to(pair.astype(jnp.float32), (8, LANES))

    for group in range(ngroup):
        one_group(group)
    bounds[...] = jnp.transpose(turned[...])[0:8, :].astype(jnp.int32)
    fetch = pltpu.make_async_copy(bounds, bounds_scalar, sem)
    fetch.start()
    fetch.wait()

    def list_chunk(chunk, filled):
        pair = bounds_scalar[0, chunk]
        base = pair >> 5

        def list_piece(piece, filled):
            work[filled] = (chunk << 12) | (base + piece * GROUP_ROWS)
            return filled + 1

        return lax.fori_loop(0, pair & 31, list_piece, filled)

    filled = lax.fori_loop(0, 32 * ngroup, list_chunk, 0)
    for extra in range(BATCH):
        work[filled + extra] = 2048
    lines = lax.broadcasted_iota(jnp.int32, (GROUP_ROWS, 2 * LANES), 0)
    columns = lax.broadcasted_iota(jnp.int32, (LANES, 2 * LANES), 0)

    def one_batch(batch, carry):
        sums, bases = [], []
        for piece in range(BATCH):
            item = work[batch * BATCH + piece]
            chunk = item >> 12
            base = pl.multiple_of(item & 4095, 8)
            cell = jnp.concatenate([keys_scratch[side, pl.ds(chunk, 1), :] for side in range(2)], axis=1)
            load = jnp.concatenate([loads_scratch[side, pl.ds(chunk, 1), :] for side in range(2)], axis=1)
            coarse = load.astype(jnp.bfloat16).astype(jnp.float32)
            here = ((cell >> 7) - base) == lines
            left = jnp.concatenate(
                [
                    jnp.where(here, coarse, 0.0).astype(jnp.bfloat16),
                    jnp.where(here, load - coarse, 0.0).astype(jnp.bfloat16),
                ],
                axis=0,
            )
            right = jnp.where((cell & (LANES - 1)) == columns, 1.0, 0.0).astype(jnp.bfloat16)
            both = lax.dot_general(
                left, right, (((1,), (1,)), ((), ())), preferred_element_type=jnp.float32
            )
            sums.append(both[:GROUP_ROWS] + both[GROUP_ROWS:])
            bases.append(base)
        for total, base in zip(sums, bases):
            grid[pl.ds(base, GROUP_ROWS), :] += total
        return carry

    lax.fori_loop(0, (filled + BATCH - 1) // BATCH, one_batch, 0)

    read.wait()
    shape = forcing_ref.shape
    for plane in range(shape[0]):
        for part in range(shape[2] // LANES):
            columns = slice(part * LANES, (part + 1) * LANES)
            first = (part * shape[0] + plane) * shape[1]
            forcing_ref[plane, :, columns] = rhs_ref[plane, :, columns] + grid[first : first + shape[1], :]


BATCH = 8


def surface_and_send(positions, normals, tension, edge_weight, owners, cells, connectivity):
    nowner = lax.axis_size(("gx", "gy", "gz"))
    vmem = pl.BlockSpec(memory_space=pltpu.VMEM)
    arrays = (positions, normals, tension, edge_weight, owners, cells, connectivity)
    return pl.pallas_call(
        surface_kernel,
        name="surface",
        out_shape=(
            jax.ShapeDtypeStruct(positions.shape, jnp.float32),
            jax.ShapeDtypeStruct((nowner, 4, LANES), jnp.float32),
        ),
        in_specs=[pl.BlockSpec(memory_space=pltpu.HBM)] * len(arrays),
        out_specs=(vmem, pl.BlockSpec(memory_space=pltpu.HBM)),
        scratch_shapes=[pltpu.VMEM(array.shape, array.dtype) for array in arrays]
        + [
            pltpu.VMEM((3, LANES), jnp.float32),
            pltpu.VMEM((3, LANES), jnp.float32),
            pltpu.VMEM((nowner, 4, LANES), jnp.float32),
            pltpu.VMEM((8, positions.shape[1] + LANES), jnp.float32),
            pltpu.VMEM((positions.shape[1] // LANES, LANES), jnp.float32),
            pltpu.VMEM((128, LANES), jnp.float32),
            pltpu.VMEM((144, LANES), jnp.float32),
            pltpu.VMEM((nowner, LANES), jnp.int32),
            pltpu.VMEM((8, LANES), jnp.int32),
            pltpu.SMEM((8, LANES), jnp.int32),
            pltpu.SemaphoreType.DMA((7,)),
            pltpu.SemaphoreType.DMA,
            pltpu.SemaphoreType.DMA((2,)),
            pltpu.SemaphoreType.DMA((2,)),
            pltpu.SemaphoreType.DMA,
            pltpu.SemaphoreType.DMA,
        ],
        compiler_params=pltpu.CompilerParams(
            vmem_limit_bytes=VMEM_BYTES, collective_id=1, has_side_effects=True
        ),
    )(*arrays)


def spread_cells(got, pressure_rhs, force):
    vmem = pl.BlockSpec(memory_space=pltpu.VMEM)
    return pl.pallas_call(
        spread_kernel,
        name="spread",
        out_shape=(
            jax.ShapeDtypeStruct(pressure_rhs.shape, jnp.float32),
            jax.ShapeDtypeStruct(force.shape, jnp.float32),
        ),
        in_specs=[vmem, pl.BlockSpec(memory_space=pltpu.HBM), vmem],
        out_specs=(vmem, vmem),
        scratch_shapes=[
            pltpu.VMEM((2, 128, LANES), jnp.int32),
            pltpu.VMEM((2, 128, LANES), jnp.float32),
            pltpu.VMEM((2048 + 128, LANES), jnp.float32),
            pltpu.VMEM((128, LANES), jnp.float32),
            pltpu.VMEM((8, LANES), jnp.int32),
            pltpu.SMEM((8, LANES), jnp.int32),
            pltpu.SMEM((512,), jnp.int32),
            pltpu.VMEM(pressure_rhs.shape, jnp.float32),
            pltpu.SemaphoreType.DMA,
            pltpu.SemaphoreType.DMA,
        ],
        compiler_params=pltpu.CompilerParams(vmem_limit_bytes=VMEM_BYTES),
    )(got, pressure_rhs, force)


AXES = ("gx", "gy", "gz")


def halo_copies(sides, slot, send_sems, recv_sems):
    copies = []
    for which, (axis, step, source, target) in enumerate(sides):
        here = lax.axis_index(axis)
        there = here + step
        back = here - step
        size = lax.axis_size(axis)
        copy = pltpu.make_async_remote_copy(
            src_ref=source,
            dst_ref=target,
            send_sem=send_sems.at[slot, which],
            recv_sem=recv_sems.at[slot, which],
            device_id={axis: there},
            device_id_type=pl.DeviceIdType.MESH,
        )
        copies.append((copy, (there >= 0) & (there < size), (back >= 0) & (back < size)))
    return copies


def cycle_kernel(
    plane_rows, forcing_hbm, shift_hbm, pressure_ref, forcing_ref, shift_ref,
    wide_a, wide_b, coarse_a, coarse_b, inverse, update, coarse_rhs, coarse_inverse, coarse_update,
    rows_out, rows_in, columns_out, columns_in, send_sems, recv_sems, load_sems,
):
    reads = [
        pltpu.make_async_copy(source, target, load_sems.at[which])
        for which, (source, target) in enumerate(((forcing_hbm, forcing_ref), (shift_hbm, shift_ref)))
    ]
    for read in reads:
        read.start()
    width = forcing_ref.shape[1]
    nplane = forcing_ref.shape[0] // plane_rows
    ncoarse = nplane // 2
    tiles = plane_rows // 8
    wide, coarse = (wide_a, wide_b), (coarse_a, coarse_b)
    blank = jnp.zeros((plane_rows, width), jnp.float32)
    for slot in range(2):
        wide[slot][0:plane_rows, :] = blank
        wide[slot][(nplane + 1) * plane_rows : (nplane + 2) * plane_rows, :] = blank
        coarse[slot][0:plane_rows, :] = blank
        coarse[slot][(ncoarse + 1) * plane_rows : (ncoarse + 2) * plane_rows, :] = blank
        for side in range(2):
            rows_in[slot, side] = jnp.zeros(rows_in.shape[2:], jnp.float32)
            columns_in[slot, side] = jnp.zeros(columns_in.shape[2:], jnp.float32)

    barrier = pltpu.get_barrier_semaphore()
    neighbours = 0
    for axis in AXES:
        here, size = lax.axis_index(axis), lax.axis_size(axis)
        for step in (-1, 1):
            there = here + step
            exists = (there >= 0) & (there < size)
            neighbours = neighbours + exists.astype(jnp.int32)

            @pl.when(exists)
            def _():
                pl.semaphore_signal(
                    barrier, inc=1, device_id={axis: there}, device_id_type=pl.DeviceIdType.MESH
                )

    for read in reads:
        read.wait()

    lane = lax.broadcasted_iota(jnp.int32, (8, LANES), 1)

    def columns_of(field, plane, slot, low, high):
        rows_out[slot, 0, pl.ds(plane, 1), :] = field[0:1, :]
        rows_out[slot, 1, pl.ds(plane, 1), :] = field[plane_rows - 1 : plane_rows, :]
        for tile in range(tiles):
            rows = slice(8 * tile, 8 * tile + 8)
            mine = lane == plane * tiles + tile
            first = pick(field[rows, 0:LANES], jnp.zeros((8, LANES), jnp.int32), 1)
            last = pick(field[rows, width - LANES : width], jnp.full((8, LANES), LANES - 1, jnp.int32), 1)
            low = jnp.where(mine, first, low)
            high = jnp.where(mine, last, high)
        return low, high

    def exchange_faces(field, count, slot, low, high):
        columns_out[slot, 0] = low
        columns_out[slot, 1] = high
        here = pl.ds(0, count)

        def planes(first):
            return field.at[pl.ds(first * plane_rows, plane_rows), :]

        sides = (
            ("gx", -1, planes(1), planes(count + 1)),
            ("gx", 1, planes(count), planes(0)),
            ("gy", -1, rows_out.at[slot, 0, here], rows_in.at[slot, 1, here]),
            ("gy", 1, rows_out.at[slot, 1, here], rows_in.at[slot, 0, here]),
            ("gz", -1, columns_out.at[slot, 0], columns_in.at[slot, 1]),
            ("gz", 1, columns_out.at[slot, 1], columns_in.at[slot, 0]),
        )
        copies = halo_copies(sides, slot, send_sems, recv_sems)
        for copy, sends, receives in copies:
            pl.when(sends)(copy.start)
        for copy, sends, receives in copies:
            pl.when(sends)(copy.wait_send)
            pl.when(receives)(copy.wait_recv)

    row_index = lax.broadcasted_iota(jnp.int32, (plane_rows, width), 0)
    lane_index = lax.broadcasted_iota(jnp.int32, (plane_rows, LANES), 1)

    def beside(field, plane, slot, reach):
        first = pl.multiple_of((plane + 1) * plane_rows, plane_rows)
        centre_plane = field[pl.ds(first, plane_rows), :]
        total = field[pl.ds(first - plane_rows, plane_rows), :] + field[pl.ds(first + plane_rows, plane_rows), :]
        above = rows_in[slot, 0, pl.ds(plane, 1), :]
        below = rows_in[slot, 1, pl.ds(plane, 1), :]
        total = total + jnp.where(row_index < reach, above, pltpu.roll(centre_plane, reach, 0))
        total = total + jnp.where(
            row_index >= plane_rows - reach, below, pltpu.roll(centre_plane, plane_rows - reach, 0)
        )
        spread_low, spread_high = [], []
        for tile in range(tiles):
            where = jnp.full((8, LANES), plane * tiles + tile, jnp.int32)
            spread_low.append(pick(columns_in[slot, 0], where, 1))
            spread_high.append(pick(columns_in[slot, 1], where, 1))
        left = pltpu.roll(centre_plane, reach, 1)
        right = pltpu.roll(centre_plane, width - reach, 1)
        left_edge = jnp.where(lane_index < reach, jnp.concatenate(spread_low, axis=0), left[:, :LANES])
        right_edge = jnp.where(
            lane_index >= LANES - reach, jnp.concatenate(spread_high, axis=0), right[:, width - LANES :]
        )
        total = total + jnp.concatenate([left_edge, left[:, LANES:]], axis=1)
        total = total + jnp.concatenate([right[:, : width - LANES], right_edge], axis=1)
        return centre_plane, total

    def rows_of(plane):
        return pl.ds(pl.multiple_of(plane * plane_rows, plane_rows), plane_rows)

    nothing = jnp.zeros((8, LANES), jnp.float32)

    def each_plane(count, step):
        return lax.fori_loop(0, count, step, (nothing, nothing))

    def sweep(source, target, slot, count, reach, rhs, scale, change, keep, gain, out=None):
        def step(plane, carry):
            here = rows_of(plane)
            field, total = beside(source, plane, slot, reach)
            remain = scale[here, :] * (rhs[here, :] + total) - field
            moved = gain * remain
            if keep:
                moved = moved + keep * change[here, :]
            answer = field + moved
            if out is not None:
                out[here, :] = answer
                return carry
            change[here, :] = moved
            target[rows_of(plane + 1), :] = answer
            return columns_of(answer, plane, 1 - slot, *carry)

        return each_plane(count, step)

    ratio = centre / spread
    gains, factor = [], 1.0 / ratio
    for _ in range(COARSE_SMOOTH):
        factor_new = 1.0 / (2.0 * ratio - factor)
        gains.append((factor_new * factor, 2.0 * factor_new / spread))
        factor = factor_new

    def first_step(plane, carry):
        here = rows_of(plane)
        scale = 1.0 / (6.0 + shift_ref[here, :])
        inverse[here, :] = scale
        answer = scale * forcing_ref[here, :] * (1.0 / centre)
        update[here, :] = answer
        wide_a[rows_of(plane + 1), :] = answer
        return columns_of(answer, plane, 0, *carry)

    edges = each_plane(nplane, first_step)
    slot = 0
    pl.semaphore_wait(barrier, neighbours)
    exchange_faces(wide[slot], nplane, slot, *edges)
    for sweep_index in range(SMOOTH - 1):
        keep, gain = gains[sweep_index]
        edges = sweep(
            wide[slot], wide[1 - slot], slot, nplane, 1, forcing_ref, inverse, update, keep, gain
        )
        slot = 1 - slot
        exchange_faces(wide[slot], nplane, slot, *edges)
    smooth = wide[slot]

    lane_pair = lax.broadcasted_iota(jnp.int32, (8, LANES), 1) ^ 1
    line_pair = lax.broadcasted_iota(jnp.int32, (8, LANES), 0) ^ 1

    def pair_sum(value):
        lines = []
        for tile in range(tiles):
            parts = []
            for part in range(width // LANES):
                block = value[8 * tile : 8 * tile + 8, part * LANES : (part + 1) * LANES]
                block = block + pick(block, lane_pair, 1)
                parts.append(block + pick(block, line_pair, 0))
            lines.append(jnp.concatenate(parts, axis=1))
        return jnp.concatenate(lines, axis=0)

    smooth_slot = slot
    slot = 1 - slot

    def restrict(plane, carry):
        remains, shifts = None, None
        for half in range(2):
            fine = 2 * plane + half
            here = rows_of(fine)
            field, total = beside(smooth, fine, smooth_slot, 1)
            shift = shift_ref[here, :]
            remain = forcing_ref[here, :] - ((6.0 + shift) * field - total)
            remains = remain if remains is None else remains + remain
            shifts = shift if shifts is None else shifts + shift
        rhs = 0.5 * pair_sum(remains)
        scale = 1.0 / (6.0 + 0.5 * pair_sum(shifts))
        answer = scale * rhs * (1.0 / centre)
        here = rows_of(plane)
        coarse_rhs[here, :] = rhs
        coarse_inverse[here, :] = scale
        coarse_update[here, :] = answer
        coarse[slot][rows_of(plane + 1), :] = answer
        return columns_of(answer, plane, slot, *carry)

    edges = each_plane(ncoarse, restrict)
    for sweep_index in range(COARSE_SMOOTH - 1):
        exchange_faces(coarse[slot], ncoarse, slot, *edges)
        keep, gain = gains[sweep_index]
        edges = sweep(
            coarse[slot], coarse[1 - slot], slot, ncoarse, 2,
            coarse_rhs, coarse_inverse, coarse_update, keep, gain,
        )
        slot = 1 - slot
    fix = coarse[slot]

    def begin_again(plane, carry):
        here = rows_of(plane + 1)
        answer = smooth[here, :] + fix[rows_of(lax.div(plane, 2) + 1), :]
        wide[slot][here, :] = answer
        return columns_of(answer, plane, slot, *carry)

    edges = each_plane(nplane, begin_again)
    for sweep_index in range(SMOOTH):
        exchange_faces(wide[slot], nplane, slot, *edges)
        keep, gain = gains[sweep_index - 1] if sweep_index else (0.0, 1.0 / centre)
        edges = sweep(
            wide[slot], wide[1 - slot], slot, nplane, 1, forcing_ref, inverse, update, keep, gain,
            pressure_ref if sweep_index == SMOOTH - 1 else None,
        )
        slot = 1 - slot


def multigrid(forcing, shift_diag):
    planes, rows, width = forcing.shape
    vmem = pl.BlockSpec(memory_space=pltpu.VMEM)
    flat = (planes * rows, width)
    half = (planes // 2 * rows, width)
    f32 = jnp.float32
    return pl.pallas_call(
        functools.partial(cycle_kernel, rows),
        name="multigrid",
        out_shape=jax.ShapeDtypeStruct(flat, f32),
        in_specs=[pl.BlockSpec(memory_space=pltpu.HBM)] * 2,
        out_specs=vmem,
        scratch_shapes=[
            pltpu.VMEM(flat, f32),
            pltpu.VMEM(flat, f32),
            pltpu.VMEM((flat[0] + 2 * rows, width), f32),
            pltpu.VMEM((flat[0] + 2 * rows, width), f32),
            pltpu.VMEM((half[0] + 2 * rows, width), f32),
            pltpu.VMEM((half[0] + 2 * rows, width), f32),
            pltpu.VMEM(flat, f32),
            pltpu.VMEM(flat, f32),
            pltpu.VMEM(half, f32),
            pltpu.VMEM(half, f32),
            pltpu.VMEM(half, f32),
            pltpu.VMEM((2, 2, planes, width), f32),
            pltpu.VMEM((2, 2, planes, width), f32),
            pltpu.VMEM((2, 2, 8, LANES), f32),
            pltpu.VMEM((2, 2, 8, LANES), f32),
            pltpu.SemaphoreType.DMA((2, 6)),
            pltpu.SemaphoreType.DMA((2, 6)),
            pltpu.SemaphoreType.DMA((2,)),
        ],
        compiler_params=pltpu.CompilerParams(
            vmem_limit_bytes=VMEM_BYTES, collective_id=0, has_side_effects=True
        ),
    )(forcing.reshape(flat), shift_diag.reshape(flat)).reshape(forcing.shape)


def body(
    pressure_rhs,
    shift_diag,
    positions,
    normals,
    tension,
    edge_weight,
    owner_map,
    cell_map,
    connectivity,
):
    ndevice = lax.axis_size(("gx", "gy", "gz"))
    nrow = positions.shape[1] // LANES
    force, got = surface_and_send(
        positions,
        normals,
        tension.reshape(nrow, LANES),
        edge_weight,
        owner_map.reshape(nrow, LANES),
        cell_map.reshape(nrow, LANES),
        connectivity,
    )
    forcing, surface_force = spread_cells(got.reshape(4 * ndevice, LANES), pressure_rhs, force)
    pressure = multigrid(forcing, shift_diag)
    return (pressure, surface_force)


def solution(mesh):
    return jax.shard_map(
        body,
        mesh=mesh,
        in_specs=(
            P("gx", "gy", "gz"),
            P("gx", "gy", "gz"),
            P(None, ("gx", "gy", "gz")),
            P(None, ("gx", "gy", "gz")),
            P(("gx", "gy", "gz")),
            P(None, ("gx", "gy", "gz")),
            P(("gx", "gy", "gz"), None),
            P(("gx", "gy", "gz")),
            P(None, ("gx", "gy", "gz")),
        ),
        out_specs=(P("gx", "gy", "gz"), P(None, ("gx", "gy", "gz"))),
        check_vma=False,
    )
```

```python
import functools
import jax
import jax.numpy as jnp
from jax import lax
from jax.experimental import pallas as pl
from jax.experimental.pallas import tpu as pltpu
from jax.sharding import PartitionSpec as P

HALO = 64
SMOOTH = 3
COARSE_SMOOTH = 4


centre = 1.125
spread = 0.875


LANES = 128
BIG = 524288.0
GROUP_ROWS = 80
CELL_BITS = 18


def permute(value, lane_xor, sub_xor):
    if sub_xor:
        where = lax.broadcasted_iota(jnp.int32, value.shape, 0) ^ sub_xor
        value = pick(value, where, 0)
    if lane_xor:
        where = lax.broadcasted_iota(jnp.int32, value.shape, 1) ^ lane_xor
        value = pick(value, where, 1)
    return value


def pick(value, where, axis):
    numbers = lax.GatherDimensionNumbers(
        offset_dims=(),
        collapsed_slice_dims=(axis,),
        start_index_map=(axis,),
        operand_batching_dims=(1 - axis,),
        start_indices_batching_dims=(1 - axis,),
    )
    return lax.gather(
        value,
        where[:, :, None],
        numbers,
        (1, 1),
        mode=lax.GatherScatterMode.PROMISE_IN_BOUNDS,
    )


def exchange(keys, loads, places, bits, top):
    lane_xor = sub_xor = row_xor = 0
    for bit in bits:
        kind, amount = places[bit]
        lane_xor |= amount if kind == "l" else 0
        sub_xor |= amount if kind == "s" else 0
        row_xor |= amount if kind == "v" else 0
    top_kind, top_amount = places[top]
    count = len(keys)
    new_keys, new_loads = [None] * count, [None] * count
    if top_kind == "v":
        for a in range(count):
            if a & top_amount:
                continue
            b = a ^ row_xor
            low, high, low_load, high_load = keys[a], keys[b], loads[a], loads[b]
            stored = b
            if lane_xor or sub_xor:
                high = permute(high, lane_xor, sub_xor)
                high_load = permute(high_load, lane_xor, sub_xor)
                stored = a | top_amount
            swap = low > high
            new_keys[a] = jnp.minimum(low, high)
            new_keys[stored] = jnp.maximum(low, high)
            new_loads[a] = jnp.where(swap, high_load, low_load)
            new_loads[stored] = jnp.where(swap, low_load, high_load)
        return new_keys, new_loads
    axis = 1 if top_kind == "l" else 0
    upper = (lax.broadcasted_iota(jnp.int32, keys[0].shape, axis) & top_amount) != 0
    for a in range(count):
        b = a ^ row_xor
        other = permute(keys[b], lane_xor, sub_xor)
        other_load = permute(loads[b], lane_xor, sub_xor)
        best = jnp.where(upper, jnp.maximum(keys[a], other), jnp.minimum(keys[a], other))
        new_keys[a] = best
        new_loads[a] = jnp.where(best == keys[a], loads[a], other_load)
    return new_keys, new_loads


def merge_levels(groups, places, first, last):
    for level in range(first, last + 1):
        groups = [exchange(*group, places, range(level + 1), level) for group in groups]
        for bit in reversed(range(level)):
            groups = [exchange(*group, places, (bit,), bit) for group in groups]
    return groups


VMEM_BYTES = 67043328


def device_of(index):
    ny, nz = lax.axis_size("gy"), lax.axis_size("gz")
    return {"gx": index // (ny * nz), "gy": (index // nz) % ny, "gz": index % nz}


def surface_kernel(
    positions_hbm, normals_hbm, tension_hbm, weight_hbm, owner_hbm, cell_hbm, connect_hbm,
    force_ref, got_ref,
    positions_ref, normals_ref, tension_ref, weight_ref, owner_ref, cell_ref, connect_ref,
    low_ref, high_ref, packed_ref, wide, jumps, turned, lists, below_ref, counted, counted_scalar,
    load_sems, sem, edge_send, edge_recv, all_send, all_recv,
):
    npoint = positions_ref.shape[1]
    nrow = npoint // LANES
    nowner = packed_ref.shape[0]
    total = npoint * nowner
    me = lax.axis_index(("gx", "gy", "gz"))
    begin = me * npoint
    sources = (positions_hbm, connect_hbm, weight_hbm, normals_hbm, tension_hbm, owner_hbm, cell_hbm)
    targets = (positions_ref, connect_ref, weight_ref, normals_ref, tension_ref, owner_ref, cell_ref)
    reads = [
        pltpu.make_async_copy(source, target, load_sems.at[which])
        for which, (source, target) in enumerate(zip(sources, targets))
    ]
    for read in reads:
        read.start()

    barrier = pltpu.get_barrier_semaphore()

    def greet(offset, carry):
        pl.semaphore_signal(
            barrier, inc=1, device_id=device_of((me + offset) % nowner),
            device_id_type=pl.DeviceIdType.MESH,
        )
        return carry

    lax.fori_loop(1, nowner, greet, 0)
    for read in reads:
        read.wait()

    half = lax.broadcasted_iota(jnp.int32, (3, LANES), 1) < HALO
    first_block = pltpu.roll(positions_ref[:, 0:LANES], HALO, 1)
    before = first_block
    for row in range(1, nrow):
        after = pltpu.roll(positions_ref[:, row * LANES : (row + 1) * LANES], HALO, 1)
        wide[0:3, row * LANES : (row + 1) * LANES] = jnp.where(half, before, after)
        before = after
    last_block = before

    def one_row(row, carry):
        at = row * LANES if isinstance(row, int) else pl.multiple_of(row * LANES, LANES)
        here, there = pl.ds(at, LANES), pl.ds(at + LANES, LANES)
        blank = jnp.zeros((2, LANES), jnp.int32)
        index = jnp.concatenate([connect_ref[:, here], blank], axis=0)
        index = ((index - begin + HALO) & (total - 1)) - at
        weight = jnp.concatenate([weight_ref[:, here], blank.astype(jnp.float32)], axis=0)
        second = index >= LANES
        index = index & (LANES - 1)
        strength = tension_ref[pl.ds(row, 1), :]
        jump = jnp.zeros((1, LANES), jnp.float32)
        for axis in range(3):
            lower = jnp.broadcast_to(wide[axis : axis + 1, here], (8, LANES))
            upper = jnp.broadcast_to(wide[axis : axis + 1, there], (8, LANES))
            taken = jnp.where(second, pick(upper, index, 1), pick(lower, index, 1))
            pulled = weight * (taken - positions_ref[axis : axis + 1, here])
            force = strength * jnp.sum(pulled, axis=0, keepdims=True)
            force_ref[axis : axis + 1, here] = force
            jump = jump + force * normals_ref[axis : axis + 1, here]
        jumps[pl.ds(row, 1), :] = jump
        return carry

    lax.fori_loop(0, (nrow - 2) // 2, lambda i, c: one_row(2 * i + 2, one_row(2 * i + 1, c)), 0, unroll=4)

    pl.semaphore_wait(barrier, nowner - 1)
    edges = (
        (positions_ref.at[:, pl.ds(npoint - LANES, LANES)], low_ref, 1),
        (positions_ref.at[:, pl.ds(0, LANES)], high_ref, nowner - 1),
    )
    sends = []
    for which, (source, target, offset) in enumerate(edges):
        sends.append(
            pltpu.make_async_remote_copy(
                src_ref=source, dst_ref=target,
                send_sem=edge_send.at[which], recv_sem=edge_recv.at[which],
                device_id=device_of((me + offset) % nowner), device_id_type=pl.DeviceIdType.MESH,
            )
        )
    for send in sends:
        send.start()

    ranks = lax.broadcasted_iota(jnp.int32, (nowner, LANES), 0)

    def count_row(row, below):
        names = owner_ref[pl.ds(row, 1), :]
        return below + jnp.where(names < ranks, 1, 0)

    below = lax.fori_loop(0, nrow, count_row, jnp.zeros((nowner, LANES), jnp.int32), unroll=4)
    for bit in range(7):
        below = below + pltpu.roll(below, 1 << bit, 1)
    below_ref[...] = below
    counted[...] = jnp.transpose(below_ref[...])[0:8, :]
    fetch = pltpu.make_async_copy(counted, counted_scalar, sem)

    keys, loads = [], []
    for tile in range(nrow // 8):
        rows = slice(8 * tile, 8 * tile + 8)
        cell = cell_ref[rows, :]
        cell = ((cell & 384) << 9) | ((cell >> 9) << 7) | (cell & 127)
        key = ((owner_ref[rows, :] << CELL_BITS) | cell) << 1
        load = jumps[rows, :]
        if tile in (0, nrow // 8 - 1):
            line = lax.broadcasted_iota(jnp.int32, (8, LANES), 0)
            lane = lax.broadcasted_iota(jnp.int32, (8, LANES), 1)
            late = line == (7 if tile else 0)
            key = key | jnp.where(late, 1, 0)
            load = jnp.where(late, (lane + (LANES if tile else 0)).astype(jnp.float32), load)
        keys.append(key)
        loads.append(load)
    fetch.start()
    places = [("v", 1), ("v", 2), ("v", 4), ("s", 1), ("s", 2), ("s", 4)]
    places += [("l", 1 << bit) for bit in range(7)]
    ((keys, loads),) = merge_levels([(keys, loads)], places, 0, 12)
    for send in sends:
        send.wait()
    wide[0:3, 0:LANES] = jnp.where(half, pltpu.roll(low_ref[...], HALO, 1), first_block)
    wide[0:3, npoint : npoint + LANES] = jnp.where(half, last_block, pltpu.roll(high_ref[...], HALO, 1))
    one_row(0, 0)
    one_row(nrow - 1, 0)

    first_jumps = jnp.broadcast_to(jumps[0:1, :], (8, LANES))
    last_jumps = jnp.broadcast_to(jumps[nrow - 1 : nrow, :], (8, LANES))
    for tile in range(nrow // 8):
        late = (keys[tile] & 1) == 1
        which = jnp.where(late, loads[tile], 0.0).astype(jnp.int32)
        lane = which & (LANES - 1)
        value = jnp.where(which >= LANES, pick(last_jumps, lane, 1), pick(first_jumps, lane, 1))
        loads[tile] = jnp.where(late, value, loads[tile])
        keys[tile] = keys[tile] >> 1
    for which, arrays in ((0, keys), (1, loads)):
        for tile in range(8):
            value = arrays[tile]
            if which == 0:
                value = (value & ((1 << CELL_BITS) - 1)).astype(jnp.float32)
            turned[pl.ds(tile, 8, stride=8), :] = value
        turned[64:128, :] = jnp.zeros((64, LANES), jnp.float32)
        flipped = jnp.transpose(turned[...])
        turned[...] = flipped
        even = turned[pl.ds(0, 64, stride=2), :]
        odd = pltpu.roll(turned[pl.ds(1, 64, stride=2), :], 64, 1)
        lane = lax.broadcasted_iota(jnp.int32, (64, LANES), 1)
        lists[pl.ds(which, 64, stride=2), :] = jnp.where(lane < 64, even, odd)
    lists[128:144, :] = jnp.zeros((16, LANES), jnp.float32)
    fetch.wait()

    lane = lax.broadcasted_iota(jnp.int32, (8, LANES), 1)
    line = lax.broadcasted_iota(jnp.int32, (8, LANES), 0)
    slot = lane + LANES * (line >> 1)
    filler = jnp.where((line & 1) == 0, BIG, 0.0).astype(jnp.float32)

    def one_owner(owner, carry):
        start = counted_scalar[0, owner]
        following = jnp.where(owner == nowner - 1, npoint, counted_scalar[0, jnp.minimum(owner + 1, nowner - 1)])
        shift = start & (LANES - 1)
        block = lists[pl.ds((start >> 7) * 2, 8), :]
        block = pltpu.roll(block, (LANES - shift) & (LANES - 1), 1)
        block = jnp.where(lane < LANES - shift, block, pltpu.roll(block, 6, 0))
        block = jnp.where(slot < following - start, block, filler)
        packed_ref[owner] = block[0:4, :]
        return carry

    lax.fori_loop(0, nowner, one_owner, 0, unroll=8)

    def send_one(offset, carry):
        other = (me + offset) % nowner
        pltpu.make_async_remote_copy(
            src_ref=packed_ref.at[other], dst_ref=got_ref.at[me],
            send_sem=all_send, recv_sem=all_recv,
            device_id=device_of(other), device_id_type=pl.DeviceIdType.MESH,
        ).start()
        return carry

    lax.fori_loop(1, nowner, send_one, 0)
    keep = pltpu.make_async_copy(packed_ref.at[me], got_ref.at[me], sem)
    keep.start()
    everything = pltpu.make_async_remote_copy(
        src_ref=packed_ref.at[pl.ds(0, nowner - 1)], dst_ref=got_ref.at[pl.ds(0, nowner - 1)],
        send_sem=all_send, recv_sem=all_recv,
        device_id=device_of((me + 1) % nowner), device_id_type=pl.DeviceIdType.MESH,
    )
    everything.wait_send()
    everything.wait_recv()
    keep.wait()


def spread_kernel(
    got_ref, force_in, grid, force_ref,
    keys_scratch, loads_scratch, turned, bounds, bounds_scalar, work, sem,
):
    force_ref[...] = force_in[...]
    nsender = got_ref.shape[0] // 4
    ngroup = nsender // 32
    places = [("l", 1 << bit) for bit in range(7)] + [("v", 1), ("v", 2), ("v", 4)]
    places += [("s", 1), ("s", 2), ("s", 4)]

    def zero(step, carry):
        grid[pl.ds(pl.multiple_of(step * 64, 64), 64), :] = jnp.zeros((64, LANES), jnp.float32)
        return carry

    lax.fori_loop(0, grid.shape[0] // 64, zero, 0)

    def read_group(group):
        keys, loads = [], []
        for quarter in range(4):
            for side in range(2):
                first = (group * 32 + quarter * 8) * 4 + 2 * side
                keys.append(got_ref[pl.ds(first, 8, stride=4), :])
                loads.append(got_ref[pl.ds(first + 1, 8, stride=4), :])
        return keys, loads

    def store_group(group, keys, loads):
        for quarter in range(4):
            rows = pl.ds(group * 32 + quarter, 8, stride=4)
            last = jnp.full((8, 1), -1, jnp.int32)
            base = None
            for side in range(2):
                key = keys[2 * quarter + side]
                columns = slice(side * LANES, (side + 1) * LANES)
                cell = key.astype(jnp.int32)
                keys_scratch[side, rows, :] = cell
                loads_scratch[side, rows, :] = loads[2 * quarter + side]
                inside = key < BIG
                line = (cell >> 7).astype(jnp.float32)
                top = jnp.max(jnp.where(inside, line, -1.0), axis=1, keepdims=True)
                last = jnp.maximum(last, top.astype(jnp.int32))
                if side == 0:
                    base = jnp.min(line, axis=1, keepdims=True).astype(jnp.int32) & -8
            repeats = jnp.where(last < 0, 0, (((last - base) * 52429) >> 22) + 1)
            pair = jnp.where(last < 0, 0, base) * 32 + repeats
            turned[rows, :] = jnp.broadcast_to(pair.astype(jnp.float32), (8, LANES))

    for first in range(0, ngroup, TOGETHER):
        chosen = range(first, first + TOGETHER)
        merged = merge_levels([read_group(group) for group in chosen], places, 8, 12)
        for group, (keys, loads) in zip(chosen, merged):
            store_group(group, keys, loads)
    bounds[...] = jnp.transpose(turned[...])[0:8, :].astype(jnp.int32)
    fetch = pltpu.make_async_copy(bounds, bounds_scalar, sem)
    fetch.start()
    fetch.wait()

    def list_chunk(chunk, filled):
        pair = bounds_scalar[0, chunk]
        base = pair >> 5

        def list_piece(piece, filled):
            work[filled] = (chunk << 12) | (base + piece * GROUP_ROWS)
            return filled + 1

        return lax.fori_loop(0, pair & 31, list_piece, filled)

    filled = lax.fori_loop(0, 32 * ngroup, list_chunk, 0)
    for extra in range(BATCH):
        work[filled + extra] = 2048
    lines = lax.broadcasted_iota(jnp.int32, (GROUP_ROWS, 2 * LANES), 0)
    columns = lax.broadcasted_iota(jnp.int32, (LANES, 2 * LANES), 0)

    def one_batch(batch, carry):
        sums, bases = [], []
        for piece in range(BATCH):
            item = work[batch * BATCH + piece]
            chunk = item >> 12
            base = pl.multiple_of(item & 4095, 8)
            cell = jnp.concatenate([keys_scratch[side, pl.ds(chunk, 1), :] for side in range(2)], axis=1)
            load = jnp.concatenate([loads_scratch[side, pl.ds(chunk, 1), :] for side in range(2)], axis=1)
            coarse = load.astype(jnp.bfloat16).astype(jnp.float32)
            here = ((cell >> 7) - base) == lines
            left = jnp.concatenate(
                [
                    jnp.where(here, coarse, 0.0).astype(jnp.bfloat16),
                    jnp.where(here, load - coarse, 0.0).astype(jnp.bfloat16),
                ],
                axis=0,
            )
            right = jnp.where((cell & (LANES - 1)) == columns, 1.0, 0.0).astype(jnp.bfloat16)
            both = lax.dot_general(
                left, right, (((1,), (1,)), ((), ())), preferred_element_type=jnp.float32
            )
            sums.append(both[:GROUP_ROWS] + both[GROUP_ROWS:])
            bases.append(base)
        for total, base in zip(sums, bases):
            grid[pl.ds(base, GROUP_ROWS), :] += total
        return carry

    lax.fori_loop(0, (filled + BATCH - 1) // BATCH, one_batch, 0)


BATCH = 16
TOGETHER = 4


def surface_and_send(positions, normals, tension, edge_weight, owners, cells, connectivity):
    nowner = lax.axis_size(("gx", "gy", "gz"))
    vmem = pl.BlockSpec(memory_space=pltpu.VMEM)
    arrays = (positions, normals, tension, edge_weight, owners, cells, connectivity)
    return pl.pallas_call(
        surface_kernel,
        name="surface",
        out_shape=(
            jax.ShapeDtypeStruct(positions.shape, jnp.float32),
            jax.ShapeDtypeStruct((nowner, 4, LANES), jnp.float32),
        ),
        in_specs=[pl.BlockSpec(memory_space=pltpu.HBM)] * len(arrays),
        out_specs=(vmem, pl.BlockSpec(memory_space=pltpu.HBM)),
        scratch_shapes=[pltpu.VMEM(array.shape, array.dtype) for array in arrays]
        + [
            pltpu.VMEM((3, LANES), jnp.float32),
            pltpu.VMEM((3, LANES), jnp.float32),
            pltpu.VMEM((nowner, 4, LANES), jnp.float32),
            pltpu.VMEM((8, positions.shape[1] + LANES), jnp.float32),
            pltpu.VMEM((positions.shape[1] // LANES, LANES), jnp.float32),
            pltpu.VMEM((128, LANES), jnp.float32),
            pltpu.VMEM((144, LANES), jnp.float32),
            pltpu.VMEM((nowner, LANES), jnp.int32),
            pltpu.VMEM((8, LANES), jnp.int32),
            pltpu.SMEM((8, LANES), jnp.int32),
            pltpu.SemaphoreType.DMA((7,)),
            pltpu.SemaphoreType.DMA,
            pltpu.SemaphoreType.DMA((2,)),
            pltpu.SemaphoreType.DMA((2,)),
            pltpu.SemaphoreType.DMA,
            pltpu.SemaphoreType.DMA,
        ],
        compiler_params=pltpu.CompilerParams(
            vmem_limit_bytes=VMEM_BYTES, collective_id=1, has_side_effects=True
        ),
    )(*arrays)


def spread_cells(got, force, ncell):
    vmem = pl.BlockSpec(memory_space=pltpu.VMEM)
    return pl.pallas_call(
        spread_kernel,
        name="spread",
        out_shape=(
            jax.ShapeDtypeStruct((ncell // LANES + 128, LANES), jnp.float32),
            jax.ShapeDtypeStruct(force.shape, jnp.float32),
        ),
        in_specs=[vmem, vmem],
        out_specs=(vmem, vmem),
        scratch_shapes=[
            pltpu.VMEM((2, 128, LANES), jnp.int32),
            pltpu.VMEM((2, 128, LANES), jnp.float32),
            pltpu.VMEM((128, LANES), jnp.float32),
            pltpu.VMEM((8, LANES), jnp.int32),
            pltpu.SMEM((8, LANES), jnp.int32),
            pltpu.SMEM((512,), jnp.int32),
            pltpu.SemaphoreType.DMA,
        ],
        cost_estimate=pl.CostEstimate(flops=10**10, bytes_accessed=10**7, transcendentals=0),
        compiler_params=pltpu.CompilerParams(vmem_limit_bytes=32 * 1024 * 1024),
    )(got, force)


AXES = ("gx", "gy", "gz")


def halo_copies(sides, slot, send_sems, recv_sems):
    copies = []
    for which, (axis, step, source, target) in enumerate(sides):
        here = lax.axis_index(axis)
        there = here + step
        back = here - step
        size = lax.axis_size(axis)
        copy = pltpu.make_async_remote_copy(
            src_ref=source,
            dst_ref=target,
            send_sem=send_sems.at[slot, which],
            recv_sem=recv_sems.at[slot, which],
            device_id={axis: there},
            device_id_type=pl.DeviceIdType.MESH,
        )
        copies.append((copy, (there >= 0) & (there < size), (back >= 0) & (back < size)))
    return copies


def cycle_kernel(
    plane_rows, added_ref, rhs_ref, shift_ref, pressure_ref, forcing_ref,
    wide_a, wide_b, coarse_a, coarse_b, inverse, update, coarse_rhs, coarse_inverse, coarse_update,
    rows_out, rows_in, columns_out, columns_in, send_sems, recv_sems,
):
    width = forcing_ref.shape[1]
    nplane = forcing_ref.shape[0] // plane_rows
    ncoarse = nplane // 2
    tiles = plane_rows // 8
    wide, coarse = (wide_a, wide_b), (coarse_a, coarse_b)
    blank = jnp.zeros((plane_rows, width), jnp.float32)
    for slot in range(2):
        wide[slot][0:plane_rows, :] = blank
        wide[slot][(nplane + 1) * plane_rows : (nplane + 2) * plane_rows, :] = blank
        coarse[slot][0:plane_rows, :] = blank
        coarse[slot][(ncoarse + 1) * plane_rows : (ncoarse + 2) * plane_rows, :] = blank
        for side in range(2):
            rows_in[slot, side] = jnp.zeros(rows_in.shape[2:], jnp.float32)
            columns_in[slot, side] = jnp.zeros(columns_in.shape[2:], jnp.float32)

    barrier = pltpu.get_barrier_semaphore()
    neighbours = 0
    for axis in AXES:
        here, size = lax.axis_index(axis), lax.axis_size(axis)
        for step in (-1, 1):
            there = here + step
            exists = (there >= 0) & (there < size)
            neighbours = neighbours + exists.astype(jnp.int32)

            @pl.when(exists)
            def _():
                pl.semaphore_signal(
                    barrier, inc=1, device_id={axis: there}, device_id_type=pl.DeviceIdType.MESH
                )


    lane = lax.broadcasted_iota(jnp.int32, (8, LANES), 1)

    def columns_of(field, plane, slot, low, high):
        rows_out[slot, 0, pl.ds(plane, 1), :] = field[0:1, :]
        rows_out[slot, 1, pl.ds(plane, 1), :] = field[plane_rows - 1 : plane_rows, :]
        for tile in range(tiles):
            rows = slice(8 * tile, 8 * tile + 8)
            mine = lane == plane * tiles + tile
            first = pick(field[rows, 0:LANES], jnp.zeros((8, LANES), jnp.int32), 1)
            last = pick(field[rows, width - LANES : width], jnp.full((8, LANES), LANES - 1, jnp.int32), 1)
            low = jnp.where(mine, first, low)
            high = jnp.where(mine, last, high)
        return low, high

    def exchange_faces(field, count, slot, low, high):
        columns_out[slot, 0] = low
        columns_out[slot, 1] = high
        here = pl.ds(0, count)

        def planes(first):
            return field.at[pl.ds(first * plane_rows, plane_rows), :]

        sides = (
            ("gx", -1, planes(1), planes(count + 1)),
            ("gx", 1, planes(count), planes(0)),
            ("gy", -1, rows_out.at[slot, 0, here], rows_in.at[slot, 1, here]),
            ("gy", 1, rows_out.at[slot, 1, here], rows_in.at[slot, 0, here]),
            ("gz", -1, columns_out.at[slot, 0], columns_in.at[slot, 1]),
            ("gz", 1, columns_out.at[slot, 1], columns_in.at[slot, 0]),
        )
        copies = halo_copies(sides, slot, send_sems, recv_sems)
        for copy, sends, receives in copies:
            pl.when(sends)(copy.start)
        for copy, sends, receives in copies:
            pl.when(sends)(copy.wait_send)
            pl.when(receives)(copy.wait_recv)

    row_index = lax.broadcasted_iota(jnp.int32, (plane_rows, width), 0)
    lane_index = lax.broadcasted_iota(jnp.int32, (plane_rows, LANES), 1)

    def beside(field, plane, slot, reach):
        first = pl.multiple_of((plane + 1) * plane_rows, plane_rows)
        centre_plane = field[pl.ds(first, plane_rows), :]
        total = field[pl.ds(first - plane_rows, plane_rows), :] + field[pl.ds(first + plane_rows, plane_rows), :]
        above = rows_in[slot, 0, pl.ds(plane, 1), :]
        below = rows_in[slot, 1, pl.ds(plane, 1), :]
        total = total + jnp.where(row_index < reach, above, pltpu.roll(centre_plane, reach, 0))
        total = total + jnp.where(
            row_index >= plane_rows - reach, below, pltpu.roll(centre_plane, plane_rows - reach, 0)
        )
        spread_low, spread_high = [], []
        for tile in range(tiles):
            where = jnp.full((8, LANES), plane * tiles + tile, jnp.int32)
            spread_low.append(pick(columns_in[slot, 0], where, 1))
            spread_high.append(pick(columns_in[slot, 1], where, 1))
        left = pltpu.roll(centre_plane, reach, 1)
        right = pltpu.roll(centre_plane, width - reach, 1)
        left_edge = jnp.where(lane_index < reach, jnp.concatenate(spread_low, axis=0), left[:, :LANES])
        right_edge = jnp.where(
            lane_index >= LANES - reach, jnp.concatenate(spread_high, axis=0), right[:, width - LANES :]
        )
        total = total + jnp.concatenate([left_edge, left[:, LANES:]], axis=1)
        total = total + jnp.concatenate([right[:, : width - LANES], right_edge], axis=1)
        return centre_plane, total

    def rows_of(plane):
        return pl.ds(pl.multiple_of(plane * plane_rows, plane_rows), plane_rows)

    nothing = jnp.zeros((8, LANES), jnp.float32)

    def each_plane(count, step):
        return lax.fori_loop(0, count, step, (nothing, nothing), unroll=8)

    def sweep(source, target, slot, count, reach, rhs, scale, change, keep, gain, out=None):
        def step(plane, carry):
            here = rows_of(plane)
            field, total = beside(source, plane, slot, reach)
            remain = scale[here, :] * (rhs[here, :] + total) - field
            moved = gain * remain
            if keep:
                moved = moved + keep * change[here, :]
            answer = field + moved
            if out is not None:
                out[here, :] = answer
                return carry
            change[here, :] = moved
            target[rows_of(plane + 1), :] = answer
            return columns_of(answer, plane, 1 - slot, *carry)

        return each_plane(count, step)

    ratio = centre / spread
    gains, factor = [], 1.0 / ratio
    for _ in range(COARSE_SMOOTH):
        factor_new = 1.0 / (2.0 * ratio - factor)
        gains.append((factor_new * factor, 2.0 * factor_new / spread))
        factor = factor_new

    def first_step(plane, carry):
        here = rows_of(plane)
        scale = 1.0 / (6.0 + shift_ref[here, :])
        inverse[here, :] = scale
        added = [added_ref[rows_of(part * nplane + plane), :] for part in range(width // LANES)]
        forcing = rhs_ref[here, :] + jnp.concatenate(added, axis=1)
        forcing_ref[here, :] = forcing
        answer = scale * forcing * (1.0 / centre)
        update[here, :] = answer
        wide_a[rows_of(plane + 1), :] = answer
        return columns_of(answer, plane, 0, *carry)

    edges = each_plane(nplane, first_step)
    slot = 0
    pl.semaphore_wait(barrier, neighbours)
    exchange_faces(wide[slot], nplane, slot, *edges)
    for sweep_index in range(SMOOTH - 1):
        keep, gain = gains[sweep_index]
        edges = sweep(
            wide[slot], wide[1 - slot], slot, nplane, 1, forcing_ref, inverse, update, keep, gain
        )
        slot = 1 - slot
        exchange_faces(wide[slot], nplane, slot, *edges)
    smooth = wide[slot]

    lane_pair = lax.broadcasted_iota(jnp.int32, (8, LANES), 1) ^ 1
    line_pair = lax.broadcasted_iota(jnp.int32, (8, LANES), 0) ^ 1

    def pair_sum(value):
        lines = []
        for tile in range(tiles):
            parts = []
            for part in range(width // LANES):
                block = value[8 * tile : 8 * tile + 8, part * LANES : (part + 1) * LANES]
                block = block + pick(block, lane_pair, 1)
                parts.append(block + pick(block, line_pair, 0))
            lines.append(jnp.concatenate(parts, axis=1))
        return jnp.concatenate(lines, axis=0)

    smooth_slot = slot
    slot = 1 - slot

    def restrict(plane, carry):
        remains, shifts = None, None
        for half in range(2):
            fine = 2 * plane + half
            here = rows_of(fine)
            field, total = beside(smooth, fine, smooth_slot, 1)
            shift = shift_ref[here, :]
            remain = forcing_ref[here, :] - ((6.0 + shift) * field - total)
            remains = remain if remains is None else remains + remain
            shifts = shift if shifts is None else shifts + shift
        rhs = 0.5 * pair_sum(remains)
        scale = 1.0 / (6.0 + 0.5 * pair_sum(shifts))
        answer = scale * rhs * (1.0 / centre)
        here = rows_of(plane)
        coarse_rhs[here, :] = rhs
        coarse_inverse[here, :] = scale
        coarse_update[here, :] = answer
        coarse[slot][rows_of(plane + 1), :] = answer
        return columns_of(answer, plane, slot, *carry)

    edges = each_plane(ncoarse, restrict)
    for sweep_index in range(COARSE_SMOOTH - 1):
        exchange_faces(coarse[slot], ncoarse, slot, *edges)
        keep, gain = gains[sweep_index]
        edges = sweep(
            coarse[slot], coarse[1 - slot], slot, ncoarse, 2,
            coarse_rhs, coarse_inverse, coarse_update, keep, gain,
        )
        slot = 1 - slot
    fix = coarse[slot]

    def begin_again(plane, carry):
        here = rows_of(plane + 1)
        answer = smooth[here, :] + fix[rows_of(lax.div(plane, 2) + 1), :]
        wide[slot][here, :] = answer
        return columns_of(answer, plane, slot, *carry)

    edges = each_plane(nplane, begin_again)
    for sweep_index in range(SMOOTH):
        exchange_faces(wide[slot], nplane, slot, *edges)
        keep, gain = gains[sweep_index - 1] if sweep_index else (0.0, 1.0 / centre)
        edges = sweep(
            wide[slot], wide[1 - slot], slot, nplane, 1, forcing_ref, inverse, update, keep, gain,
            pressure_ref if sweep_index == SMOOTH - 1 else None,
        )
        slot = 1 - slot


def multigrid(added, pressure_rhs, shift_diag):
    planes, rows, width = shift_diag.shape
    vmem = pl.BlockSpec(memory_space=pltpu.VMEM)
    flat = (planes * rows, width)
    half = (planes // 2 * rows, width)
    f32 = jnp.float32
    return pl.pallas_call(
        functools.partial(cycle_kernel, rows),
        name="multigrid",
        out_shape=jax.ShapeDtypeStruct(flat, f32),
        in_specs=[vmem] * 3,
        out_specs=vmem,
        scratch_shapes=[
            pltpu.VMEM(flat, f32),
            pltpu.VMEM((flat[0] + 2 * rows, width), f32),
            pltpu.VMEM((flat[0] + 2 * rows, width), f32),
            pltpu.VMEM((half[0] + 2 * rows, width), f32),
            pltpu.VMEM((half[0] + 2 * rows, width), f32),
            pltpu.VMEM(flat, f32),
            pltpu.VMEM(flat, f32),
            pltpu.VMEM(half, f32),
            pltpu.VMEM(half, f32),
            pltpu.VMEM(half, f32),
            pltpu.VMEM((2, 2, planes, width), f32),
            pltpu.VMEM((2, 2, planes, width), f32),
            pltpu.VMEM((2, 2, 8, LANES), f32),
            pltpu.VMEM((2, 2, 8, LANES), f32),
            pltpu.SemaphoreType.DMA((2, 6)),
            pltpu.SemaphoreType.DMA((2, 6)),
        ],
        compiler_params=pltpu.CompilerParams(
            vmem_limit_bytes=40 * 1024 * 1024, collective_id=0, has_side_effects=True
        ),
    )(added, pressure_rhs.reshape(flat), shift_diag.reshape(flat)).reshape(shift_diag.shape)


def body(
    pressure_rhs,
    shift_diag,
    positions,
    normals,
    tension,
    edge_weight,
    owner_map,
    cell_map,
    connectivity,
):
    ndevice = lax.axis_size(("gx", "gy", "gz"))
    nrow = positions.shape[1] // LANES
    force, got = surface_and_send(
        positions,
        normals,
        tension.reshape(nrow, LANES),
        edge_weight,
        owner_map.reshape(nrow, LANES),
        cell_map.reshape(nrow, LANES),
        connectivity,
    )
    added, surface_force = spread_cells(got.reshape(4 * ndevice, LANES), force, pressure_rhs.size)
    pressure = multigrid(added, pressure_rhs, shift_diag)
    return (pressure, surface_force)


def solution(mesh):
    return jax.shard_map(
        body,
        mesh=mesh,
        in_specs=(
            P("gx", "gy", "gz"),
            P("gx", "gy", "gz"),
            P(None, ("gx", "gy", "gz")),
            P(None, ("gx", "gy", "gz")),
            P(("gx", "gy", "gz")),
            P(None, ("gx", "gy", "gz")),
            P(("gx", "gy", "gz"), None),
            P(("gx", "gy", "gz")),
            P(None, ("gx", "gy", "gz")),
        ),
        out_specs=(P("gx", "gy", "gz"), P(None, ("gx", "gy", "gz"))),
        check_vma=False,
    )
```

```python
import functools
import jax
import jax.numpy as jnp
from jax import lax
from jax.experimental import pallas as pl
from jax.experimental.pallas import tpu as pltpu
from jax.sharding import PartitionSpec as P

HALO = 64
SMOOTH = 3
COARSE_SMOOTH = 4


centre = 1.125
spread = 0.875


LANES = 128
BIG = 524288.0
GROUP_ROWS = 80
CELL_BITS = 18


def permute(value, lane_xor, sub_xor):
    if sub_xor:
        where = lax.broadcasted_iota(jnp.int32, value.shape, 0) ^ sub_xor
        value = pick(value, where, 0)
    if lane_xor:
        where = lax.broadcasted_iota(jnp.int32, value.shape, 1) ^ lane_xor
        value = pick(value, where, 1)
    return value


def pick(value, where, axis):
    numbers = lax.GatherDimensionNumbers(
        offset_dims=(),
        collapsed_slice_dims=(axis,),
        start_index_map=(axis,),
        operand_batching_dims=(1 - axis,),
        start_indices_batching_dims=(1 - axis,),
    )
    return lax.gather(
        value,
        where[:, :, None],
        numbers,
        (1, 1),
        mode=lax.GatherScatterMode.PROMISE_IN_BOUNDS,
    )


def exchange(keys, loads, places, bits, top):
    lane_xor = sub_xor = row_xor = 0
    for bit in bits:
        kind, amount = places[bit]
        lane_xor |= amount if kind == "l" else 0
        sub_xor |= amount if kind == "s" else 0
        row_xor |= amount if kind == "v" else 0
    top_kind, top_amount = places[top]
    count = len(keys)
    new_keys, new_loads = [None] * count, [None] * count
    if top_kind == "v":
        for a in range(count):
            if a & top_amount:
                continue
            b = a ^ row_xor
            low, high, low_load, high_load = keys[a], keys[b], loads[a], loads[b]
            stored = b
            if lane_xor or sub_xor:
                high = permute(high, lane_xor, sub_xor)
                high_load = permute(high_load, lane_xor, sub_xor)
                stored = a | top_amount
            swap = low > high
            new_keys[a] = jnp.minimum(low, high)
            new_keys[stored] = jnp.maximum(low, high)
            new_loads[a] = jnp.where(swap, high_load, low_load)
            new_loads[stored] = jnp.where(swap, low_load, high_load)
        return new_keys, new_loads
    axis = 1 if top_kind == "l" else 0
    upper = (lax.broadcasted_iota(jnp.int32, keys[0].shape, axis) & top_amount) != 0
    for a in range(count):
        b = a ^ row_xor
        other = permute(keys[b], lane_xor, sub_xor)
        other_load = permute(loads[b], lane_xor, sub_xor)
        best = jnp.where(upper, jnp.maximum(keys[a], other), jnp.minimum(keys[a], other))
        new_keys[a] = best
        new_loads[a] = jnp.where(best == keys[a], loads[a], other_load)
    return new_keys, new_loads


def merge_levels(groups, places, first, last):
    for level in range(first, last + 1):
        groups = [exchange(*group, places, range(level + 1), level) for group in groups]
        for bit in reversed(range(level)):
            groups = [exchange(*group, places, (bit,), bit) for group in groups]
    return groups


VMEM_BYTES = 67043328


def device_of(index):
    ny, nz = lax.axis_size("gy"), lax.axis_size("gz")
    return {"gx": index // (ny * nz), "gy": (index // nz) % ny, "gz": index % nz}


def surface_kernel(
    positions_hbm, normals_hbm, tension_hbm, weight_hbm, owner_hbm, cell_hbm, connect_hbm,
    force_ref, got_ref,
    positions_ref, normals_ref, tension_ref, weight_ref, owner_ref, cell_ref, connect_ref,
    low_ref, high_ref, packed_ref, wide, jumps, turned, lists, below_ref, counted, counted_scalar,
    load_sems, sem, edge_send, edge_recv, all_send, all_recv,
):
    npoint = positions_ref.shape[1]
    nrow = npoint // LANES
    nowner = packed_ref.shape[0]
    total = npoint * nowner
    me = lax.axis_index(("gx", "gy", "gz"))
    begin = me * npoint
    sources = (positions_hbm, connect_hbm, weight_hbm, normals_hbm, tension_hbm, owner_hbm, cell_hbm)
    targets = (positions_ref, connect_ref, weight_ref, normals_ref, tension_ref, owner_ref, cell_ref)
    reads = [
        pltpu.make_async_copy(source, target, load_sems.at[which])
        for which, (source, target) in enumerate(zip(sources, targets))
    ]
    for read in reads:
        read.start()

    barrier = pltpu.get_barrier_semaphore()

    def greet(offset, carry):
        pl.semaphore_signal(
            barrier, inc=1, device_id=device_of((me + offset) % nowner),
            device_id_type=pl.DeviceIdType.MESH,
        )
        return carry

    lax.fori_loop(1, nowner, greet, 0)
    for read in reads:
        read.wait()

    half = lax.broadcasted_iota(jnp.int32, (3, LANES), 1) < HALO
    first_block = pltpu.roll(positions_ref[:, 0:LANES], HALO, 1)
    before = first_block
    for row in range(1, nrow):
        after = pltpu.roll(positions_ref[:, row * LANES : (row + 1) * LANES], HALO, 1)
        wide[0:3, row * LANES : (row + 1) * LANES] = jnp.where(half, before, after)
        before = after
    last_block = before

    def one_row(row, carry):
        at = row * LANES if isinstance(row, int) else pl.multiple_of(row * LANES, LANES)
        here, there = pl.ds(at, LANES), pl.ds(at + LANES, LANES)
        blank = jnp.zeros((2, LANES), jnp.int32)
        index = jnp.concatenate([connect_ref[:, here], blank], axis=0)
        index = ((index - begin + HALO) & (total - 1)) - at
        weight = jnp.concatenate([weight_ref[:, here], blank.astype(jnp.float32)], axis=0)
        second = index >= LANES
        index = index & (LANES - 1)
        strength = tension_ref[pl.ds(row, 1), :]
        jump = jnp.zeros((1, LANES), jnp.float32)
        for axis in range(3):
            lower = jnp.broadcast_to(wide[axis : axis + 1, here], (8, LANES))
            upper = jnp.broadcast_to(wide[axis : axis + 1, there], (8, LANES))
            taken = jnp.where(second, pick(upper, index, 1), pick(lower, index, 1))
            pulled = weight * (taken - positions_ref[axis : axis + 1, here])
            force = strength * jnp.sum(pulled, axis=0, keepdims=True)
            force_ref[axis : axis + 1, here] = force
            jump = jump + force * normals_ref[axis : axis + 1, here]
        jumps[pl.ds(row, 1), :] = jump
        return carry

    lax.fori_loop(0, (nrow - 2) // 2, lambda i, c: one_row(2 * i + 2, one_row(2 * i + 1, c)), 0, unroll=4)

    pl.semaphore_wait(barrier, nowner - 1)
    edges = (
        (positions_ref.at[:, pl.ds(npoint - LANES, LANES)], low_ref, 1),
        (positions_ref.at[:, pl.ds(0, LANES)], high_ref, nowner - 1),
    )
    sends = []
    for which, (source, target, offset) in enumerate(edges):
        sends.append(
            pltpu.make_async_remote_copy(
                src_ref=source, dst_ref=target,
                send_sem=edge_send.at[which], recv_sem=edge_recv.at[which],
                device_id=device_of((me + offset) % nowner), device_id_type=pl.DeviceIdType.MESH,
            )
        )
    for send in sends:
        send.start()

    ranks = lax.broadcasted_iota(jnp.int32, (nowner, LANES), 0)

    def count_row(row, below):
        names = owner_ref[pl.ds(row, 1), :]
        return below + jnp.where(names < ranks, 1, 0)

    below = lax.fori_loop(0, nrow, count_row, jnp.zeros((nowner, LANES), jnp.int32), unroll=4)
    for bit in range(7):
        below = below + pltpu.roll(below, 1 << bit, 1)
    below_ref[...] = below
    counted[...] = jnp.transpose(below_ref[...])[0:8, :]
    fetch = pltpu.make_async_copy(counted, counted_scalar, sem)

    keys, loads = [], []
    for tile in range(nrow // 8):
        rows = slice(8 * tile, 8 * tile + 8)
        cell = cell_ref[rows, :]
        cell = ((cell & 384) << 9) | ((cell >> 9) << 7) | (cell & 127)
        key = ((owner_ref[rows, :] << CELL_BITS) | cell) << 1
        load = jumps[rows, :]
        if tile in (0, nrow // 8 - 1):
            line = lax.broadcasted_iota(jnp.int32, (8, LANES), 0)
            lane = lax.broadcasted_iota(jnp.int32, (8, LANES), 1)
            late = line == (7 if tile else 0)
            key = key | jnp.where(late, 1, 0)
            load = jnp.where(late, (lane + (LANES if tile else 0)).astype(jnp.float32), load)
        keys.append(key)
        loads.append(load)
    fetch.start()
    places = [("v", 1), ("v", 2), ("v", 4), ("s", 1), ("s", 2), ("s", 4)]
    places += [("l", 1 << bit) for bit in range(7)]
    ((keys, loads),) = merge_levels([(keys, loads)], places, 0, 12)
    for send in sends:
        send.wait()
    wide[0:3, 0:LANES] = jnp.where(half, pltpu.roll(low_ref[...], HALO, 1), first_block)
    wide[0:3, npoint : npoint + LANES] = jnp.where(half, last_block, pltpu.roll(high_ref[...], HALO, 1))
    one_row(0, 0)
    one_row(nrow - 1, 0)

    first_jumps = jnp.broadcast_to(jumps[0:1, :], (8, LANES))
    last_jumps = jnp.broadcast_to(jumps[nrow - 1 : nrow, :], (8, LANES))
    for tile in range(nrow // 8):
        late = (keys[tile] & 1) == 1
        which = jnp.where(late, loads[tile], 0.0).astype(jnp.int32)
        lane = which & (LANES - 1)
        value = jnp.where(which >= LANES, pick(last_jumps, lane, 1), pick(first_jumps, lane, 1))
        loads[tile] = jnp.where(late, value, loads[tile])
        keys[tile] = keys[tile] >> 1
    for which, arrays in ((0, keys), (1, loads)):
        for tile in range(8):
            value = arrays[tile]
            if which == 0:
                value = (value & ((1 << CELL_BITS) - 1)).astype(jnp.float32)
            turned[pl.ds(tile, 8, stride=8), :] = value
        turned[64:128, :] = jnp.zeros((64, LANES), jnp.float32)
        flipped = jnp.transpose(turned[...])
        turned[...] = flipped
        even = turned[pl.ds(0, 64, stride=2), :]
        odd = pltpu.roll(turned[pl.ds(1, 64, stride=2), :], 64, 1)
        lane = lax.broadcasted_iota(jnp.int32, (64, LANES), 1)
        lists[pl.ds(which, 64, stride=2), :] = jnp.where(lane < 64, even, odd)
    lists[128:144, :] = jnp.zeros((16, LANES), jnp.float32)
    fetch.wait()

    lane = lax.broadcasted_iota(jnp.int32, (8, LANES), 1)
    line = lax.broadcasted_iota(jnp.int32, (8, LANES), 0)
    slot = lane + LANES * (line >> 1)
    filler = jnp.where((line & 1) == 0, BIG, 0.0).astype(jnp.float32)

    def one_owner(owner, carry):
        start = counted_scalar[0, owner]
        following = jnp.where(owner == nowner - 1, npoint, counted_scalar[0, jnp.minimum(owner + 1, nowner - 1)])
        shift = start & (LANES - 1)
        block = lists[pl.ds((start >> 7) * 2, 8), :]
        block = pltpu.roll(block, (LANES - shift) & (LANES - 1), 1)
        block = jnp.where(lane < LANES - shift, block, pltpu.roll(block, 6, 0))
        block = jnp.where(slot < following - start, block, filler)
        packed_ref[owner] = block[0:4, :]
        return carry

    lax.fori_loop(0, nowner, one_owner, 0, unroll=8)

    def send_one(offset, carry):
        other = (me + offset) % nowner
        pltpu.make_async_remote_copy(
            src_ref=packed_ref.at[other], dst_ref=got_ref.at[me],
            send_sem=all_send, recv_sem=all_recv,
            device_id=device_of(other), device_id_type=pl.DeviceIdType.MESH,
        ).start()
        return carry

    lax.fori_loop(1, nowner, send_one, 0)
    keep = pltpu.make_async_copy(packed_ref.at[me], got_ref.at[me], sem)
    keep.start()
    everything = pltpu.make_async_remote_copy(
        src_ref=packed_ref.at[pl.ds(0, nowner - 1)], dst_ref=got_ref.at[pl.ds(0, nowner - 1)],
        send_sem=all_send, recv_sem=all_recv,
        device_id=device_of((me + 1) % nowner), device_id_type=pl.DeviceIdType.MESH,
    )
    everything.wait_send()
    everything.wait_recv()
    keep.wait()


def spread_kernel(
    got_ref, force_in, grid, force_ref,
    keys_scratch, loads_scratch, turned, bounds, bounds_scalar, work, sem,
):
    force_ref[...] = force_in[...]
    nsender = got_ref.shape[0] // 4
    ngroup = nsender // 32
    places = [("l", 1 << bit) for bit in range(7)] + [("v", 1), ("v", 2), ("v", 4)]
    places += [("s", 1), ("s", 2), ("s", 4)]

    def zero(step, carry):
        grid[pl.ds(pl.multiple_of(step * 64, 64), 64), :] = jnp.zeros((64, LANES), jnp.float32)
        return carry

    lax.fori_loop(0, grid.shape[0] // 64, zero, 0)

    def read_group(group):
        keys, loads = [], []
        for quarter in range(4):
            for side in range(2):
                first = (group * 32 + quarter * 8) * 4 + 2 * side
                keys.append(got_ref[pl.ds(first, 8, stride=4), :])
                loads.append(got_ref[pl.ds(first + 1, 8, stride=4), :])
        return keys, loads

    def store_group(group, keys, loads):
        for quarter in range(4):
            rows = pl.ds(group * 32 + quarter, 8, stride=4)
            last = jnp.full((8, 1), -1, jnp.int32)
            base = None
            for side in range(2):
                key = keys[2 * quarter + side]
                columns = slice(side * LANES, (side + 1) * LANES)
                cell = key.astype(jnp.int32)
                keys_scratch[side, rows, :] = cell
                loads_scratch[side, rows, :] = loads[2 * quarter + side]
                inside = key < BIG
                line = (cell >> 7).astype(jnp.float32)
                top = jnp.max(jnp.where(inside, line, -1.0), axis=1, keepdims=True)
                last = jnp.maximum(last, top.astype(jnp.int32))
                if side == 0:
                    base = jnp.min(line, axis=1, keepdims=True).astype(jnp.int32) & -8
            repeats = jnp.where(last < 0, 0, (((last - base) * 52429) >> 22) + 1)
            pair = jnp.where(last < 0, 0, base) * 32 + repeats
            turned[rows, :] = jnp.broadcast_to(pair.astype(jnp.float32), (8, LANES))

    for first in range(0, ngroup, TOGETHER):
        chosen = range(first, first + TOGETHER)
        merged = merge_levels([read_group(group) for group in chosen], places, 8, 12)
        for group, (keys, loads) in zip(chosen, merged):
            store_group(group, keys, loads)
    bounds[...] = jnp.transpose(turned[...])[0:8, :].astype(jnp.int32)
    fetch = pltpu.make_async_copy(bounds, bounds_scalar, sem)
    fetch.start()
    fetch.wait()

    def list_chunk(chunk, filled):
        pair = bounds_scalar[0, chunk]
        base = pair >> 5

        def list_piece(piece, filled):
            work[filled] = (chunk << 12) | (base + piece * GROUP_ROWS)
            return filled + 1

        return lax.fori_loop(0, pair & 31, list_piece, filled)

    filled = lax.fori_loop(0, 32 * ngroup, list_chunk, 0)
    for extra in range(BATCH):
        work[filled + extra] = 2048
    lines = lax.broadcasted_iota(jnp.int32, (GROUP_ROWS, 2 * LANES), 0)
    columns = lax.broadcasted_iota(jnp.int32, (LANES, 2 * LANES), 0)

    def one_batch(batch, carry):
        sums, bases = [], []
        for piece in range(BATCH):
            item = work[batch * BATCH + piece]
            chunk = item >> 12
            base = pl.multiple_of(item & 4095, 8)
            cell = jnp.concatenate([keys_scratch[side, pl.ds(chunk, 1), :] for side in range(2)], axis=1)
            load = jnp.concatenate([loads_scratch[side, pl.ds(chunk, 1), :] for side in range(2)], axis=1)
            coarse = load.astype(jnp.bfloat16).astype(jnp.float32)
            here = ((cell >> 7) - base) == lines
            left = jnp.concatenate(
                [
                    jnp.where(here, coarse, 0.0).astype(jnp.bfloat16),
                    jnp.where(here, load - coarse, 0.0).astype(jnp.bfloat16),
                ],
                axis=0,
            )
            right = jnp.where((cell & (LANES - 1)) == columns, 1.0, 0.0).astype(jnp.bfloat16)
            both = lax.dot_general(
                left, right, (((1,), (1,)), ((), ())), preferred_element_type=jnp.float32
            )
            sums.append(both[:GROUP_ROWS] + both[GROUP_ROWS:])
            bases.append(base)
        for total, base in zip(sums, bases):
            grid[pl.ds(base, GROUP_ROWS), :] += total
        return carry

    lax.fori_loop(0, (filled + BATCH - 1) // BATCH, one_batch, 0)


BATCH = 16
TOGETHER = 4


def surface_and_send(positions, normals, tension, edge_weight, owners, cells, connectivity):
    nowner = lax.axis_size(("gx", "gy", "gz"))
    vmem = pl.BlockSpec(memory_space=pltpu.VMEM)
    arrays = (positions, normals, tension, edge_weight, owners, cells, connectivity)
    return pl.pallas_call(
        surface_kernel,
        name="surface",
        out_shape=(
            jax.ShapeDtypeStruct(positions.shape, jnp.float32),
            jax.ShapeDtypeStruct((nowner, 4, LANES), jnp.float32),
        ),
        in_specs=[pl.BlockSpec(memory_space=pltpu.HBM)] * len(arrays),
        out_specs=(vmem, pl.BlockSpec(memory_space=pltpu.HBM)),
        scratch_shapes=[pltpu.VMEM(array.shape, array.dtype) for array in arrays]
        + [
            pltpu.VMEM((3, LANES), jnp.float32),
            pltpu.VMEM((3, LANES), jnp.float32),
            pltpu.VMEM((nowner, 4, LANES), jnp.float32),
            pltpu.VMEM((8, positions.shape[1] + LANES), jnp.float32),
            pltpu.VMEM((positions.shape[1] // LANES, LANES), jnp.float32),
            pltpu.VMEM((128, LANES), jnp.float32),
            pltpu.VMEM((144, LANES), jnp.float32),
            pltpu.VMEM((nowner, LANES), jnp.int32),
            pltpu.VMEM((8, LANES), jnp.int32),
            pltpu.SMEM((8, LANES), jnp.int32),
            pltpu.SemaphoreType.DMA((7,)),
            pltpu.SemaphoreType.DMA,
            pltpu.SemaphoreType.DMA((2,)),
            pltpu.SemaphoreType.DMA((2,)),
            pltpu.SemaphoreType.DMA,
            pltpu.SemaphoreType.DMA,
        ],
        compiler_params=pltpu.CompilerParams(
            vmem_limit_bytes=VMEM_BYTES, collective_id=1, has_side_effects=True
        ),
    )(*arrays)


def spread_cells(got, force, ncell):
    vmem = pl.BlockSpec(memory_space=pltpu.VMEM)
    return pl.pallas_call(
        spread_kernel,
        name="spread",
        out_shape=(
            jax.ShapeDtypeStruct((ncell // LANES + 128, LANES), jnp.float32),
            jax.ShapeDtypeStruct(force.shape, jnp.float32),
        ),
        in_specs=[vmem, vmem],
        out_specs=(vmem, vmem),
        scratch_shapes=[
            pltpu.VMEM((2, 128, LANES), jnp.int32),
            pltpu.VMEM((2, 128, LANES), jnp.float32),
            pltpu.VMEM((128, LANES), jnp.float32),
            pltpu.VMEM((8, LANES), jnp.int32),
            pltpu.SMEM((8, LANES), jnp.int32),
            pltpu.SMEM((512,), jnp.int32),
            pltpu.SemaphoreType.DMA,
        ],
        cost_estimate=pl.CostEstimate(flops=10**10, bytes_accessed=10**7, transcendentals=0),
        compiler_params=pltpu.CompilerParams(vmem_limit_bytes=32 * 1024 * 1024),
    )(got, force)


AXES = ("gx", "gy", "gz")


def halo_copies(sides, slot, send_sems, recv_sems):
    copies = []
    for which, (axis, step, source, target) in enumerate(sides):
        here = lax.axis_index(axis)
        there = here + step
        back = here - step
        size = lax.axis_size(axis)
        copy = pltpu.make_async_remote_copy(
            src_ref=source,
            dst_ref=target,
            send_sem=send_sems.at[slot, which],
            recv_sem=recv_sems.at[slot, which],
            device_id={axis: there},
            device_id_type=pl.DeviceIdType.MESH,
        )
        copies.append((copy, (there >= 0) & (there < size), (back >= 0) & (back < size)))
    return copies


def cycle_kernel(
    plane_rows, added_ref, rhs_ref, shift_ref, pressure_ref, forcing_ref,
    wide_a, wide_b, coarse_a, coarse_b, inverse, update, coarse_rhs, coarse_inverse, coarse_update,
    rows_out, rows_in, columns_out, columns_in, send_sems, recv_sems,
):
    width = forcing_ref.shape[1]
    nplane = forcing_ref.shape[0] // plane_rows
    ncoarse = nplane // 2
    tiles = plane_rows // 8
    wide, coarse = (wide_a, wide_b), (coarse_a, coarse_b)
    blank = jnp.zeros((plane_rows, width), jnp.float32)
    for slot in range(2):
        wide[slot][0:plane_rows, :] = blank
        wide[slot][(nplane + 1) * plane_rows : (nplane + 2) * plane_rows, :] = blank
        coarse[slot][0:plane_rows, :] = blank
        coarse[slot][(ncoarse + 1) * plane_rows : (ncoarse + 2) * plane_rows, :] = blank
        for side in range(2):
            rows_in[slot, side] = jnp.zeros(rows_in.shape[2:], jnp.float32)
            columns_in[slot, side] = jnp.zeros(columns_in.shape[2:], jnp.float32)

    barrier = pltpu.get_barrier_semaphore()
    neighbours = 0
    for axis in AXES:
        here, size = lax.axis_index(axis), lax.axis_size(axis)
        for step in (-1, 1):
            there = here + step
            exists = (there >= 0) & (there < size)
            neighbours = neighbours + exists.astype(jnp.int32)

            @pl.when(exists)
            def _():
                pl.semaphore_signal(
                    barrier, inc=1, device_id={axis: there}, device_id_type=pl.DeviceIdType.MESH
                )


    lane = lax.broadcasted_iota(jnp.int32, (8, LANES), 1)

    def pack_columns(head, tail, plane, low, high):
        for tile in range(tiles):
            rows = slice(8 * tile, 8 * tile + 8)
            mine = lane == plane * tiles + tile
            first = pick(head[rows, :], jnp.zeros((8, LANES), jnp.int32), 1)
            last = pick(tail[rows, :], jnp.full((8, LANES), LANES - 1, jnp.int32), 1)
            low = jnp.where(mine, first, low)
            high = jnp.where(mine, last, high)
        return low, high

    def columns_of(field, plane, slot, low, high):
        rows_out[slot, 0, pl.ds(plane, 1), :] = field[0:1, :]
        rows_out[slot, 1, pl.ds(plane, 1), :] = field[plane_rows - 1 : plane_rows, :]
        return pack_columns(field[:, 0:LANES], field[:, width - LANES : width], plane, low, high)

    def exchange_faces(field, count, slot, low, high):
        columns_out[slot, 0] = low
        columns_out[slot, 1] = high
        here = pl.ds(0, count)

        def planes(first):
            return field.at[pl.ds(first * plane_rows, plane_rows), :]

        sides = (
            ("gx", -1, planes(1), planes(count + 1)),
            ("gx", 1, planes(count), planes(0)),
            ("gy", -1, rows_out.at[slot, 0, here], rows_in.at[slot, 1, here]),
            ("gy", 1, rows_out.at[slot, 1, here], rows_in.at[slot, 0, here]),
            ("gz", -1, columns_out.at[slot, 0], columns_in.at[slot, 1]),
            ("gz", 1, columns_out.at[slot, 1], columns_in.at[slot, 0]),
        )
        copies = halo_copies(sides, slot, send_sems, recv_sems)
        for copy, sends, receives in copies:
            pl.when(sends)(copy.start)

        def finish():
            for copy, sends, receives in copies:
                pl.when(sends)(copy.wait_send)
                pl.when(receives)(copy.wait_recv)

        return finish

    row_index = lax.broadcasted_iota(jnp.int32, (plane_rows, width), 0)
    lane_index = lax.broadcasted_iota(jnp.int32, (plane_rows, LANES), 1)

    def beside(field, plane, count, reach):
        first = (plane + 1) * plane_rows
        if not isinstance(plane, int):
            first = pl.multiple_of(first, plane_rows)
        middle = field[pl.ds(first, plane_rows), :]
        total = jnp.where(row_index < reach, 0.0, pltpu.roll(middle, reach, 0))
        total = total + jnp.where(
            row_index >= plane_rows - reach, 0.0, pltpu.roll(middle, plane_rows - reach, 0)
        )
        if not isinstance(plane, int) or plane > 0:
            total = total + field[pl.ds(first - plane_rows, plane_rows), :]
        if not isinstance(plane, int) or plane < count - 1:
            total = total + field[pl.ds(first + plane_rows, plane_rows), :]
        left = pltpu.roll(middle, reach, 1)
        right = pltpu.roll(middle, width - reach, 1)
        left_edge = jnp.where(lane_index < reach, 0.0, left[:, :LANES])
        right_edge = jnp.where(lane_index >= LANES - reach, 0.0, right[:, width - LANES :])
        total = total + jnp.concatenate([left_edge, left[:, LANES:]], axis=1)
        total = total + jnp.concatenate([right[:, : width - LANES], right_edge], axis=1)
        return middle, total

    def correct(source, target, padding, slot, count, reach, scale, gain, change, packed):
        def apply(first, number, columns, value):
            here, there = pl.ds(first, number), pl.ds(first + padding, number)
            moved = value if scale is None else (gain * scale[here, columns]) * value
            if change is not None:
                change[here, columns] = change[here, columns] + moved
            answer = target[there, columns] + moved
            target[there, columns] = answer
            return answer

        entire, head, tail = slice(0, width), slice(0, LANES), slice(width - LANES, width)
        apply(0, plane_rows, entire, source[0:plane_rows, :])
        apply(
            (count - 1) * plane_rows, plane_rows, entire,
            source[(count + 1) * plane_rows : (count + 2) * plane_rows, :],
        )

        def step(plane, carry):
            base = pl.multiple_of(plane * plane_rows, plane_rows)
            for row in range(reach):
                apply(base + row, 1, entire, rows_in[slot, 0, pl.ds(plane, 1), :])
                apply(base + plane_rows - 1 - row, 1, entire, rows_in[slot, 1, pl.ds(plane, 1), :])
            low, high = [], []
            for tile in range(tiles):
                where = jnp.full((8, LANES), plane * tiles + tile, jnp.int32)
                low.append(pick(columns_in[slot, 0], where, 1))
                high.append(pick(columns_in[slot, 1], where, 1))
            low = jnp.where(lane_index < reach, jnp.concatenate(low, axis=0), 0.0)
            high = jnp.where(lane_index >= LANES - reach, jnp.concatenate(high, axis=0), 0.0)
            first = apply(base, plane_rows, head, low)
            last = apply(base, plane_rows, tail, high)
            if not packed:
                return carry
            for side, row in ((0, 0), (1, plane_rows - 1)):
                rows_out[1 - slot, side, pl.ds(plane, 1), :] = target[pl.ds(base + padding + row, 1), :]
            return pack_columns(first, last, plane, *carry)

        return lax.fori_loop(0, count, step, (nothing, nothing), unroll=8)

    nothing = jnp.zeros((8, LANES), jnp.float32)

    def rows_of(plane):
        if isinstance(plane, int):
            return pl.ds(plane * plane_rows, plane_rows)
        return pl.ds(pl.multiple_of(plane * plane_rows, plane_rows), plane_rows)

    def each_plane(count, step):
        return lax.fori_loop(0, count, step, (nothing, nothing), unroll=8)

    def inner_planes(count, step):
        step(0, 0)
        lax.fori_loop(1, count - 1, step, 0, unroll=(count - 2) // 2)
        step(count - 1, 0)

    def sweep(source, target, slot, edges, count, reach, rhs, scale, change, keep, gain, out=None):
        finish = exchange_faces(source, count, slot, *edges)

        def step(plane, carry):
            here = rows_of(plane)
            field, total = beside(source, plane, count, reach)
            moved = gain * (scale[here, :] * (rhs[here, :] + total) - field)
            if keep:
                moved = moved + keep * change[here, :]
            if out is not None:
                out[here, :] = field + moved
            else:
                change[here, :] = moved
                target[rows_of(plane + 1), :] = field + moved
            return carry

        inner_planes(count, step)
        finish()
        if out is not None:
            return correct(source, out, 0, slot, count, reach, scale, gain, None, False)
        return correct(source, target, plane_rows, slot, count, reach, scale, gain, change, True)

    ratio = centre / spread
    gains, factor = [], 1.0 / ratio
    for _ in range(COARSE_SMOOTH):
        factor_new = 1.0 / (2.0 * ratio - factor)
        gains.append((factor_new * factor, 2.0 * factor_new / spread))
        factor = factor_new

    def first_step(plane, carry):
        here = rows_of(plane)
        scale = 1.0 / (6.0 + shift_ref[here, :])
        inverse[here, :] = scale
        added = [added_ref[rows_of(part * nplane + plane), :] for part in range(width // LANES)]
        forcing = rhs_ref[here, :] + jnp.concatenate(added, axis=1)
        forcing_ref[here, :] = forcing
        answer = scale * forcing * (1.0 / centre)
        update[here, :] = answer
        wide_a[rows_of(plane + 1), :] = answer
        return columns_of(answer, plane, 0, *carry)

    edges = each_plane(nplane, first_step)
    slot = 0
    pl.semaphore_wait(barrier, neighbours)
    for sweep_index in range(SMOOTH - 1):
        keep, gain = gains[sweep_index]
        edges = sweep(
            wide[slot], wide[1 - slot], slot, edges, nplane, 1, forcing_ref, inverse, update, keep, gain
        )
        slot = 1 - slot
    smooth, remains_ref = wide[slot], wide[1 - slot]

    lane_pair = lax.broadcasted_iota(jnp.int32, (8, LANES), 1) ^ 1
    line_pair = lax.broadcasted_iota(jnp.int32, (8, LANES), 0) ^ 1

    def pair_sum(value):
        lines = []
        for tile in range(tiles):
            parts = []
            for part in range(width // LANES):
                block = value[8 * tile : 8 * tile + 8, part * LANES : (part + 1) * LANES]
                block = block + pick(block, lane_pair, 1)
                parts.append(block + pick(block, line_pair, 0))
            lines.append(jnp.concatenate(parts, axis=1))
        return jnp.concatenate(lines, axis=0)

    finish = exchange_faces(smooth, nplane, slot, *edges)

    def leave(plane, carry):
        here = rows_of(plane)
        field, total = beside(smooth, plane, nplane, 1)
        remains_ref[rows_of(plane + 1), :] = forcing_ref[here, :] - ((6.0 + shift_ref[here, :]) * field - total)
        return carry

    inner_planes(nplane, leave)
    finish()
    correct(smooth, remains_ref, plane_rows, slot, nplane, 1, None, 1.0, None, False)
    slot = 1 - slot

    def restrict(plane, carry):
        remains = remains_ref[rows_of(2 * plane + 1), :] + remains_ref[rows_of(2 * plane + 2), :]
        shifts = shift_ref[rows_of(2 * plane), :] + shift_ref[rows_of(2 * plane + 1), :]
        rhs = 0.5 * pair_sum(remains)
        scale = 1.0 / (6.0 + 0.5 * pair_sum(shifts))
        answer = scale * rhs * (1.0 / centre)
        here = rows_of(plane)
        coarse_rhs[here, :] = rhs
        coarse_inverse[here, :] = scale
        coarse_update[here, :] = answer
        coarse[slot][rows_of(plane + 1), :] = answer
        return columns_of(answer, plane, slot, *carry)

    edges = each_plane(ncoarse, restrict)
    for sweep_index in range(COARSE_SMOOTH - 1):
        keep, gain = gains[sweep_index]
        edges = sweep(
            coarse[slot], coarse[1 - slot], slot, edges, ncoarse, 2,
            coarse_rhs, coarse_inverse, coarse_update, keep, gain,
        )
        slot = 1 - slot
    fix = coarse[slot]

    def begin_again(plane, carry):
        here = rows_of(plane + 1)
        answer = smooth[here, :] + fix[rows_of(lax.div(plane, 2) + 1), :]
        wide[slot][here, :] = answer
        return columns_of(answer, plane, slot, *carry)

    edges = each_plane(nplane, begin_again)
    for sweep_index in range(SMOOTH):
        keep, gain = gains[sweep_index - 1] if sweep_index else (0.0, 1.0 / centre)
        edges = sweep(
            wide[slot], wide[1 - slot], slot, edges, nplane, 1, forcing_ref, inverse, update, keep, gain,
            pressure_ref if sweep_index == SMOOTH - 1 else None,
        )
        slot = 1 - slot


def multigrid(added, pressure_rhs, shift_diag):
    planes, rows, width = shift_diag.shape
    vmem = pl.BlockSpec(memory_space=pltpu.VMEM)
    flat = (planes * rows, width)
    half = (planes // 2 * rows, width)
    f32 = jnp.float32
    return pl.pallas_call(
        functools.partial(cycle_kernel, rows),
        name="multigrid",
        out_shape=jax.ShapeDtypeStruct(flat, f32),
        in_specs=[vmem] * 3,
        out_specs=vmem,
        scratch_shapes=[
            pltpu.VMEM(flat, f32),
            pltpu.VMEM((flat[0] + 2 * rows, width), f32),
            pltpu.VMEM((flat[0] + 2 * rows, width), f32),
            pltpu.VMEM((half[0] + 2 * rows, width), f32),
            pltpu.VMEM((half[0] + 2 * rows, width), f32),
            pltpu.VMEM(flat, f32),
            pltpu.VMEM(flat, f32),
            pltpu.VMEM(half, f32),
            pltpu.VMEM(half, f32),
            pltpu.VMEM(half, f32),
            pltpu.VMEM((2, 2, planes, width), f32),
            pltpu.VMEM((2, 2, planes, width), f32),
            pltpu.VMEM((2, 2, 8, LANES), f32),
            pltpu.VMEM((2, 2, 8, LANES), f32),
            pltpu.SemaphoreType.DMA((2, 6)),
            pltpu.SemaphoreType.DMA((2, 6)),
        ],
        compiler_params=pltpu.CompilerParams(
            vmem_limit_bytes=40 * 1024 * 1024, collective_id=0, has_side_effects=True
        ),
    )(added, pressure_rhs.reshape(flat), shift_diag.reshape(flat)).reshape(shift_diag.shape)


def body(
    pressure_rhs,
    shift_diag,
    positions,
    normals,
    tension,
    edge_weight,
    owner_map,
    cell_map,
    connectivity,
):
    ndevice = lax.axis_size(("gx", "gy", "gz"))
    nrow = positions.shape[1] // LANES
    force, got = surface_and_send(
        positions,
        normals,
        tension.reshape(nrow, LANES),
        edge_weight,
        owner_map.reshape(nrow, LANES),
        cell_map.reshape(nrow, LANES),
        connectivity,
    )
    added, surface_force = spread_cells(got.reshape(4 * ndevice, LANES), force, pressure_rhs.size)
    pressure = multigrid(added, pressure_rhs, shift_diag)
    return (pressure, surface_force)


def solution(mesh):
    return jax.shard_map(
        body,
        mesh=mesh,
        in_specs=(
            P("gx", "gy", "gz"),
            P("gx", "gy", "gz"),
            P(None, ("gx", "gy", "gz")),
            P(None, ("gx", "gy", "gz")),
            P(("gx", "gy", "gz")),
            P(None, ("gx", "gy", "gz")),
            P(("gx", "gy", "gz"), None),
            P(("gx", "gy", "gz")),
            P(None, ("gx", "gy", "gz")),
        ),
        out_specs=(P("gx", "gy", "gz"), P(None, ("gx", "gy", "gz"))),
        check_vma=False,
    )
```

```python
import functools
import jax
import jax.numpy as jnp
from jax import lax
from jax.experimental import pallas as pl
from jax.experimental.pallas import tpu as pltpu
from jax.sharding import PartitionSpec as P

HALO = 64
SMOOTH = 3
COARSE_SMOOTH = 4


centre = 1.125
spread = 0.875


LANES = 128
BIG = 524288.0
GROUP_ROWS = 80
CELL_BITS = 18


def permute(value, lane_xor, sub_xor):
    if sub_xor:
        where = lax.broadcasted_iota(jnp.int32, value.shape, 0) ^ sub_xor
        value = pick(value, where, 0)
    if lane_xor:
        where = lax.broadcasted_iota(jnp.int32, value.shape, 1) ^ lane_xor
        value = pick(value, where, 1)
    return value


def pick(value, where, axis):
    numbers = lax.GatherDimensionNumbers(
        offset_dims=(),
        collapsed_slice_dims=(axis,),
        start_index_map=(axis,),
        operand_batching_dims=(1 - axis,),
        start_indices_batching_dims=(1 - axis,),
    )
    return lax.gather(
        value,
        where[:, :, None],
        numbers,
        (1, 1),
        mode=lax.GatherScatterMode.PROMISE_IN_BOUNDS,
    )


def exchange(keys, loads, places, bits, top):
    lane_xor = sub_xor = row_xor = 0
    for bit in bits:
        kind, amount = places[bit]
        lane_xor |= amount if kind == "l" else 0
        sub_xor |= amount if kind == "s" else 0
        row_xor |= amount if kind == "v" else 0
    top_kind, top_amount = places[top]
    count = len(keys)
    new_keys, new_loads = [None] * count, [None] * count
    if top_kind == "v":
        for a in range(count):
            if a & top_amount:
                continue
            b = a ^ row_xor
            low, high, low_load, high_load = keys[a], keys[b], loads[a], loads[b]
            stored = b
            if lane_xor or sub_xor:
                high = permute(high, lane_xor, sub_xor)
                high_load = permute(high_load, lane_xor, sub_xor)
                stored = a | top_amount
            swap = low > high
            new_keys[a] = jnp.minimum(low, high)
            new_keys[stored] = jnp.maximum(low, high)
            new_loads[a] = jnp.where(swap, high_load, low_load)
            new_loads[stored] = jnp.where(swap, low_load, high_load)
        return new_keys, new_loads
    axis = 1 if top_kind == "l" else 0
    upper = (lax.broadcasted_iota(jnp.int32, keys[0].shape, axis) & top_amount) != 0
    for a in range(count):
        b = a ^ row_xor
        other = permute(keys[b], lane_xor, sub_xor)
        other_load = permute(loads[b], lane_xor, sub_xor)
        best = jnp.where(upper, jnp.maximum(keys[a], other), jnp.minimum(keys[a], other))
        new_keys[a] = best
        new_loads[a] = jnp.where(best == keys[a], loads[a], other_load)
    return new_keys, new_loads


def merge_levels(groups, places, first, last):
    for level in range(first, last + 1):
        groups = [exchange(*group, places, range(level + 1), level) for group in groups]
        for bit in reversed(range(level)):
            groups = [exchange(*group, places, (bit,), bit) for group in groups]
    return groups


VMEM_BYTES = 67043328


def device_of(index):
    ny, nz = lax.axis_size("gy"), lax.axis_size("gz")
    return {"gx": index // (ny * nz), "gy": (index // nz) % ny, "gz": index % nz}


def surface_kernel(
    positions_hbm, normals_hbm, tension_hbm, weight_hbm, owner_hbm, cell_hbm, connect_hbm,
    got_ref,
    positions_ref, normals_ref, tension_ref, weight_ref, owner_ref, cell_ref, connect_ref,
    low_ref, high_ref, packed_ref, force_ref, wide, jumps, turned, lists, below_ref, counted, counted_scalar,
    load_sems, sem, keep_sem, edge_send, edge_recv, all_send, all_recv,
):
    npoint = positions_ref.shape[1]
    nrow = npoint // LANES
    nowner = packed_ref.shape[0]
    total = npoint * nowner
    me = lax.axis_index(("gx", "gy", "gz"))
    begin = me * npoint
    sources = (positions_hbm, connect_hbm, weight_hbm, normals_hbm, tension_hbm, owner_hbm, cell_hbm)
    targets = (positions_ref, connect_ref, weight_ref, normals_ref, tension_ref, owner_ref, cell_ref)
    reads = [
        pltpu.make_async_copy(source, target, load_sems.at[which])
        for which, (source, target) in enumerate(zip(sources, targets))
    ]
    for read in reads:
        read.start()

    barrier = pltpu.get_barrier_semaphore()

    def greet(offset, carry):
        pl.semaphore_signal(
            barrier, inc=1, device_id=device_of((me + offset) % nowner),
            device_id_type=pl.DeviceIdType.MESH,
        )
        return carry

    lax.fori_loop(1, nowner, greet, 0)
    for read in reads:
        read.wait()

    half = lax.broadcasted_iota(jnp.int32, (3, LANES), 1) < HALO
    first_block = pltpu.roll(positions_ref[:, 0:LANES], HALO, 1)
    before = first_block
    for row in range(1, nrow):
        after = pltpu.roll(positions_ref[:, row * LANES : (row + 1) * LANES], HALO, 1)
        wide[0:3, row * LANES : (row + 1) * LANES] = jnp.where(half, before, after)
        before = after
    last_block = before

    def one_row(row, carry):
        at = row * LANES if isinstance(row, int) else pl.multiple_of(row * LANES, LANES)
        here, there = pl.ds(at, LANES), pl.ds(at + LANES, LANES)
        blank = jnp.zeros((2, LANES), jnp.int32)
        index = jnp.concatenate([connect_ref[:, here], blank], axis=0)
        index = ((index - begin + HALO) & (total - 1)) - at
        weight = jnp.concatenate([weight_ref[:, here], blank.astype(jnp.float32)], axis=0)
        second = index >= LANES
        index = index & (LANES - 1)
        strength = tension_ref[pl.ds(row, 1), :]
        jump = jnp.zeros((1, LANES), jnp.float32)
        for axis in range(3):
            lower = jnp.broadcast_to(wide[axis : axis + 1, here], (8, LANES))
            upper = jnp.broadcast_to(wide[axis : axis + 1, there], (8, LANES))
            taken = jnp.where(second, pick(upper, index, 1), pick(lower, index, 1))
            pulled = weight * (taken - positions_ref[axis : axis + 1, here])
            force = strength * jnp.sum(pulled, axis=0, keepdims=True)
            force_ref[row, axis : axis + 1, :] = force
            jump = jump + force * normals_ref[axis : axis + 1, here]
        jumps[pl.ds(row, 1), :] = jump
        return carry

    lax.fori_loop(0, (nrow - 2) // 2, lambda i, c: one_row(2 * i + 2, one_row(2 * i + 1, c)), 0, unroll=4)

    pl.semaphore_wait(barrier, nowner - 1)
    edges = (
        (positions_ref.at[:, pl.ds(npoint - LANES, LANES)], low_ref, 1),
        (positions_ref.at[:, pl.ds(0, LANES)], high_ref, nowner - 1),
    )
    sends = []
    for which, (source, target, offset) in enumerate(edges):
        sends.append(
            pltpu.make_async_remote_copy(
                src_ref=source, dst_ref=target,
                send_sem=edge_send.at[which], recv_sem=edge_recv.at[which],
                device_id=device_of((me + offset) % nowner), device_id_type=pl.DeviceIdType.MESH,
            )
        )
    for send in sends:
        send.start()

    ranks = lax.broadcasted_iota(jnp.int32, (nowner, LANES), 0)

    def count_row(row, below):
        names = owner_ref[pl.ds(row, 1), :]
        return below + jnp.where(names < ranks, 1, 0)

    below = lax.fori_loop(0, nrow, count_row, jnp.zeros((nowner, LANES), jnp.int32), unroll=4)
    for bit in range(7):
        below = below + pltpu.roll(below, 1 << bit, 1)
    below_ref[...] = below
    counted[...] = jnp.transpose(below_ref[...])[0:8, :]
    fetch = pltpu.make_async_copy(counted, counted_scalar, sem)

    keys, loads = [], []
    for tile in range(nrow // 8):
        rows = slice(8 * tile, 8 * tile + 8)
        cell = cell_ref[rows, :]
        cell = ((cell & 384) << 9) | ((cell >> 9) << 7) | (cell & 127)
        key = ((owner_ref[rows, :] << CELL_BITS) | cell) << 1
        load = jumps[rows, :]
        if tile in (0, nrow // 8 - 1):
            line = lax.broadcasted_iota(jnp.int32, (8, LANES), 0)
            lane = lax.broadcasted_iota(jnp.int32, (8, LANES), 1)
            late = line == (7 if tile else 0)
            key = key | jnp.where(late, 1, 0)
            load = jnp.where(late, (lane + (LANES if tile else 0)).astype(jnp.float32), load)
        keys.append(key)
        loads.append(load)
    fetch.start()
    places = [("v", 1), ("v", 2), ("v", 4), ("s", 1), ("s", 2), ("s", 4)]
    places += [("l", 1 << bit) for bit in range(7)]
    ((keys, loads),) = merge_levels([(keys, loads)], places, 0, 12)
    for send in sends:
        send.wait()
    wide[0:3, 0:LANES] = jnp.where(half, pltpu.roll(low_ref[...], HALO, 1), first_block)
    wide[0:3, npoint : npoint + LANES] = jnp.where(half, last_block, pltpu.roll(high_ref[...], HALO, 1))
    one_row(0, 0)
    one_row(nrow - 1, 0)
    hand_on = pltpu.make_async_copy(force_ref, got_ref.at[pl.ds(nowner, nrow)], keep_sem)

    first_jumps = jnp.broadcast_to(jumps[0:1, :], (8, LANES))
    last_jumps = jnp.broadcast_to(jumps[nrow - 1 : nrow, :], (8, LANES))
    for tile in range(nrow // 8):
        late = (keys[tile] & 1) == 1
        which = jnp.where(late, loads[tile], 0.0).astype(jnp.int32)
        lane = which & (LANES - 1)
        value = jnp.where(which >= LANES, pick(last_jumps, lane, 1), pick(first_jumps, lane, 1))
        loads[tile] = jnp.where(late, value, loads[tile])
        keys[tile] = keys[tile] >> 1
    for which, arrays in ((0, keys), (1, loads)):
        for tile in range(8):
            value = arrays[tile]
            if which == 0:
                value = (value & ((1 << CELL_BITS) - 1)).astype(jnp.float32)
            turned[pl.ds(tile, 8, stride=8), :] = value
        turned[64:128, :] = jnp.zeros((64, LANES), jnp.float32)
        flipped = jnp.transpose(turned[...])
        turned[...] = flipped
        even = turned[pl.ds(0, 64, stride=2), :]
        odd = pltpu.roll(turned[pl.ds(1, 64, stride=2), :], 64, 1)
        lane = lax.broadcasted_iota(jnp.int32, (64, LANES), 1)
        lists[pl.ds(which, 64, stride=2), :] = jnp.where(lane < 64, even, odd)
    lists[128:144, :] = jnp.zeros((16, LANES), jnp.float32)
    fetch.wait()

    lane = lax.broadcasted_iota(jnp.int32, (8, LANES), 1)
    line = lax.broadcasted_iota(jnp.int32, (8, LANES), 0)
    slot = lane + LANES * (line >> 1)
    filler = jnp.where((line & 1) == 0, BIG, 0.0).astype(jnp.float32)

    def one_owner(owner, carry):
        start = counted_scalar[0, owner]
        following = jnp.where(owner == nowner - 1, npoint, counted_scalar[0, jnp.minimum(owner + 1, nowner - 1)])
        shift = start & (LANES - 1)
        block = lists[pl.ds((start >> 7) * 2, 8), :]
        block = pltpu.roll(block, (LANES - shift) & (LANES - 1), 1)
        block = jnp.where(lane < LANES - shift, block, pltpu.roll(block, 6, 0))
        block = jnp.where(slot < following - start, block, filler)
        packed_ref[owner] = block[0:4, :]
        return carry

    def send_to(other):
        pltpu.make_async_remote_copy(
            src_ref=packed_ref.at[other], dst_ref=got_ref.at[me],
            send_sem=all_send, recv_sem=all_recv,
            device_id=device_of(other), device_id_type=pl.DeviceIdType.MESH,
        ).start()

    def pack_some(step, carry):
        for piece in range(8):
            one_owner((me + 8 * step + piece) % nowner, 0)
        return carry

    def pack_and_send(step, carry):
        pack_some(step, carry)
        for piece in range(8):
            send_to((me + 8 * (step - 1) + piece) % nowner)
        return carry

    pack_some(0, 0)
    pack_some(1, 0)
    for piece in range(1, 8):
        send_to((me + piece) % nowner)
    lax.fori_loop(2, nowner // 8, pack_and_send, 0)
    for piece in range(8):
        send_to((me + nowner - 8 + piece) % nowner)
    keep = pltpu.make_async_copy(packed_ref.at[me], got_ref.at[me], sem)
    keep.start()
    hand_on.start()
    everything = pltpu.make_async_remote_copy(
        src_ref=packed_ref.at[pl.ds(0, nowner - 1)], dst_ref=got_ref.at[pl.ds(0, nowner - 1)],
        send_sem=all_send, recv_sem=all_recv,
        device_id=device_of((me + 1) % nowner), device_id_type=pl.DeviceIdType.MESH,
    )
    everything.wait_send()
    everything.wait_recv()
    keep.wait()
    hand_on.wait()


def spread_kernel(
    got_ref, grid, force_ref,
    keys_scratch, loads_scratch, turned, bounds, bounds_scalar, work, sem,
):
    nrow = force_ref.shape[1] // LANES
    nsender = got_ref.shape[0] // 4 - nrow
    for row in range(nrow):
        first = 4 * (nsender + row)
        force_ref[:, row * LANES : (row + 1) * LANES] = got_ref[first : first + 3, :]
    ngroup = nsender // 32
    places = [("l", 1 << bit) for bit in range(7)] + [("v", 1), ("v", 2), ("v", 4)]
    places += [("s", 1), ("s", 2), ("s", 4)]

    def zero(step, carry):
        grid[pl.ds(pl.multiple_of(step * 64, 64), 64), :] = jnp.zeros((64, LANES), jnp.float32)
        return carry

    lax.fori_loop(0, grid.shape[0] // 64, zero, 0)

    def read_group(group):
        keys, loads = [], []
        for quarter in range(4):
            for side in range(2):
                first = (group * 32 + quarter * 8) * 4 + 2 * side
                keys.append(got_ref[pl.ds(first, 8, stride=4), :])
                loads.append(got_ref[pl.ds(first + 1, 8, stride=4), :])
        return keys, loads

    def store_group(group, keys, loads):
        for quarter in range(4):
            rows = pl.ds(group * 32 + quarter, 8, stride=4)
            last = jnp.full((8, 1), -1, jnp.int32)
            base = None
            for side in range(2):
                key = keys[2 * quarter + side]
                columns = slice(side * LANES, (side + 1) * LANES)
                cell = key.astype(jnp.int32)
                keys_scratch[side, rows, :] = cell
                loads_scratch[side, rows, :] = loads[2 * quarter + side]
                inside = key < BIG
                line = (cell >> 7).astype(jnp.float32)
                top = jnp.max(jnp.where(inside, line, -1.0), axis=1, keepdims=True)
                last = jnp.maximum(last, top.astype(jnp.int32))
                if side == 0:
                    base = jnp.min(line, axis=1, keepdims=True).astype(jnp.int32) & -8
            repeats = jnp.where(last < 0, 0, (((last - base) * 52429) >> 22) + 1)
            pair = jnp.where(last < 0, 0, base) * 32 + repeats
            turned[rows, :] = jnp.broadcast_to(pair.astype(jnp.float32), (8, LANES))

    for first in range(0, ngroup, TOGETHER):
        chosen = range(first, first + TOGETHER)
        merged = merge_levels([read_group(group) for group in chosen], places, 8, 12)
        for group, (keys, loads) in zip(chosen, merged):
            store_group(group, keys, loads)
    bounds[...] = jnp.transpose(turned[...])[0:8, :].astype(jnp.int32)
    fetch = pltpu.make_async_copy(bounds, bounds_scalar, sem)
    fetch.start()
    fetch.wait()

    def list_chunk(chunk, filled):
        pair = bounds_scalar[0, chunk]
        base = pair >> 5

        def list_piece(piece, filled):
            work[filled] = (chunk << 12) | (base + piece * GROUP_ROWS)
            return filled + 1

        return lax.fori_loop(0, pair & 31, list_piece, filled)

    filled = lax.fori_loop(0, 32 * ngroup, list_chunk, 0)
    for extra in range(BATCH):
        work[filled + extra] = 2048
    lines = lax.broadcasted_iota(jnp.int32, (GROUP_ROWS, 2 * LANES), 0)
    columns = lax.broadcasted_iota(jnp.int32, (LANES, 2 * LANES), 0)

    def one_batch(batch, carry):
        sums, bases = [], []
        for piece in range(BATCH):
            item = work[batch * BATCH + piece]
            chunk = item >> 12
            base = pl.multiple_of(item & 4095, 8)
            cell = jnp.concatenate([keys_scratch[side, pl.ds(chunk, 1), :] for side in range(2)], axis=1)
            load = jnp.concatenate([loads_scratch[side, pl.ds(chunk, 1), :] for side in range(2)], axis=1)
            coarse = load.astype(jnp.bfloat16).astype(jnp.float32)
            here = ((cell >> 7) - base) == lines
            left = jnp.concatenate(
                [
                    jnp.where(here, coarse, 0.0).astype(jnp.bfloat16),
                    jnp.where(here, load - coarse, 0.0).astype(jnp.bfloat16),
                ],
                axis=0,
            )
            right = jnp.where((cell & (LANES - 1)) == columns, 1.0, 0.0).astype(jnp.bfloat16)
            both = lax.dot_general(
                left, right, (((1,), (1,)), ((), ())), preferred_element_type=jnp.float32
            )
            sums.append(both[:GROUP_ROWS] + both[GROUP_ROWS:])
            bases.append(base)
        for total, base in zip(sums, bases):
            grid[pl.ds(base, GROUP_ROWS), :] += total
        return carry

    lax.fori_loop(0, (filled + BATCH - 1) // BATCH, one_batch, 0)


BATCH = 16
TOGETHER = 4


def surface_and_send(positions, normals, tension, edge_weight, owners, cells, connectivity):
    nowner = lax.axis_size(("gx", "gy", "gz"))
    arrays = (positions, normals, tension, edge_weight, owners, cells, connectivity)
    return pl.pallas_call(
        surface_kernel,
        name="surface",
        out_shape=jax.ShapeDtypeStruct((nowner + tension.shape[0], 4, LANES), jnp.float32),
        in_specs=[pl.BlockSpec(memory_space=pltpu.HBM)] * len(arrays),
        out_specs=pl.BlockSpec(memory_space=pltpu.HBM),
        scratch_shapes=[pltpu.VMEM(array.shape, array.dtype) for array in arrays]
        + [
            pltpu.VMEM((3, LANES), jnp.float32),
            pltpu.VMEM((3, LANES), jnp.float32),
            pltpu.VMEM((nowner, 4, LANES), jnp.float32),
            pltpu.VMEM((tension.shape[0], 4, LANES), jnp.float32),
            pltpu.VMEM((8, positions.shape[1] + LANES), jnp.float32),
            pltpu.VMEM((positions.shape[1] // LANES, LANES), jnp.float32),
            pltpu.VMEM((128, LANES), jnp.float32),
            pltpu.VMEM((144, LANES), jnp.float32),
            pltpu.VMEM((nowner, LANES), jnp.int32),
            pltpu.VMEM((8, LANES), jnp.int32),
            pltpu.SMEM((8, LANES), jnp.int32),
            pltpu.SemaphoreType.DMA((7,)),
            pltpu.SemaphoreType.DMA,
            pltpu.SemaphoreType.DMA,
            pltpu.SemaphoreType.DMA((2,)),
            pltpu.SemaphoreType.DMA((2,)),
            pltpu.SemaphoreType.DMA,
            pltpu.SemaphoreType.DMA,
        ],
        compiler_params=pltpu.CompilerParams(
            vmem_limit_bytes=VMEM_BYTES, collective_id=1, has_side_effects=True
        ),
    )(*arrays)


def spread_cells(got, npoint, ncell):
    vmem = pl.BlockSpec(memory_space=pltpu.VMEM)
    return pl.pallas_call(
        spread_kernel,
        name="spread",
        out_shape=(
            jax.ShapeDtypeStruct((ncell // LANES + 128, LANES), jnp.float32),
            jax.ShapeDtypeStruct((3, npoint), jnp.float32),
        ),
        in_specs=[vmem],
        out_specs=(vmem, vmem),
        scratch_shapes=[
            pltpu.VMEM((2, 128, LANES), jnp.int32),
            pltpu.VMEM((2, 128, LANES), jnp.float32),
            pltpu.VMEM((128, LANES), jnp.float32),
            pltpu.VMEM((8, LANES), jnp.int32),
            pltpu.SMEM((8, LANES), jnp.int32),
            pltpu.SMEM((512,), jnp.int32),
            pltpu.SemaphoreType.DMA,
        ],
        cost_estimate=pl.CostEstimate(flops=10**10, bytes_accessed=10**7, transcendentals=0),
        compiler_params=pltpu.CompilerParams(vmem_limit_bytes=32 * 1024 * 1024),
    )(got)


AXES = ("gx", "gy", "gz")


def halo_copies(sides, slot, send_sems, recv_sems):
    copies = []
    for which, (axis, step, source, target) in enumerate(sides):
        here = lax.axis_index(axis)
        there = here + step
        back = here - step
        size = lax.axis_size(axis)
        copy = pltpu.make_async_remote_copy(
            src_ref=source,
            dst_ref=target,
            send_sem=send_sems.at[slot, which],
            recv_sem=recv_sems.at[slot, which],
            device_id={axis: there},
            device_id_type=pl.DeviceIdType.MESH,
        )
        copies.append((copy, (there >= 0) & (there < size), (back >= 0) & (back < size)))
    return copies


def cycle_kernel(
    plane_rows, added_ref, rhs_ref, shift_ref, pressure_ref, forcing_ref,
    wide_a, wide_b, coarse_a, coarse_b, inverse, update, coarse_rhs, coarse_inverse, coarse_update,
    rows_out, rows_in, columns_out, columns_in, send_sems, recv_sems,
):
    width = forcing_ref.shape[1]
    nplane = forcing_ref.shape[0] // plane_rows
    ncoarse = nplane // 2
    tiles = plane_rows // 8
    wide, coarse = (wide_a, wide_b), (coarse_a, coarse_b)
    blank = jnp.zeros((plane_rows, width), jnp.float32)
    for slot in range(2):
        wide[slot][0:plane_rows, :] = blank
        wide[slot][(nplane + 1) * plane_rows : (nplane + 2) * plane_rows, :] = blank
        coarse[slot][0:plane_rows, :] = blank
        coarse[slot][(ncoarse + 1) * plane_rows : (ncoarse + 2) * plane_rows, :] = blank
        for side in range(2):
            rows_in[slot, side] = jnp.zeros(rows_in.shape[2:], jnp.float32)
            columns_in[slot, side] = jnp.zeros(columns_in.shape[2:], jnp.float32)

    barrier = pltpu.get_barrier_semaphore()
    neighbours = 0
    for axis in AXES:
        here, size = lax.axis_index(axis), lax.axis_size(axis)
        for step in (-1, 1):
            there = here + step
            exists = (there >= 0) & (there < size)
            neighbours = neighbours + exists.astype(jnp.int32)

            @pl.when(exists)
            def _():
                pl.semaphore_signal(
                    barrier, inc=1, device_id={axis: there}, device_id_type=pl.DeviceIdType.MESH
                )


    lane = lax.broadcasted_iota(jnp.int32, (8, LANES), 1)

    def pack_columns(head, tail, plane, low, high):
        for tile in range(tiles):
            rows = slice(8 * tile, 8 * tile + 8)
            mine = lane == plane * tiles + tile
            first = pick(head[rows, :], jnp.zeros((8, LANES), jnp.int32), 1)
            last = pick(tail[rows, :], jnp.full((8, LANES), LANES - 1, jnp.int32), 1)
            low = jnp.where(mine, first, low)
            high = jnp.where(mine, last, high)
        return low, high

    def columns_of(field, plane, slot, low, high):
        rows_out[slot, 0, pl.ds(plane, 1), :] = field[0:1, :]
        rows_out[slot, 1, pl.ds(plane, 1), :] = field[plane_rows - 1 : plane_rows, :]
        return pack_columns(field[:, 0:LANES], field[:, width - LANES : width], plane, low, high)

    def exchange_faces(field, count, slot, low, high):
        columns_out[slot, 0] = low
        columns_out[slot, 1] = high
        here = pl.ds(0, count)

        def planes(first):
            return field.at[pl.ds(first * plane_rows, plane_rows), :]

        sides = (
            ("gx", -1, planes(1), planes(count + 1)),
            ("gx", 1, planes(count), planes(0)),
            ("gy", -1, rows_out.at[slot, 0, here], rows_in.at[slot, 1, here]),
            ("gy", 1, rows_out.at[slot, 1, here], rows_in.at[slot, 0, here]),
            ("gz", -1, columns_out.at[slot, 0], columns_in.at[slot, 1]),
            ("gz", 1, columns_out.at[slot, 1], columns_in.at[slot, 0]),
        )
        copies = halo_copies(sides, slot, send_sems, recv_sems)
        for copy, sends, receives in copies:
            pl.when(sends)(copy.start)

        def finish():
            for copy, sends, receives in copies:
                pl.when(sends)(copy.wait_send)
                pl.when(receives)(copy.wait_recv)

        return finish

    row_index = lax.broadcasted_iota(jnp.int32, (plane_rows, width), 0)
    lane_index = lax.broadcasted_iota(jnp.int32, (plane_rows, LANES), 1)

    def beside(field, plane, count, reach):
        first = (plane + 1) * plane_rows
        if not isinstance(plane, int):
            first = pl.multiple_of(first, plane_rows)
        middle = field[pl.ds(first, plane_rows), :]
        total = jnp.where(row_index < reach, 0.0, pltpu.roll(middle, reach, 0))
        total = total + jnp.where(
            row_index >= plane_rows - reach, 0.0, pltpu.roll(middle, plane_rows - reach, 0)
        )
        if not isinstance(plane, int) or plane > 0:
            total = total + field[pl.ds(first - plane_rows, plane_rows), :]
        if not isinstance(plane, int) or plane < count - 1:
            total = total + field[pl.ds(first + plane_rows, plane_rows), :]
        left = pltpu.roll(middle, reach, 1)
        right = pltpu.roll(middle, width - reach, 1)
        left_edge = jnp.where(lane_index < reach, 0.0, left[:, :LANES])
        right_edge = jnp.where(lane_index >= LANES - reach, 0.0, right[:, width - LANES :])
        total = total + jnp.concatenate([left_edge, left[:, LANES:]], axis=1)
        total = total + jnp.concatenate([right[:, : width - LANES], right_edge], axis=1)
        return middle, total

    def correct(source, target, padding, slot, count, reach, scale, gain, change, packed):
        def apply(first, number, columns, value):
            here, there = pl.ds(first, number), pl.ds(first + padding, number)
            moved = value if scale is None else (gain * scale[here, columns]) * value
            if change is not None:
                change[here, columns] = change[here, columns] + moved
            answer = target[there, columns] + moved
            target[there, columns] = answer
            return answer

        entire, head, tail = slice(0, width), slice(0, LANES), slice(width - LANES, width)
        apply(0, plane_rows, entire, source[0:plane_rows, :])
        apply(
            (count - 1) * plane_rows, plane_rows, entire,
            source[(count + 1) * plane_rows : (count + 2) * plane_rows, :],
        )

        def step(plane, carry):
            base = pl.multiple_of(plane * plane_rows, plane_rows)
            for row in range(reach):
                apply(base + row, 1, entire, rows_in[slot, 0, pl.ds(plane, 1), :])
                apply(base + plane_rows - 1 - row, 1, entire, rows_in[slot, 1, pl.ds(plane, 1), :])
            low, high = [], []
            for tile in range(tiles):
                where = jnp.full((8, LANES), plane * tiles + tile, jnp.int32)
                low.append(pick(columns_in[slot, 0], where, 1))
                high.append(pick(columns_in[slot, 1], where, 1))
            low = jnp.where(lane_index < reach, jnp.concatenate(low, axis=0), 0.0)
            high = jnp.where(lane_index >= LANES - reach, jnp.concatenate(high, axis=0), 0.0)
            first = apply(base, plane_rows, head, low)
            last = apply(base, plane_rows, tail, high)
            if not packed:
                return carry
            for side, row in ((0, 0), (1, plane_rows - 1)):
                rows_out[1 - slot, side, pl.ds(plane, 1), :] = target[pl.ds(base + padding + row, 1), :]
            return pack_columns(first, last, plane, *carry)

        return lax.fori_loop(0, count, step, (nothing, nothing), unroll=8)

    nothing = jnp.zeros((8, LANES), jnp.float32)

    def rows_of(plane):
        if isinstance(plane, int):
            return pl.ds(plane * plane_rows, plane_rows)
        return pl.ds(pl.multiple_of(plane * plane_rows, plane_rows), plane_rows)

    def each_plane(count, step):
        return lax.fori_loop(0, count, step, (nothing, nothing), unroll=8)

    def inner_planes(count, step):
        step(0, 0)
        lax.fori_loop(1, count - 1, step, 0, unroll=(count - 2) // 2)
        step(count - 1, 0)

    def sweep(source, target, slot, edges, count, reach, rhs, scale, change, keep, gain, out=None):
        finish = exchange_faces(source, count, slot, *edges)

        def step(plane, carry):
            here = rows_of(plane)
            field, total = beside(source, plane, count, reach)
            moved = gain * (scale[here, :] * (rhs[here, :] + total) - field)
            if keep:
                moved = moved + keep * change[here, :]
            if out is not None:
                out[here, :] = field + moved
            else:
                change[here, :] = moved
                target[rows_of(plane + 1), :] = field + moved
            return carry

        inner_planes(count, step)
        finish()
        if out is not None:
            return correct(source, out, 0, slot, count, reach, scale, gain, None, False)
        return correct(source, target, plane_rows, slot, count, reach, scale, gain, change, True)

    ratio = centre / spread
    gains, factor = [], 1.0 / ratio
    for _ in range(COARSE_SMOOTH):
        factor_new = 1.0 / (2.0 * ratio - factor)
        gains.append((factor_new * factor, 2.0 * factor_new / spread))
        factor = factor_new

    def first_step(plane, carry):
        here = rows_of(plane)
        scale = 1.0 / (6.0 + shift_ref[here, :])
        inverse[here, :] = scale
        added = [added_ref[rows_of(part * nplane + plane), :] for part in range(width // LANES)]
        forcing = rhs_ref[here, :] + jnp.concatenate(added, axis=1)
        forcing_ref[here, :] = forcing
        answer = scale * forcing * (1.0 / centre)
        update[here, :] = answer
        wide_a[rows_of(plane + 1), :] = answer
        return columns_of(answer, plane, 0, *carry)

    edges = each_plane(nplane, first_step)
    slot = 0
    pl.semaphore_wait(barrier, neighbours)
    for sweep_index in range(SMOOTH - 1):
        keep, gain = gains[sweep_index]
        edges = sweep(
            wide[slot], wide[1 - slot], slot, edges, nplane, 1, forcing_ref, inverse, update, keep, gain
        )
        slot = 1 - slot
    smooth, remains_ref = wide[slot], wide[1 - slot]

    lane_pair = lax.broadcasted_iota(jnp.int32, (8, LANES), 1) ^ 1
    line_pair = lax.broadcasted_iota(jnp.int32, (8, LANES), 0) ^ 1

    def pair_sum(value):
        lines = []
        for tile in range(tiles):
            parts = []
            for part in range(width // LANES):
                block = value[8 * tile : 8 * tile + 8, part * LANES : (part + 1) * LANES]
                block = block + pick(block, lane_pair, 1)
                parts.append(block + pick(block, line_pair, 0))
            lines.append(jnp.concatenate(parts, axis=1))
        return jnp.concatenate(lines, axis=0)

    finish = exchange_faces(smooth, nplane, slot, *edges)

    def leave(plane, carry):
        here = rows_of(plane)
        field, total = beside(smooth, plane, nplane, 1)
        remains_ref[rows_of(plane + 1), :] = forcing_ref[here, :] - ((6.0 + shift_ref[here, :]) * field - total)
        return carry

    inner_planes(nplane, leave)
    finish()
    correct(smooth, remains_ref, plane_rows, slot, nplane, 1, None, 1.0, None, False)
    slot = 1 - slot

    def restrict(plane, carry):
        remains = remains_ref[rows_of(2 * plane + 1), :] + remains_ref[rows_of(2 * plane + 2), :]
        shifts = shift_ref[rows_of(2 * plane), :] + shift_ref[rows_of(2 * plane + 1), :]
        rhs = 0.5 * pair_sum(remains)
        scale = 1.0 / (6.0 + 0.5 * pair_sum(shifts))
        answer = scale * rhs * (1.0 / centre)
        here = rows_of(plane)
        coarse_rhs[here, :] = rhs
        coarse_inverse[here, :] = scale
        coarse_update[here, :] = answer
        coarse[slot][rows_of(plane + 1), :] = answer
        return columns_of(answer, plane, slot, *carry)

    edges = each_plane(ncoarse, restrict)
    for sweep_index in range(COARSE_SMOOTH - 1):
        keep, gain = gains[sweep_index]
        edges = sweep(
            coarse[slot], coarse[1 - slot], slot, edges, ncoarse, 2,
            coarse_rhs, coarse_inverse, coarse_update, keep, gain,
        )
        slot = 1 - slot
    fix = coarse[slot]

    def begin_again(plane, carry):
        here = rows_of(plane + 1)
        answer = smooth[here, :] + fix[rows_of(lax.div(plane, 2) + 1), :]
        wide[slot][here, :] = answer
        return columns_of(answer, plane, slot, *carry)

    edges = each_plane(nplane, begin_again)
    for sweep_index in range(SMOOTH):
        keep, gain = gains[sweep_index - 1] if sweep_index else (0.0, 1.0 / centre)
        edges = sweep(
            wide[slot], wide[1 - slot], slot, edges, nplane, 1, forcing_ref, inverse, update, keep, gain,
            pressure_ref if sweep_index == SMOOTH - 1 else None,
        )
        slot = 1 - slot


def multigrid(added, pressure_rhs, shift_diag):
    planes, rows, width = shift_diag.shape
    vmem = pl.BlockSpec(memory_space=pltpu.VMEM)
    flat = (planes * rows, width)
    half = (planes // 2 * rows, width)
    f32 = jnp.float32
    return pl.pallas_call(
        functools.partial(cycle_kernel, rows),
        name="multigrid",
        out_shape=jax.ShapeDtypeStruct(flat, f32),
        in_specs=[vmem] * 3,
        out_specs=vmem,
        scratch_shapes=[
            pltpu.VMEM(flat, f32),
            pltpu.VMEM((flat[0] + 2 * rows, width), f32),
            pltpu.VMEM((flat[0] + 2 * rows, width), f32),
            pltpu.VMEM((half[0] + 2 * rows, width), f32),
            pltpu.VMEM((half[0] + 2 * rows, width), f32),
            pltpu.VMEM(flat, f32),
            pltpu.VMEM(flat, f32),
            pltpu.VMEM(half, f32),
            pltpu.VMEM(half, f32),
            pltpu.VMEM(half, f32),
            pltpu.VMEM((2, 2, planes, width), f32),
            pltpu.VMEM((2, 2, planes, width), f32),
            pltpu.VMEM((2, 2, 8, LANES), f32),
            pltpu.VMEM((2, 2, 8, LANES), f32),
            pltpu.SemaphoreType.DMA((2, 6)),
            pltpu.SemaphoreType.DMA((2, 6)),
        ],
        compiler_params=pltpu.CompilerParams(
            vmem_limit_bytes=40 * 1024 * 1024, collective_id=0, has_side_effects=True
        ),
    )(added, pressure_rhs.reshape(flat), shift_diag.reshape(flat)).reshape(shift_diag.shape)


def body(
    pressure_rhs,
    shift_diag,
    positions,
    normals,
    tension,
    edge_weight,
    owner_map,
    cell_map,
    connectivity,
):
    nrow = positions.shape[1] // LANES
    got = surface_and_send(
        positions,
        normals,
        tension.reshape(nrow, LANES),
        edge_weight,
        owner_map.reshape(nrow, LANES),
        cell_map.reshape(nrow, LANES),
        connectivity,
    )
    added, surface_force = spread_cells(got.reshape(-1, LANES), positions.shape[1], pressure_rhs.size)
    pressure = multigrid(added, pressure_rhs, shift_diag)
    return (pressure, surface_force)


def solution(mesh):
    return jax.shard_map(
        body,
        mesh=mesh,
        in_specs=(
            P("gx", "gy", "gz"),
            P("gx", "gy", "gz"),
            P(None, ("gx", "gy", "gz")),
            P(None, ("gx", "gy", "gz")),
            P(("gx", "gy", "gz")),
            P(None, ("gx", "gy", "gz")),
            P(("gx", "gy", "gz"), None),
            P(("gx", "gy", "gz")),
            P(None, ("gx", "gy", "gz")),
        ),
        out_specs=(P("gx", "gy", "gz"), P(None, ("gx", "gy", "gz"))),
        check_vma=False,
    )
```

```python
import functools
import jax
import jax.numpy as jnp
from jax import lax
from jax.experimental import pallas as pl
from jax.experimental.pallas import tpu as pltpu
from jax.sharding import PartitionSpec as P

HALO = 64
SMOOTH = 3
COARSE_SMOOTH = 4


centre = 1.125
spread = 0.875


LANES = 128
BIG = 524288.0
GROUP_ROWS = 80
CELL_BITS = 18


def permute(value, lane_xor, sub_xor):
    if sub_xor:
        where = lax.broadcasted_iota(jnp.int32, value.shape, 0) ^ sub_xor
        value = pick(value, where, 0)
    if lane_xor:
        where = lax.broadcasted_iota(jnp.int32, value.shape, 1) ^ lane_xor
        value = pick(value, where, 1)
    return value


def pick(value, where, axis):
    numbers = lax.GatherDimensionNumbers(
        offset_dims=(),
        collapsed_slice_dims=(axis,),
        start_index_map=(axis,),
        operand_batching_dims=(1 - axis,),
        start_indices_batching_dims=(1 - axis,),
    )
    return lax.gather(
        value,
        where[:, :, None],
        numbers,
        (1, 1),
        mode=lax.GatherScatterMode.PROMISE_IN_BOUNDS,
    )


def exchange(keys, loads, places, bits, top):
    lane_xor = sub_xor = row_xor = 0
    for bit in bits:
        kind, amount = places[bit]
        lane_xor |= amount if kind == "l" else 0
        sub_xor |= amount if kind == "s" else 0
        row_xor |= amount if kind == "v" else 0
    top_kind, top_amount = places[top]
    count = len(keys)
    new_keys, new_loads = [None] * count, [None] * count
    if top_kind == "v":
        for a in range(count):
            if a & top_amount:
                continue
            b = a ^ row_xor
            low, high, low_load, high_load = keys[a], keys[b], loads[a], loads[b]
            stored = b
            if lane_xor or sub_xor:
                high = permute(high, lane_xor, sub_xor)
                high_load = permute(high_load, lane_xor, sub_xor)
                stored = a | top_amount
            swap = low > high
            new_keys[a] = jnp.minimum(low, high)
            new_keys[stored] = jnp.maximum(low, high)
            new_loads[a] = jnp.where(swap, high_load, low_load)
            new_loads[stored] = jnp.where(swap, low_load, high_load)
        return new_keys, new_loads
    axis = 1 if top_kind == "l" else 0
    upper = (lax.broadcasted_iota(jnp.int32, keys[0].shape, axis) & top_amount) != 0
    for a in range(count):
        b = a ^ row_xor
        other = permute(keys[b], lane_xor, sub_xor)
        other_load = permute(loads[b], lane_xor, sub_xor)
        best = jnp.where(upper, jnp.maximum(keys[a], other), jnp.minimum(keys[a], other))
        new_keys[a] = best
        new_loads[a] = jnp.where(best == keys[a], loads[a], other_load)
    return new_keys, new_loads


def merge_levels(groups, places, first, last):
    for level in range(first, last + 1):
        groups = [exchange(*group, places, range(level + 1), level) for group in groups]
        for bit in reversed(range(level)):
            groups = [exchange(*group, places, (bit,), bit) for group in groups]
    return groups


VMEM_BYTES = 67043328


def device_of(index):
    ny, nz = lax.axis_size("gy"), lax.axis_size("gz")
    return {"gx": index // (ny * nz), "gy": (index // nz) % ny, "gz": index % nz}


def surface_kernel(
    positions_hbm, normals_hbm, tension_hbm, weight_hbm, owner_hbm, cell_hbm, connect_hbm,
    got_ref,
    positions_ref, normals_ref, tension_ref, weight_ref, owner_ref, cell_ref, connect_ref,
    low_ref, high_ref, packed_ref, force_ref, wide, jumps, turned, lists, below_ref, counted, counted_scalar,
    load_sems, sem, keep_sem, edge_send, edge_recv, all_send, all_recv,
):
    npoint = positions_ref.shape[1]
    nrow = npoint // LANES
    nowner = packed_ref.shape[0]
    total = npoint * nowner
    me = lax.axis_index(("gx", "gy", "gz"))
    begin = me * npoint
    sources = (positions_hbm, connect_hbm, weight_hbm, normals_hbm, tension_hbm, owner_hbm, cell_hbm)
    targets = (positions_ref, connect_ref, weight_ref, normals_ref, tension_ref, owner_ref, cell_ref)
    reads = [
        pltpu.make_async_copy(source, target, load_sems.at[which])
        for which, (source, target) in enumerate(zip(sources, targets))
    ]
    for read in reads:
        read.start()

    barrier = pltpu.get_barrier_semaphore()

    def greet(offset, carry):
        pl.semaphore_signal(
            barrier, inc=1, device_id=device_of((me + offset) % nowner),
            device_id_type=pl.DeviceIdType.MESH,
        )
        return carry

    lax.fori_loop(1, nowner, greet, 0)
    for read in reads:
        read.wait()

    half = lax.broadcasted_iota(jnp.int32, (3, LANES), 1) < HALO
    first_block = pltpu.roll(positions_ref[:, 0:LANES], HALO, 1)
    before = first_block
    for row in range(1, nrow):
        after = pltpu.roll(positions_ref[:, row * LANES : (row + 1) * LANES], HALO, 1)
        wide[0:3, row * LANES : (row + 1) * LANES] = jnp.where(half, before, after)
        before = after
    last_block = before

    def one_row(row, carry):
        at = row * LANES if isinstance(row, int) else pl.multiple_of(row * LANES, LANES)
        here, there = pl.ds(at, LANES), pl.ds(at + LANES, LANES)
        blank = jnp.zeros((2, LANES), jnp.int32)
        index = jnp.concatenate([connect_ref[:, here], blank], axis=0)
        index = ((index - begin + HALO) & (total - 1)) - at
        weight = jnp.concatenate([weight_ref[:, here], blank.astype(jnp.float32)], axis=0)
        second = index >= LANES
        index = index & (LANES - 1)
        strength = tension_ref[pl.ds(row, 1), :]
        jump = jnp.zeros((1, LANES), jnp.float32)
        for axis in range(3):
            lower = jnp.broadcast_to(wide[axis : axis + 1, here], (8, LANES))
            upper = jnp.broadcast_to(wide[axis : axis + 1, there], (8, LANES))
            taken = jnp.where(second, pick(upper, index, 1), pick(lower, index, 1))
            pulled = weight * (taken - positions_ref[axis : axis + 1, here])
            force = strength * jnp.sum(pulled, axis=0, keepdims=True)
            force_ref[row, axis : axis + 1, :] = force
            jump = jump + force * normals_ref[axis : axis + 1, here]
        jumps[pl.ds(row, 1), :] = jump
        return carry

    lax.fori_loop(0, (nrow - 2) // 2, lambda i, c: one_row(2 * i + 2, one_row(2 * i + 1, c)), 0, unroll=4)

    pl.semaphore_wait(barrier, nowner - 1)
    edges = (
        (positions_ref.at[:, pl.ds(npoint - LANES, LANES)], low_ref, 1),
        (positions_ref.at[:, pl.ds(0, LANES)], high_ref, nowner - 1),
    )
    sends = []
    for which, (source, target, offset) in enumerate(edges):
        sends.append(
            pltpu.make_async_remote_copy(
                src_ref=source, dst_ref=target,
                send_sem=edge_send.at[which], recv_sem=edge_recv.at[which],
                device_id=device_of((me + offset) % nowner), device_id_type=pl.DeviceIdType.MESH,
            )
        )
    for send in sends:
        send.start()

    ranks = lax.broadcasted_iota(jnp.int32, (nowner, LANES), 0)

    def count_row(row, below):
        names = owner_ref[pl.ds(row, 1), :]
        return below + jnp.where(names < ranks, 1, 0)

    below = lax.fori_loop(0, nrow, count_row, jnp.zeros((nowner, LANES), jnp.int32), unroll=4)
    for bit in range(7):
        below = below + pltpu.roll(below, 1 << bit, 1)
    below_ref[...] = below
    counted[...] = jnp.transpose(below_ref[...])[0:8, :]
    fetch = pltpu.make_async_copy(counted, counted_scalar, sem)

    keys, loads = [], []
    for tile in range(nrow // 8):
        rows = slice(8 * tile, 8 * tile + 8)
        cell = cell_ref[rows, :]
        cell = ((cell & 384) << 9) | ((cell >> 9) << 7) | (cell & 127)
        key = ((owner_ref[rows, :] << CELL_BITS) | cell) << 1
        load = jumps[rows, :]
        if tile in (0, nrow // 8 - 1):
            line = lax.broadcasted_iota(jnp.int32, (8, LANES), 0)
            lane = lax.broadcasted_iota(jnp.int32, (8, LANES), 1)
            late = line == (7 if tile else 0)
            key = key | jnp.where(late, 1, 0)
            load = jnp.where(late, (lane + (LANES if tile else 0)).astype(jnp.float32), load)
        keys.append(key)
        loads.append(load)
    fetch.start()
    places = [("v", 1), ("v", 2), ("v", 4), ("s", 1), ("s", 2), ("s", 4)]
    places += [("l", 1 << bit) for bit in range(7)]
    ((keys, loads),) = merge_levels([(keys, loads)], places, 0, 12)
    for send in sends:
        send.wait()
    wide[0:3, 0:LANES] = jnp.where(half, pltpu.roll(low_ref[...], HALO, 1), first_block)
    wide[0:3, npoint : npoint + LANES] = jnp.where(half, last_block, pltpu.roll(high_ref[...], HALO, 1))
    one_row(0, 0)
    one_row(nrow - 1, 0)
    hand_on = pltpu.make_async_copy(force_ref, got_ref.at[pl.ds(nowner, nrow)], keep_sem)

    first_jumps = jnp.broadcast_to(jumps[0:1, :], (8, LANES))
    last_jumps = jnp.broadcast_to(jumps[nrow - 1 : nrow, :], (8, LANES))
    for tile in range(nrow // 8):
        late = (keys[tile] & 1) == 1
        which = jnp.where(late, loads[tile], 0.0).astype(jnp.int32)
        lane = which & (LANES - 1)
        value = jnp.where(which >= LANES, pick(last_jumps, lane, 1), pick(first_jumps, lane, 1))
        loads[tile] = jnp.where(late, value, loads[tile])
        keys[tile] = keys[tile] >> 1
    for which, arrays in ((0, keys), (1, loads)):
        for tile in range(8):
            value = arrays[tile]
            if which == 0:
                value = (value & ((1 << CELL_BITS) - 1)).astype(jnp.float32)
            turned[pl.ds(tile, 8, stride=8), :] = value
        turned[64:128, :] = jnp.zeros((64, LANES), jnp.float32)
        flipped = jnp.transpose(turned[...])
        turned[...] = flipped
        even = turned[pl.ds(0, 64, stride=2), :]
        odd = pltpu.roll(turned[pl.ds(1, 64, stride=2), :], 64, 1)
        lane = lax.broadcasted_iota(jnp.int32, (64, LANES), 1)
        lists[pl.ds(which, 64, stride=2), :] = jnp.where(lane < 64, even, odd)
    lists[128:144, :] = jnp.zeros((16, LANES), jnp.float32)
    fetch.wait()

    lane = lax.broadcasted_iota(jnp.int32, (8, LANES), 1)
    line = lax.broadcasted_iota(jnp.int32, (8, LANES), 0)
    slot = lane + LANES * (line >> 1)
    filler = jnp.where((line & 1) == 0, BIG, 0.0).astype(jnp.float32)

    def one_owner(owner, carry):
        start = counted_scalar[0, owner]
        following = jnp.where(owner == nowner - 1, npoint, counted_scalar[0, jnp.minimum(owner + 1, nowner - 1)])
        shift = start & (LANES - 1)
        block = lists[pl.ds((start >> 7) * 2, 8), :]
        block = pltpu.roll(block, (LANES - shift) & (LANES - 1), 1)
        block = jnp.where(lane < LANES - shift, block, pltpu.roll(block, 6, 0))
        block = jnp.where(slot < following - start, block, filler)
        packed_ref[owner] = block[0:4, :]
        return carry

    def send_to(other):
        pltpu.make_async_remote_copy(
            src_ref=packed_ref.at[other], dst_ref=got_ref.at[me],
            send_sem=all_send, recv_sem=all_recv,
            device_id=device_of(other), device_id_type=pl.DeviceIdType.MESH,
        ).start()

    def pack_some(step, carry):
        for piece in range(8):
            one_owner((me + 8 * step + piece) % nowner, 0)
        return carry

    def pack_and_send(step, carry):
        pack_some(step, carry)
        for piece in range(8):
            send_to((me + 8 * (step - 1) + piece) % nowner)
        return carry

    pack_some(0, 0)
    pack_some(1, 0)
    for piece in range(1, 8):
        send_to((me + piece) % nowner)
    lax.fori_loop(2, nowner // 8, pack_and_send, 0)
    for piece in range(8):
        send_to((me + nowner - 8 + piece) % nowner)
    keep = pltpu.make_async_copy(packed_ref.at[me], got_ref.at[me], sem)
    keep.start()
    hand_on.start()
    everything = pltpu.make_async_remote_copy(
        src_ref=packed_ref.at[pl.ds(0, nowner - 1)], dst_ref=got_ref.at[pl.ds(0, nowner - 1)],
        send_sem=all_send, recv_sem=all_recv,
        device_id=device_of((me + 1) % nowner), device_id_type=pl.DeviceIdType.MESH,
    )
    everything.wait_send()
    everything.wait_recv()
    keep.wait()
    hand_on.wait()


def spread_kernel(
    got_ref, grid, force_ref,
    keys_scratch, loads_scratch, turned, bounds, bounds_scalar, work, sem,
):
    nrow = force_ref.shape[1] // LANES
    nsender = got_ref.shape[0] // 4 - nrow
    for row in range(nrow):
        first = 4 * (nsender + row)
        force_ref[:, row * LANES : (row + 1) * LANES] = got_ref[first : first + 3, :]
    ngroup = nsender // 32
    places = [("l", 1 << bit) for bit in range(7)] + [("v", 1), ("v", 2), ("v", 4)]
    places += [("s", 1), ("s", 2), ("s", 4)]

    def zero(step, carry):
        grid[pl.ds(pl.multiple_of(step * 64, 64), 64), :] = jnp.zeros((64, LANES), jnp.float32)
        return carry

    lax.fori_loop(0, grid.shape[0] // 64, zero, 0)

    def read_group(group):
        keys, loads = [], []
        for quarter in range(4):
            for side in range(2):
                first = (group * 32 + quarter * 8) * 4 + 2 * side
                keys.append(got_ref[pl.ds(first, 8, stride=4), :])
                loads.append(got_ref[pl.ds(first + 1, 8, stride=4), :])
        return keys, loads

    def store_group(group, keys, loads):
        for quarter in range(4):
            rows = pl.ds(group * 32 + quarter, 8, stride=4)
            last = jnp.full((8, 1), -1, jnp.int32)
            base = None
            for side in range(2):
                key = keys[2 * quarter + side]
                columns = slice(side * LANES, (side + 1) * LANES)
                cell = key.astype(jnp.int32)
                keys_scratch[side, rows, :] = cell
                loads_scratch[side, rows, :] = loads[2 * quarter + side]
                inside = key < BIG
                line = (cell >> 7).astype(jnp.float32)
                top = jnp.max(jnp.where(inside, line, -1.0), axis=1, keepdims=True)
                last = jnp.maximum(last, top.astype(jnp.int32))
                if side == 0:
                    base = jnp.min(line, axis=1, keepdims=True).astype(jnp.int32) & -8
            repeats = jnp.where(last < 0, 0, (((last - base) * 52429) >> 22) + 1)
            pair = jnp.where(last < 0, 0, base) * 32 + repeats
            turned[rows, :] = jnp.broadcast_to(pair.astype(jnp.float32), (8, LANES))

    for first in range(0, ngroup, TOGETHER):
        chosen = range(first, first + TOGETHER)
        merged = merge_levels([read_group(group) for group in chosen], places, 8, 12)
        for group, (keys, loads) in zip(chosen, merged):
            store_group(group, keys, loads)
    bounds[...] = jnp.transpose(turned[...])[0:8, :].astype(jnp.int32)
    fetch = pltpu.make_async_copy(bounds, bounds_scalar, sem)
    fetch.start()
    fetch.wait()

    def list_chunk(chunk, filled):
        pair = bounds_scalar[0, chunk]
        base = pair >> 5

        def list_piece(piece, filled):
            work[filled] = (chunk << 12) | (base + piece * GROUP_ROWS)
            return filled + 1

        return lax.fori_loop(0, pair & 31, list_piece, filled)

    filled = lax.fori_loop(0, 32 * ngroup, list_chunk, 0)
    for extra in range(BATCH):
        work[filled + extra] = 2048
    lines = lax.broadcasted_iota(jnp.int32, (GROUP_ROWS, 2 * LANES), 0)
    columns = lax.broadcasted_iota(jnp.int32, (LANES, 2 * LANES), 0)

    def one_batch(batch, carry):
        sums, bases = [], []
        for piece in range(BATCH):
            item = work[batch * BATCH + piece]
            chunk = item >> 12
            base = pl.multiple_of(item & 4095, 8)
            cell = jnp.concatenate([keys_scratch[side, pl.ds(chunk, 1), :] for side in range(2)], axis=1)
            load = jnp.concatenate([loads_scratch[side, pl.ds(chunk, 1), :] for side in range(2)], axis=1)
            coarse = load.astype(jnp.bfloat16).astype(jnp.float32)
            here = ((cell >> 7) - base) == lines
            left = jnp.concatenate(
                [
                    jnp.where(here, coarse, 0.0).astype(jnp.bfloat16),
                    jnp.where(here, load - coarse, 0.0).astype(jnp.bfloat16),
                ],
                axis=0,
            )
            right = jnp.where((cell & (LANES - 1)) == columns, 1.0, 0.0).astype(jnp.bfloat16)
            both = lax.dot_general(
                left, right, (((1,), (1,)), ((), ())), preferred_element_type=jnp.float32
            )
            sums.append(both[:GROUP_ROWS] + both[GROUP_ROWS:])
            bases.append(base)
        for total, base in zip(sums, bases):
            grid[pl.ds(base, GROUP_ROWS), :] += total
        return carry

    lax.fori_loop(0, (filled + BATCH - 1) // BATCH, one_batch, 0)


BATCH = 16
TOGETHER = 4


def surface_and_send(positions, normals, tension, edge_weight, owners, cells, connectivity):
    nowner = lax.axis_size(("gx", "gy", "gz"))
    arrays = (positions, normals, tension, edge_weight, owners, cells, connectivity)
    return pl.pallas_call(
        surface_kernel,
        name="surface",
        out_shape=jax.ShapeDtypeStruct((nowner + tension.shape[0], 4, LANES), jnp.float32),
        in_specs=[pl.BlockSpec(memory_space=pltpu.HBM)] * len(arrays),
        out_specs=pl.BlockSpec(memory_space=pltpu.HBM),
        scratch_shapes=[pltpu.VMEM(array.shape, array.dtype) for array in arrays]
        + [
            pltpu.VMEM((3, LANES), jnp.float32),
            pltpu.VMEM((3, LANES), jnp.float32),
            pltpu.VMEM((nowner, 4, LANES), jnp.float32),
            pltpu.VMEM((tension.shape[0], 4, LANES), jnp.float32),
            pltpu.VMEM((8, positions.shape[1] + LANES), jnp.float32),
            pltpu.VMEM((positions.shape[1] // LANES, LANES), jnp.float32),
            pltpu.VMEM((128, LANES), jnp.float32),
            pltpu.VMEM((144, LANES), jnp.float32),
            pltpu.VMEM((nowner, LANES), jnp.int32),
            pltpu.VMEM((8, LANES), jnp.int32),
            pltpu.SMEM((8, LANES), jnp.int32),
            pltpu.SemaphoreType.DMA((7,)),
            pltpu.SemaphoreType.DMA,
            pltpu.SemaphoreType.DMA,
            pltpu.SemaphoreType.DMA((2,)),
            pltpu.SemaphoreType.DMA((2,)),
            pltpu.SemaphoreType.DMA,
            pltpu.SemaphoreType.DMA,
        ],
        compiler_params=pltpu.CompilerParams(
            vmem_limit_bytes=VMEM_BYTES, collective_id=1, has_side_effects=True
        ),
    )(*arrays)


def spread_cells(got, npoint, ncell):
    vmem = pl.BlockSpec(memory_space=pltpu.VMEM)
    return pl.pallas_call(
        spread_kernel,
        name="spread",
        out_shape=(
            jax.ShapeDtypeStruct((ncell // LANES + 128, LANES), jnp.float32),
            jax.ShapeDtypeStruct((3, npoint), jnp.float32),
        ),
        in_specs=[vmem],
        out_specs=(vmem, vmem),
        scratch_shapes=[
            pltpu.VMEM((2, 128, LANES), jnp.int32),
            pltpu.VMEM((2, 128, LANES), jnp.float32),
            pltpu.VMEM((128, LANES), jnp.float32),
            pltpu.VMEM((8, LANES), jnp.int32),
            pltpu.SMEM((8, LANES), jnp.int32),
            pltpu.SMEM((512,), jnp.int32),
            pltpu.SemaphoreType.DMA,
        ],
        cost_estimate=pl.CostEstimate(flops=10**10, bytes_accessed=10**7, transcendentals=0),
        compiler_params=pltpu.CompilerParams(vmem_limit_bytes=32 * 1024 * 1024),
    )(got)


AXES = ("gx", "gy", "gz")


def halo_copies(sides, slot, send_sems, recv_sems):
    copies = []
    for which, (axis, step, source, target) in enumerate(sides):
        here = lax.axis_index(axis)
        there = here + step
        back = here - step
        size = lax.axis_size(axis)
        copy = pltpu.make_async_remote_copy(
            src_ref=source,
            dst_ref=target,
            send_sem=send_sems.at[slot, which],
            recv_sem=recv_sems.at[slot, which],
            device_id={axis: there},
            device_id_type=pl.DeviceIdType.MESH,
        )
        copies.append((copy, (there >= 0) & (there < size), (back >= 0) & (back < size)))
    return copies


def cycle_kernel(
    plane_rows, added_ref, rhs_ref, shift_ref, pressure_ref, forcing_ref,
    wide_a, wide_b, coarse_a, coarse_b, inverse, update, coarse_rhs, coarse_inverse, coarse_update,
    rows_out, rows_in, columns_out, columns_in, send_sems, recv_sems,
):
    width = forcing_ref.shape[1]
    nplane = forcing_ref.shape[0] // plane_rows
    ncoarse = nplane // 2
    tiles = plane_rows // 8
    wide, coarse = (wide_a, wide_b), (coarse_a, coarse_b)
    blank = jnp.zeros((plane_rows, width), jnp.float32)
    for slot in range(2):
        wide[slot][0:plane_rows, :] = blank
        wide[slot][(nplane + 1) * plane_rows : (nplane + 2) * plane_rows, :] = blank
        coarse[slot][0:plane_rows, :] = blank
        coarse[slot][(ncoarse + 1) * plane_rows : (ncoarse + 2) * plane_rows, :] = blank
        for side in range(2):
            rows_in[slot, side] = jnp.zeros(rows_in.shape[2:], jnp.float32)
            columns_in[slot, side] = jnp.zeros(columns_in.shape[2:], jnp.float32)

    barrier = pltpu.get_barrier_semaphore()
    neighbours = 0
    for axis in AXES:
        here, size = lax.axis_index(axis), lax.axis_size(axis)
        for step in (-1, 1):
            there = here + step
            exists = (there >= 0) & (there < size)
            neighbours = neighbours + exists.astype(jnp.int32)

            @pl.when(exists)
            def _():
                pl.semaphore_signal(
                    barrier, inc=1, device_id={axis: there}, device_id_type=pl.DeviceIdType.MESH
                )


    lane = lax.broadcasted_iota(jnp.int32, (8, LANES), 1)

    def pack_columns(head, tail, plane, low, high):
        for tile in range(tiles):
            rows = slice(8 * tile, 8 * tile + 8)
            mine = lane == plane * tiles + tile
            first = pick(head[rows, :], jnp.zeros((8, LANES), jnp.int32), 1)
            last = pick(tail[rows, :], jnp.full((8, LANES), LANES - 1, jnp.int32), 1)
            low = jnp.where(mine, first, low)
            high = jnp.where(mine, last, high)
        return low, high

    def columns_of(field, plane, slot, low, high):
        rows_out[slot, 0, pl.ds(plane, 1), :] = field[0:1, :]
        rows_out[slot, 1, pl.ds(plane, 1), :] = field[plane_rows - 1 : plane_rows, :]
        return pack_columns(field[:, 0:LANES], field[:, width - LANES : width], plane, low, high)

    def face_copies(field, count, slot):
        here = pl.ds(0, count)

        def planes(first):
            return field.at[pl.ds(first * plane_rows, plane_rows), :]

        sides = (
            ("gx", -1, planes(1), planes(count + 1)),
            ("gx", 1, planes(count), planes(0)),
            ("gy", -1, rows_out.at[slot, 0, here], rows_in.at[slot, 1, here]),
            ("gy", 1, rows_out.at[slot, 1, here], rows_in.at[slot, 0, here]),
            ("gz", -1, columns_out.at[slot, 0], columns_in.at[slot, 1]),
            ("gz", 1, columns_out.at[slot, 1], columns_in.at[slot, 0]),
        )
        return halo_copies(sides, slot, send_sems, recv_sems)

    def start_all(copies):
        for copy, sends, receives in copies:
            pl.when(sends)(copy.start)

    def exchange_faces(field, count, slot, started, low, high):
        columns_out[slot, 0] = low
        columns_out[slot, 1] = high
        copies = face_copies(field, count, slot)
        start_all(copies[2:] if started else copies)

        def finish():
            for copy, sends, receives in copies:
                pl.when(sends)(copy.wait_send)
                pl.when(receives)(copy.wait_recv)

        return finish

    row_index = lax.broadcasted_iota(jnp.int32, (plane_rows, width), 0)
    lane_index = lax.broadcasted_iota(jnp.int32, (plane_rows, LANES), 1)

    def beside(field, plane, count, reach):
        first = (plane + 1) * plane_rows
        if not isinstance(plane, int):
            first = pl.multiple_of(first, plane_rows)
        middle = field[pl.ds(first, plane_rows), :]
        total = jnp.where(row_index < reach, 0.0, pltpu.roll(middle, reach, 0))
        total = total + jnp.where(
            row_index >= plane_rows - reach, 0.0, pltpu.roll(middle, plane_rows - reach, 0)
        )
        if not isinstance(plane, int) or plane > 0:
            total = total + field[pl.ds(first - plane_rows, plane_rows), :]
        if not isinstance(plane, int) or plane < count - 1:
            total = total + field[pl.ds(first + plane_rows, plane_rows), :]
        left = pltpu.roll(middle, reach, 1)
        right = pltpu.roll(middle, width - reach, 1)
        left_edge = jnp.where(lane_index < reach, 0.0, left[:, :LANES])
        right_edge = jnp.where(lane_index >= LANES - reach, 0.0, right[:, width - LANES :])
        total = total + jnp.concatenate([left_edge, left[:, LANES:]], axis=1)
        total = total + jnp.concatenate([right[:, : width - LANES], right_edge], axis=1)
        return middle, total

    def correct(source, target, padding, slot, count, reach, scale, gain, change, packed):
        def apply(first, number, columns, value):
            here, there = pl.ds(first, number), pl.ds(first + padding, number)
            moved = value if scale is None else (gain * scale[here, columns]) * value
            if change is not None:
                change[here, columns] = change[here, columns] + moved
            answer = target[there, columns] + moved
            target[there, columns] = answer
            return answer

        entire, head, tail = slice(0, width), slice(0, LANES), slice(width - LANES, width)
        apply(0, plane_rows, entire, source[0:plane_rows, :])
        apply(
            (count - 1) * plane_rows, plane_rows, entire,
            source[(count + 1) * plane_rows : (count + 2) * plane_rows, :],
        )

        def step(plane, carry):
            base = plane * plane_rows
            if not isinstance(plane, int):
                base = pl.multiple_of(base, plane_rows)
            for row in range(reach):
                apply(base + row, 1, entire, rows_in[slot, 0, pl.ds(plane, 1), :])
                apply(base + plane_rows - 1 - row, 1, entire, rows_in[slot, 1, pl.ds(plane, 1), :])
            low, high = [], []
            for tile in range(tiles):
                where = jnp.full((8, LANES), plane * tiles + tile, jnp.int32)
                low.append(pick(columns_in[slot, 0], where, 1))
                high.append(pick(columns_in[slot, 1], where, 1))
            low = jnp.where(lane_index < reach, jnp.concatenate(low, axis=0), 0.0)
            high = jnp.where(lane_index >= LANES - reach, jnp.concatenate(high, axis=0), 0.0)
            first = apply(base, plane_rows, head, low)
            last = apply(base, plane_rows, tail, high)
            if not packed:
                return carry
            for side, row in ((0, 0), (1, plane_rows - 1)):
                rows_out[1 - slot, side, pl.ds(plane, 1), :] = target[pl.ds(base + padding + row, 1), :]
            return pack_columns(first, last, plane, *carry)

        edges = (nothing, nothing)
        for plane in (0, count - 1, 1, 2):
            edges = step(plane, edges)
        if packed:
            start_all(face_copies(target, count, 1 - slot)[:2])
        return lax.fori_loop(3, count - 1, step, edges, unroll=min(6, count - 4))

    nothing = jnp.zeros((8, LANES), jnp.float32)

    def rows_of(plane):
        if isinstance(plane, int):
            return pl.ds(plane * plane_rows, plane_rows)
        return pl.ds(pl.multiple_of(plane * plane_rows, plane_rows), plane_rows)

    def each_plane(count, step):
        return lax.fori_loop(0, count, step, (nothing, nothing), unroll=8)

    def inner_planes(count, step):
        step(0, 0)
        lax.fori_loop(1, count - 1, step, 0, unroll=2)
        step(count - 1, 0)

    def sweep(source, target, slot, edges, count, reach, rhs, scale, change, keep, gain, started, onward, out=None):
        finish = exchange_faces(source, count, slot, started, *edges)

        def step(plane, carry):
            here = rows_of(plane)
            field, total = beside(source, plane, count, reach)
            moved = gain * (scale[here, :] * (rhs[here, :] + total) - field)
            if keep:
                moved = moved + keep * change[here, :]
            if out is not None:
                out[here, :] = field + moved
            else:
                change[here, :] = moved
                target[rows_of(plane + 1), :] = field + moved
            return carry

        inner_planes(count, step)
        finish()
        if out is not None:
            return correct(source, out, 0, slot, count, reach, scale, gain, None, False)
        return correct(source, target, plane_rows, slot, count, reach, scale, gain, change, onward)

    ratio = centre / spread
    gains, factor = [], 1.0 / ratio
    for _ in range(COARSE_SMOOTH):
        factor_new = 1.0 / (2.0 * ratio - factor)
        gains.append((factor_new * factor, 2.0 * factor_new / spread))
        factor = factor_new

    def first_step(plane, carry):
        here = rows_of(plane)
        scale = 1.0 / (6.0 + shift_ref[here, :])
        inverse[here, :] = scale
        added = [added_ref[rows_of(part * nplane + plane), :] for part in range(width // LANES)]
        forcing = rhs_ref[here, :] + jnp.concatenate(added, axis=1)
        forcing_ref[here, :] = forcing
        answer = scale * forcing * (1.0 / centre)
        update[here, :] = answer
        wide_a[rows_of(plane + 1), :] = answer
        return columns_of(answer, plane, 0, *carry)

    edges = each_plane(nplane, first_step)
    slot = 0
    pl.semaphore_wait(barrier, neighbours)
    for sweep_index in range(SMOOTH - 1):
        keep, gain = gains[sweep_index]
        edges = sweep(
            wide[slot], wide[1 - slot], slot, edges, nplane, 1, forcing_ref, inverse, update, keep, gain,
            sweep_index > 0, True,
        )
        slot = 1 - slot
    smooth, remains_ref = wide[slot], wide[1 - slot]

    lane_pair = lax.broadcasted_iota(jnp.int32, (8, LANES), 1) ^ 1
    line_pair = lax.broadcasted_iota(jnp.int32, (8, LANES), 0) ^ 1

    def pair_sum(value):
        lines = []
        for tile in range(tiles):
            parts = []
            for part in range(width // LANES):
                block = value[8 * tile : 8 * tile + 8, part * LANES : (part + 1) * LANES]
                block = block + pick(block, lane_pair, 1)
                parts.append(block + pick(block, line_pair, 0))
            lines.append(jnp.concatenate(parts, axis=1))
        return jnp.concatenate(lines, axis=0)

    finish = exchange_faces(smooth, nplane, slot, True, *edges)

    def leave(plane, carry):
        here = rows_of(plane)
        field, total = beside(smooth, plane, nplane, 1)
        remains_ref[rows_of(plane + 1), :] = forcing_ref[here, :] - ((6.0 + shift_ref[here, :]) * field - total)
        return carry

    inner_planes(nplane, leave)
    finish()
    correct(smooth, remains_ref, plane_rows, slot, nplane, 1, None, 1.0, None, False)
    slot = 1 - slot

    def restrict(plane, carry):
        remains = remains_ref[rows_of(2 * plane + 1), :] + remains_ref[rows_of(2 * plane + 2), :]
        shifts = shift_ref[rows_of(2 * plane), :] + shift_ref[rows_of(2 * plane + 1), :]
        rhs = 0.5 * pair_sum(remains)
        scale = 1.0 / (6.0 + 0.5 * pair_sum(shifts))
        answer = scale * rhs * (1.0 / centre)
        here = rows_of(plane)
        coarse_rhs[here, :] = rhs
        coarse_inverse[here, :] = scale
        coarse_update[here, :] = answer
        coarse[slot][rows_of(plane + 1), :] = answer
        return columns_of(answer, plane, slot, *carry)

    edges = each_plane(ncoarse, restrict)
    for sweep_index in range(COARSE_SMOOTH - 1):
        keep, gain = gains[sweep_index]
        edges = sweep(
            coarse[slot], coarse[1 - slot], slot, edges, ncoarse, 2,
            coarse_rhs, coarse_inverse, coarse_update, keep, gain,
            sweep_index > 0, sweep_index < COARSE_SMOOTH - 2,
        )
        slot = 1 - slot
    fix = coarse[slot]

    def begin_again(plane, carry):
        here = rows_of(plane + 1)
        answer = smooth[here, :] + fix[rows_of(lax.div(plane, 2) + 1), :]
        wide[slot][here, :] = answer
        return columns_of(answer, plane, slot, *carry)

    edges = each_plane(nplane, begin_again)
    for sweep_index in range(SMOOTH):
        keep, gain = gains[sweep_index - 1] if sweep_index else (0.0, 1.0 / centre)
        edges = sweep(
            wide[slot], wide[1 - slot], slot, edges, nplane, 1, forcing_ref, inverse, update, keep, gain,
            sweep_index > 0, True, pressure_ref if sweep_index == SMOOTH - 1 else None,
        )
        slot = 1 - slot


def multigrid(added, pressure_rhs, shift_diag):
    planes, rows, width = shift_diag.shape
    vmem = pl.BlockSpec(memory_space=pltpu.VMEM)
    flat = (planes * rows, width)
    half = (planes // 2 * rows, width)
    f32 = jnp.float32
    return pl.pallas_call(
        functools.partial(cycle_kernel, rows),
        name="multigrid",
        out_shape=jax.ShapeDtypeStruct(flat, f32),
        in_specs=[vmem] * 3,
        out_specs=vmem,
        scratch_shapes=[
            pltpu.VMEM(flat, f32),
            pltpu.VMEM((flat[0] + 2 * rows, width), f32),
            pltpu.VMEM((flat[0] + 2 * rows, width), f32),
            pltpu.VMEM((half[0] + 2 * rows, width), f32),
            pltpu.VMEM((half[0] + 2 * rows, width), f32),
            pltpu.VMEM(flat, f32),
            pltpu.VMEM(flat, f32),
            pltpu.VMEM(half, f32),
            pltpu.VMEM(half, f32),
            pltpu.VMEM(half, f32),
            pltpu.VMEM((2, 2, planes, width), f32),
            pltpu.VMEM((2, 2, planes, width), f32),
            pltpu.VMEM((2, 2, 8, LANES), f32),
            pltpu.VMEM((2, 2, 8, LANES), f32),
            pltpu.SemaphoreType.DMA((2, 6)),
            pltpu.SemaphoreType.DMA((2, 6)),
        ],
        compiler_params=pltpu.CompilerParams(
            vmem_limit_bytes=40 * 1024 * 1024, collective_id=0, has_side_effects=True
        ),
    )(added, pressure_rhs.reshape(flat), shift_diag.reshape(flat)).reshape(shift_diag.shape)


def body(
    pressure_rhs,
    shift_diag,
    positions,
    normals,
    tension,
    edge_weight,
    owner_map,
    cell_map,
    connectivity,
):
    nrow = positions.shape[1] // LANES
    got = surface_and_send(
        positions,
        normals,
        tension.reshape(nrow, LANES),
        edge_weight,
        owner_map.reshape(nrow, LANES),
        cell_map.reshape(nrow, LANES),
        connectivity,
    )
    added, surface_force = spread_cells(got.reshape(-1, LANES), positions.shape[1], pressure_rhs.size)
    pressure = multigrid(added, pressure_rhs, shift_diag)
    return (pressure, surface_force)


def solution(mesh):
    return jax.shard_map(
        body,
        mesh=mesh,
        in_specs=(
            P("gx", "gy", "gz"),
            P("gx", "gy", "gz"),
            P(None, ("gx", "gy", "gz")),
            P(None, ("gx", "gy", "gz")),
            P(("gx", "gy", "gz")),
            P(None, ("gx", "gy", "gz")),
            P(("gx", "gy", "gz"), None),
            P(("gx", "gy", "gz")),
            P(None, ("gx", "gy", "gz")),
        ),
        out_specs=(P("gx", "gy", "gz"), P(None, ("gx", "gy", "gz"))),
        check_vma=False,
    )
```
